8 devices in a mesh: dp: 1 (over z), ep: 8 (over y, x, core).
Axes of the slice: x: 2, y: 2, z: 1, core: 2. Of those that a mesh axis runs over, the one named last changes fastest.
Arguments:
- hidden: bfloat16 [4096, 2560], P(('dp', 'ep'))
- w_router: bfloat16 [2560, 64], replicated
- w_gate: bfloat16 [64, 2560, 1536], P('ep')
- w_up: bfloat16 [64, 2560, 1536], P('ep')
- w_down: bfloat16 [64, 1536, 2560], P('ep')
- shared_gate: bfloat16 [2560, 3072], replicated
- shared_up: bfloat16 [2560, 3072], replicated
- shared_down: bfloat16 [3072, 2560], replicated
- top_idx: int32 [4096, 6], P(('dp', 'ep'))
- keep_mask: int32 [4096, 6], P(('dp', 'ep'))
Outputs:
- output: bfloat16 [4096, 2560], P(('dp', 'ep'))
All inputs are finite; a program needn't handle non-finite values.
Results may differ from the reference program's by a relative error of at most 0.00691395.
Values are sent between devices in bfloat16 or wider.
A program may use at most 1 GiB of HBM per device.

```python
import math
import jax
import jax.numpy as jnp
from jax import lax

HIDDEN = 2560
EXPERTS = 64
EXPERT_FF = 1536
SHARED_FF = 3072
TOP_K = 6
DEV_LIMIT = 6
TOKENS = 512
GROUP_SIZE = 8
CAPACITY = 96

ROUTE_SCALE = 16.0
PER_DEVICE = EXPERTS // GROUP_SIZE
PART_TOKENS = GROUP_SIZE * TOKENS
ROUTED_GAIN = EXPERTS / (ROUTE_SCALE * math.sqrt(TOP_K))


def draw_routing(route_key):
    k_noise, k_dev, k_exp, k_hot = jax.random.split(route_key, 4)
    expert_ids = jnp.arange(EXPERTS, dtype=jnp.int32)
    noise_int = jax.random.randint(k_noise, (PART_TOKENS, EXPERTS), 0, 256, dtype=jnp.int32)
    dev_bias = jax.random.randint(k_dev, (GROUP_SIZE,), 0, 128, dtype=jnp.int32)
    exp_bias = jax.random.randint(k_exp, (EXPERTS,), 0, 64, dtype=jnp.int32)
    hot_expert = jax.random.randint(k_hot, (), 0, EXPERTS, dtype=jnp.int32)
    bias_all = exp_bias + jnp.repeat(dev_bias, PER_DEVICE) + jnp.where(expert_ids == hot_expert, 1024, 0)
    pair_score = (noise_int + bias_all[None, :]) * EXPERTS + expert_ids[None, :]
    dev_score = jnp.max(pair_score.reshape(PART_TOKENS, GROUP_SIZE, PER_DEVICE), axis=2)
    top_dev = lax.top_k(dev_score, DEV_LIMIT)[1]
    chosen = jnp.any(top_dev[:, :, None] == jnp.arange(GROUP_SIZE, dtype=jnp.int32)[None, None, :], axis=1)
    masked = jnp.where(jnp.repeat(chosen, PER_DEVICE, axis=1), pair_score, -1)
    top_idx = lax.top_k(masked, TOP_K)[1].astype(jnp.int32)

    def rank_pairs(src_pairs):
        onehot = (src_pairs[:, None] == expert_ids[None, :]).astype(jnp.int32)
        return jnp.sum((jnp.cumsum(onehot, axis=0) - 1) * onehot, axis=1)

    pair_rank = lax.map(rank_pairs, top_idx.reshape(GROUP_SIZE, TOKENS * TOP_K))
    keep_mask = (pair_rank < CAPACITY).astype(jnp.int32).reshape(PART_TOKENS, TOP_K)
    return top_idx, keep_mask


def draw_bank(bank_key, mat_shape, std_scale):
    key_list = jax.random.split(bank_key, EXPERTS)
    return lax.map(lambda one_key: (jax.random.normal(one_key, mat_shape, jnp.float32) * std_scale).astype(jnp.bfloat16), key_list)


def draw_matrix(mat_key, mat_shape, std_scale):
    return (jax.random.normal(mat_key, mat_shape, jnp.float32) * std_scale).astype(jnp.bfloat16)


def setup_inputs(seed: int = 0, part: int = 0) -> dict:
    root_key = jax.random.key(seed)
    part_key = jax.random.fold_in(root_key, part)
    k_hidden, k_route = jax.random.split(part_key, 2)
    k_router, k_gate, k_up, k_down, k_sgate, k_sup, k_sdown = jax.random.split(root_key, 7)
    top_idx, keep_mask = draw_routing(k_route)
    in_scale = HIDDEN ** -0.5
    return {
        "hidden": draw_matrix(k_hidden, (PART_TOKENS, HIDDEN), 1.0),
        "w_router": draw_matrix(k_router, (HIDDEN, EXPERTS), 0.5 * in_scale),
        "w_gate": draw_bank(k_gate, (HIDDEN, EXPERT_FF), in_scale),
        "w_up": draw_bank(k_up, (HIDDEN, EXPERT_FF), in_scale),
        "w_down": draw_bank(k_down, (EXPERT_FF, HIDDEN), ROUTED_GAIN * EXPERT_FF ** -0.5),
        "shared_gate": draw_matrix(k_sgate, (HIDDEN, SHARED_FF), in_scale),
        "shared_up": draw_matrix(k_sup, (HIDDEN, SHARED_FF), in_scale),
        "shared_down": draw_matrix(k_sdown, (SHARED_FF, HIDDEN), SHARED_FF ** -0.5),
        "top_idx": top_idx,
        "keep_mask": keep_mask,
    }


def swiglu(tok_rows, gate_w, up_w, down_w):
    h_gate = jnp.dot(tok_rows, gate_w, preferred_element_type=jnp.float32)
    h_up = jnp.dot(tok_rows, up_w, preferred_element_type=jnp.float32)
    act_rows = (jax.nn.silu(h_gate) * h_up).astype(jnp.bfloat16)
    return jnp.dot(act_rows, down_w, preferred_element_type=jnp.float32)


def reference(hidden, w_router, w_gate, w_up, w_down, shared_gate, shared_up, shared_down, top_idx, keep_mask):
    logits = jnp.dot(hidden, w_router, preferred_element_type=jnp.float32)
    router_prob = jax.nn.softmax(logits, axis=-1)
    gate_vals = ROUTE_SCALE * jnp.take_along_axis(router_prob, top_idx, axis=1) * keep_mask.astype(jnp.float32)
    pair_expert = top_idx.reshape(-1)
    pair_kept = keep_mask.reshape(-1) > 0
    pair_gate = gate_vals.reshape(-1)
    pair_token = jnp.arange(PART_TOKENS * TOP_K, dtype=jnp.int32) // TOP_K
    max_rows = GROUP_SIZE * CAPACITY

    def expert_step(routed_acc, per_expert):
        gate_w, up_w, down_w, expert_id = per_expert
        member = pair_kept & (pair_expert == expert_id)
        pair_slot = jnp.where(member, jnp.cumsum(member.astype(jnp.int32)) - 1, max_rows)
        row_token = jnp.zeros((max_rows,), jnp.int32).at[pair_slot].set(pair_token, mode="drop")
        row_gate = jnp.zeros((max_rows,), jnp.float32).at[pair_slot].set(pair_gate, mode="drop")
        expert_out = swiglu(hidden[row_token], gate_w, up_w, down_w).astype(jnp.bfloat16)
        routed_acc = routed_acc.at[row_token].add(row_gate[:, None] * expert_out.astype(jnp.float32))
        return routed_acc, None

    routed = lax.scan(expert_step, jnp.zeros((PART_TOKENS, HIDDEN), jnp.float32), (w_gate, w_up, w_down, jnp.arange(EXPERTS, dtype=jnp.int32)))[0]
    shared = lax.map(lambda tok_block: swiglu(tok_block, shared_gate, shared_up, shared_down), hidden.reshape(GROUP_SIZE, TOKENS, HIDDEN)).reshape(PART_TOKENS, HIDDEN)
    return (shared + routed).astype(jnp.bfloat16)
```

```python
import functools

import jax
import jax.numpy as jnp
from jax import lax
from jax.experimental import pallas as pl
from jax.experimental.pallas import tpu as pltpu
from jax.sharding import PartitionSpec as P

ROUTE_SCALE = 16.0
CAP = 96
VMEM_BYTES = 66_900_000
MESH = pl.DeviceIdType.MESH
F32 = jnp.float32
BF16 = jnp.bfloat16


def dot(a, b):
    return jnp.dot(a, b, preferred_element_type=F32)


def swiglu(tok_rows, gate_w, up_w, down_w):
    h_gate = dot(tok_rows, gate_w)
    h_up = dot(tok_rows, up_w)
    act_rows = (jax.nn.silu(h_gate) * h_up).astype(BF16)
    return dot(act_rows, down_w)


def route_kernel(x_ref, w_ref, idx_ref, keep_ref, tab_ref):
    experts, tokens = w_ref.shape[1], x_ref.shape[0]
    logits = lax.dot_general(w_ref[...], x_ref[...], (((0,), (1,)), ((), ())), preferred_element_type=F32)
    e = jnp.exp(logits - jnp.max(logits, axis=0, keepdims=True))
    prob = e / jnp.sum(e, axis=0, keepdims=True)
    expert_id = lax.broadcasted_iota(jnp.int32, (experts, tokens), 0)
    member = jnp.zeros((experts, tokens), F32)
    for k in range(idx_ref.shape[0]):
        hit = (expert_id == idx_ref[k : k + 1, :]) & (keep_ref[k : k + 1, :] > 0)
        member = jnp.where(hit, 1.0, member)
    earlier = lax.broadcasted_iota(jnp.int32, (tokens, tokens), 0) < lax.broadcasted_iota(jnp.int32, (tokens, tokens), 1)
    rank = dot(member.astype(BF16), jnp.where(earlier, 1.0, 0.0).astype(BF16))
    slot = jnp.where(member > 0, rank, -1.0)
    gate = ROUTE_SCALE * prob * member
    half = tab_ref.shape[1] // 2
    for d in range(tab_ref.shape[0]):
        tab_ref[d, :half, :] = slot[d * half : (d + 1) * half]
        tab_ref[d, half:, :] = gate[d * half : (d + 1) * half]


def up_kernel(tab_ref, x_hbm, w1_hbm, w3_hbm, act_hbm, xg, xbuf, dbuf, wg, wu, ab, x_sem, w_sem, a_sem):
    groups, tokens, width = x_hbm.shape
    per_dev, _, ff = w1_hbm.shape
    tn = wg.shape[2]
    nt = ff // tn
    steps = per_dev * nt
    xc = 512

    def x_copy(s, slot):
        return pltpu.make_async_copy(x_hbm.at[s], xbuf.at[slot], x_sem.at[slot])

    def w_copies(it, slot):
        e, n = it // nt, lax.rem(it, nt)
        cols = pl.ds(pl.multiple_of(n * tn, tn), tn)
        return (
            pltpu.make_async_copy(w1_hbm.at[e, :, cols], wg.at[slot], w_sem.at[0, slot]),
            pltpu.make_async_copy(w3_hbm.at[e, :, cols], wu.at[slot], w_sem.at[1, slot]),
        )

    def a_copy(it, slot):
        e, n = it // nt, lax.rem(it, nt)
        cols = pl.ds(pl.multiple_of(n * tn, tn), tn)
        return pltpu.make_async_copy(ab.at[slot], act_hbm.at[e, :, cols], a_sem.at[slot])

    x_copy(0, 0).start()
    for c in w_copies(0, 0):
        c.start()
    row = lax.broadcasted_iota(jnp.int32, (CAP, tokens), 0).astype(F32)

    def gather(s, _):
        slot = lax.rem(s, 2)

        @pl.when(s + 1 < groups)
        def _():
            x_copy(s + 1, 1 - slot).start()

        for e in range(per_dev):
            dbuf[e * CAP : (e + 1) * CAP, :] = jnp.where(row == tab_ref[s, e : e + 1, :], 1.0, 0.0).astype(BF16)
        x_copy(s, slot).wait()
        rows = pl.ds(pl.multiple_of(s * CAP, CAP), CAP)

        def cols_step(n, _):
            cols = pl.ds(pl.multiple_of(n * xc, xc), xc)
            got = dot(dbuf[...], xbuf[slot, :, cols]).astype(BF16)
            xg[:, rows, cols] = got.reshape(per_dev, CAP, xc)
            return 0

        lax.fori_loop(0, width // xc, cols_step, 0)
        return 0

    lax.fori_loop(0, groups, gather, 0)

    def main(it, _):
        slot = lax.rem(it, 2)
        e = it // nt

        @pl.when(it + 1 < steps)
        def _():
            for c in w_copies(it + 1, 1 - slot):
                c.start()

        for c in w_copies(it, slot):
            c.wait()

        @pl.when(it >= 2)
        def _():
            a_copy(it - 2, slot).wait()

        h_gate = dot(xg[e], wg[slot])
        h_up = dot(xg[e], wu[slot])
        ab[slot] = (jax.nn.silu(h_gate) * h_up).astype(BF16)
        a_copy(it, slot).start()
        return 0

    lax.fori_loop(0, steps, main, 0)
    a_copy(steps - 2, steps % 2).wait()
    a_copy(steps - 1, (steps - 1) % 2).wait()


def down_kernel(
    tab_ref, act_hbm, w2_hbm, ys_hbm, y_hbm,
    comb, act, part, wbuf, fsend, frecv, mine, bsend, brecv, acc, ybuf,
    act_sem, w_sem, acc_sem, y_sem, fs_sem, fr_sem, bs_sem, br_sem, credit,
):
    groups, pair, tokens = tab_ref.shape
    per_dev = pair // 2
    rows = per_dev * CAP
    cw = wbuf.shape[2]
    nc = acc.shape[0]
    steps = 4 * nc

    me = lax.axis_index("ep")
    core, chip = lax.rem(me, 2), me // 2
    partner = me + 1 - 2 * core
    yb, xb = chip // 2, lax.rem(chip, 2)

    def chip_at(j):
        m = 3 - j
        return 2 * lax.rem(yb + m // 2, 2) + lax.rem(xb + lax.rem(m, 2), 2)

    def w_copy(it, slot):
        c, e = it // per_dev, lax.rem(it, per_dev)
        cols = pl.ds(pl.multiple_of(c * cw, cw), cw)
        return pltpu.make_async_copy(w2_hbm.at[e, :, cols], wbuf.at[slot], w_sem.at[slot])

    def act_copy(e):
        return pltpu.make_async_copy(act_hbm.at[e], act.at[e], act_sem.at[e])

    def acc_copy(c):
        return pltpu.make_async_copy(ys_hbm.at[:, pl.ds(c * cw, cw)], acc.at[c], acc_sem.at[c])

    w_copy(0, 0).start()
    for e in range(per_dev):
        act_copy(e).start()
    for c in range(nc):
        acc_copy(c).start()

    barrier = pltpu.get_barrier_semaphore()
    pl.semaphore_signal(barrier, inc=1, device_id={"ep": partner}, device_id_type=MESH)
    for j in range(3):
        pl.semaphore_signal(barrier, inc=1, device_id={"ep": 2 * chip_at(j) + core}, device_id_type=MESH)
    pl.semaphore_wait(barrier, 4)

    lane = lax.broadcasted_iota(jnp.int32, (per_dev, rows), 1)
    first = lax.broadcasted_iota(jnp.int32, (per_dev, rows), 0) * CAP
    inside = (lane >= first) & (lane < first + CAP)
    spread = jnp.where(inside, 1.0, 0.0).astype(BF16)
    want = jnp.sum(jnp.where(inside, lane - first, 0).astype(F32), axis=0, keepdims=True)

    def over_slots(v):
        return lax.dot_general(v, spread, (((0,), (0,)), ((), ())), preferred_element_type=F32)

    def build(s, _):
        hit = over_slots(tab_ref[s, :per_dev, :].astype(BF16)) == want
        gate = tab_ref[s, per_dev:, :]
        hi = gate.astype(BF16)
        rest = gate - hi.astype(F32)
        mid = rest.astype(BF16)
        low = (rest - mid.astype(F32)).astype(BF16)
        for k, piece in enumerate((hi, mid, low)):
            comb[k, s] = jnp.where(hit, over_slots(piece), 0.0).astype(BF16)
        return 0

    lax.fori_loop(0, groups, build, 0)
    for c in range(nc):
        acc_copy(c).wait()

    def f_copy(slot):
        return pltpu.make_async_remote_copy(
            src_ref=fsend.at[slot], dst_ref=frecv.at[slot], send_sem=fs_sem.at[slot], recv_sem=fr_sem.at[slot],
            device_id={"ep": partner}, device_id_type=MESH)

    def b_copy(j, c):
        slot = lax.rem(c, 2)
        return pltpu.make_async_remote_copy(
            src_ref=bsend.at[j, slot], dst_ref=brecv.at[j, c], send_sem=bs_sem.at[j, slot], recv_sem=br_sem.at[j, c],
            device_id={"ep": 2 * chip_at(j) + core}, device_id_type=MESH)

    def combine(s):
        return dot(comb[0, s], part[s]) + dot(comb[1, s], part[s]) + dot(comb[2, s], part[s])

    def launch(h):
        j = lax.rem(h, 4)

        @pl.when(j < 3)
        def _():
            b_copy(j, h // 4).start()

    def consume(h):
        slot, c, j = lax.rem(h, 2), h // 4, lax.rem(h, 4)
        f_copy(slot).wait_recv()

        @pl.when(j < 3)
        def _():
            @pl.when(c >= 2)
            def _():
                b_copy(j, c - 2).wait_send()

            bsend[j, lax.rem(c, 2)] = (mine[slot] + frecv[slot]).astype(BF16)

        @pl.when(j == 3)
        def _():
            acc[c] = acc[c] + (mine[slot] + frecv[slot])

        @pl.when(h + 2 < steps)
        def _():
            pl.semaphore_signal(credit, inc=1, device_id={"ep": partner}, device_id_type=MESH)

    def chunk(c, _):
        def down(e, _):
            it = c * per_dev + e
            slot = lax.rem(it, 2)

            @pl.when(it + 1 < nc * per_dev)
            def _():
                w_copy(it + 1, 1 - slot).start()

            w_copy(it, slot).wait()

            @pl.when(c == 0)
            def _():
                act_copy(e).wait()

            got = dot(act[e], wbuf[slot]).astype(BF16)
            part[:, pl.ds(pl.multiple_of(e * CAP, CAP), CAP), :] = got.reshape(groups, CAP, cw)
            return 0

        lax.fori_loop(0, per_dev, down, 0)

        def pair_step(j, _):
            g = 4 * c + j
            slot = lax.rem(g, 2)
            q = chip_at(j)

            @pl.when(g >= 2)
            def _():
                f_copy(slot).wait_send()

            fsend[slot] = combine(2 * q + 1 - core)
            mine[slot] = combine(2 * q + core)

            @pl.when(g >= 2)
            def _():
                pl.semaphore_wait(credit, 1)

            f_copy(slot).start()

            @pl.when(g >= 2)
            def _():
                launch(g - 2)

            @pl.when(g >= 1)
            def _():
                consume(g - 1)

            return 0

        lax.fori_loop(0, 4, pair_step, 0)
        return 0

    lax.fori_loop(0, nc, chunk, 0)
    launch(steps - 2)
    consume(steps - 1)
    f_copy(0).wait_send()
    f_copy(1).wait_send()

    def y_copy(c):
        return pltpu.make_async_copy(ybuf.at[c % 2], y_hbm.at[:, pl.ds(c * cw, cw)], y_sem.at[c % 2])

    for c in range(nc):
        for j in range(3):
            b_copy(j, c).wait_recv()
            if c >= nc - 2:
                b_copy(j, c).wait_send()
        if c >= 2:
            y_copy(c - 2).wait()
        total = acc[c]
        for j in range(3):
            total = total + brecv[j, c].astype(F32)
        ybuf[c % 2] = total.astype(BF16)
        y_copy(c).start()
    y_copy(nc - 2).wait()
    y_copy(nc - 1).wait()


def solution(mesh):
    groups = mesh.shape["ep"]
    tok_spec = P(("dp", "ep"), None)
    bank_spec = P("ep", None, None)
    vmem = pl.BlockSpec(memory_space=pltpu.VMEM)
    hbm = pl.BlockSpec(memory_space=pl.ANY)

    def device_fn(hidden, w_router, w_gate, w_up, w_down, shared_gate, shared_up, shared_down, top_idx, keep_mask):
        tokens, width = hidden.shape
        per_dev, _, ff = w_gate.shape
        rows = groups * CAP
        tn, cw = 256, 256
        nc = width // cw
        x_all = lax.all_gather(hidden, "ep", axis=0, tiled=False)
        tab = pl.pallas_call(
            route_kernel,
            out_shape=jax.ShapeDtypeStruct((groups, 2 * per_dev, tokens), F32),
            in_specs=[vmem] * 4,
            out_specs=vmem,
            name="route",
        )(hidden, w_router, top_idx.T, keep_mask.T)
        tab = lax.all_to_all(tab, "ep", 0, 0, tiled=True)
        shared = swiglu(hidden, shared_gate, shared_up, shared_down)
        act = pl.pallas_call(
            up_kernel,
            out_shape=jax.ShapeDtypeStruct((per_dev, rows, ff), BF16),
            in_specs=[vmem, hbm, hbm, hbm],
            out_specs=hbm,
            scratch_shapes=[
                pltpu.VMEM((per_dev, rows, width), BF16),
                pltpu.VMEM((2, tokens, width), BF16),
                pltpu.VMEM((per_dev * CAP, tokens), BF16),
                pltpu.VMEM((2, width, tn), BF16),
                pltpu.VMEM((2, width, tn), BF16),
                pltpu.VMEM((2, rows, tn), BF16),
                pltpu.SemaphoreType.DMA((2,)),
                pltpu.SemaphoreType.DMA((2, 2)),
                pltpu.SemaphoreType.DMA((2,)),
            ],
            compiler_params=pltpu.CompilerParams(vmem_limit_bytes=VMEM_BYTES),
            cost_estimate=pl.CostEstimate(flops=4 * per_dev * rows * width * ff, bytes_accessed=4 * per_dev * width * ff, transcendentals=0),
            name="up",
        )(tab, x_all, w_gate, w_up)
        return pl.pallas_call(
            down_kernel,
            out_shape=jax.ShapeDtypeStruct((tokens, width), BF16),
            in_specs=[vmem, hbm, hbm, hbm],
            out_specs=hbm,
            scratch_shapes=[
                pltpu.VMEM((3, groups, tokens, per_dev * CAP), BF16),
                pltpu.VMEM((per_dev, rows, ff), BF16),
                pltpu.VMEM((groups, per_dev * CAP, cw), BF16),
                pltpu.VMEM((2, ff, cw), BF16),
                pltpu.VMEM((2, tokens, cw), F32),
                pltpu.VMEM((2, tokens, cw), F32),
                pltpu.VMEM((2, tokens, cw), F32),
                pltpu.VMEM((3, 2, tokens, cw), BF16),
                pltpu.VMEM((3, nc, tokens, cw), BF16),
                pltpu.VMEM((nc, tokens, cw), F32),
                pltpu.VMEM((2, tokens, cw), BF16),
                pltpu.SemaphoreType.DMA((per_dev,)),
                pltpu.SemaphoreType.DMA((2,)),
                pltpu.SemaphoreType.DMA((nc,)),
                pltpu.SemaphoreType.DMA((2,)),
                pltpu.SemaphoreType.DMA((2,)),
                pltpu.SemaphoreType.DMA((2,)),
                pltpu.SemaphoreType.DMA((3, 2)),
                pltpu.SemaphoreType.DMA((3, nc)),
                pltpu.SemaphoreType.REGULAR,
            ],
            compiler_params=pltpu.CompilerParams(vmem_limit_bytes=VMEM_BYTES, collective_id=0, has_side_effects=True),
            cost_estimate=pl.CostEstimate(flops=8 * per_dev * rows * width * ff, bytes_accessed=2 * per_dev * width * ff, transcendentals=0),
            name="down",
        )(tab, act, w_down, shared)

    return jax.shard_map(device_fn, mesh=mesh, in_specs=(tok_spec, P(), bank_spec, bank_spec, bank_spec, P(), P(), P(), tok_spec, tok_spec), out_specs=tok_spec, check_vma=False)
```

```python
import functools

import jax
import jax.numpy as jnp
from jax import lax
from jax.experimental import pallas as pl
from jax.experimental.pallas import tpu as pltpu
from jax.sharding import PartitionSpec as P

ROUTE_SCALE = 16.0
CAP = 96
VMEM_BYTES = 66_900_000
MESH = pl.DeviceIdType.MESH
F32 = jnp.float32
BF16 = jnp.bfloat16


def dot(a, b):
    return jnp.dot(a, b, preferred_element_type=F32)


def route_kernel(x_ref, w_ref, idx_ref, keep_ref, tab_ref):
    experts, tokens = w_ref.shape[1], x_ref.shape[0]
    logits = lax.dot_general(w_ref[...], x_ref[...], (((0,), (1,)), ((), ())), preferred_element_type=F32)
    e = jnp.exp(logits - jnp.max(logits, axis=0, keepdims=True))
    prob = e / jnp.sum(e, axis=0, keepdims=True)
    expert_id = lax.broadcasted_iota(jnp.int32, (experts, tokens), 0)
    member = jnp.zeros((experts, tokens), F32)
    for k in range(idx_ref.shape[0]):
        hit = (expert_id == idx_ref[k : k + 1, :]) & (keep_ref[k : k + 1, :] > 0)
        member = jnp.where(hit, 1.0, member)
    earlier = lax.broadcasted_iota(jnp.int32, (tokens, tokens), 0) < lax.broadcasted_iota(jnp.int32, (tokens, tokens), 1)
    rank = dot(member.astype(BF16), jnp.where(earlier, 1.0, 0.0).astype(BF16))
    slot = jnp.where(member > 0, rank, -1.0)
    gate = ROUTE_SCALE * prob * member
    half = tab_ref.shape[1] // 2
    for d in range(tab_ref.shape[0]):
        tab_ref[d, :half, :] = slot[d * half : (d + 1) * half]
        tab_ref[d, half:, :] = gate[d * half : (d + 1) * half]


def relatives():
    me = lax.axis_index("ep")
    core, chip = lax.rem(me, 2), me // 2
    yb, xb = chip // 2, lax.rem(chip, 2)

    def first_core(r):
        return 2 * (2 * lax.rem(yb + r // 2, 2) + lax.rem(xb + lax.rem(r, 2), 2))

    return me, core, me + 1 - 2 * core, first_core


def up_kernel(
    tab_ref, x_hbm, w1_hbm, w3_hbm, sg_hbm, su_hbm, sd_hbm, tabs_ref, ys_hbm, act_hbm, x_all,
    tabs, xown, xbuf, xg, dbuf, wg, wu, wd, hs, ab, yb,
    own_sem, x_sem, w_sem, d_sem, a_sem, y_sem, ts_sem, tr_sem, xs_sem, xr_sem,
):
    groups = tabs.shape[0]
    tokens, width = x_hbm.shape
    per_dev, _, ff = w1_hbm.shape
    slots, _, tn = wg.shape
    nt, ns, nd = ff // tn, sg_hbm.shape[1] // tn, width // tn
    steps = per_dev * nt
    xc = 512
    early = 2 * CAP
    late = groups * CAP - early
    forward_at = (5 * steps) // 8

    me, core, partner, first_core = relatives()

    def block_copy(k, src, pos, device):
        return pltpu.make_async_remote_copy(
            src_ref=src, dst_ref=x_all.at[pos], send_sem=xs_sem.at[k], recv_sem=xr_sem.at[pos],
            device_id={"ep": device}, device_id_type=MESH)

    def table_copy(r, k):
        dst = first_core(r) + k
        return pltpu.make_async_remote_copy(
            src_ref=tab_ref.at[dst], dst_ref=tabs.at[2 * r + core], send_sem=ts_sem.at[2 * r + k], recv_sem=tr_sem.at[2 * r + core],
            device_id={"ep": dst}, device_id_type=MESH)

    sends = [
        block_copy(0, x_hbm, core, partner),
        block_copy(1, x_hbm, 2 + core, first_core(1) + core),
        block_copy(2, x_hbm, 4 + core, first_core(2) + core),
        block_copy(3, x_all.at[2 + core], 2 + core, partner),
        block_copy(4, x_all.at[4 + core], 4 + core, partner),
        block_copy(5, x_all.at[4 - core], 6 + core, first_core(1 + core) + core),
        block_copy(6, x_all.at[6 + core], 6 + core, partner),
    ]

    def arrived(pos):
        block_copy(0, x_hbm, pos, partner).wait_recv()

    def w_start(t):
        slot = lax.rem(t, slots)

        def go(a, b):
            pltpu.make_async_copy(a, wg.at[slot], w_sem.at[0, slot]).start()
            pltpu.make_async_copy(b, wu.at[slot], w_sem.at[1, slot]).start()

        @pl.when(t < ns)
        def _():
            cols = pl.ds(pl.multiple_of(t * tn, tn), tn)
            go(sg_hbm.at[:, cols], su_hbm.at[:, cols])

        @pl.when((t >= ns) & (t < ns + 2 * steps))
        def _():
            it = lax.rem(t - ns, steps)
            cols = pl.ds(pl.multiple_of(lax.rem(it, nt) * tn, tn), tn)
            go(w1_hbm.at[it // nt, :, cols], w3_hbm.at[it // nt, :, cols])

    def w_wait(t):
        slot = lax.rem(t, slots)
        pltpu.make_async_copy(sg_hbm.at[:, pl.ds(0, tn)], wg.at[slot], w_sem.at[0, slot]).wait()
        pltpu.make_async_copy(sg_hbm.at[:, pl.ds(0, tn)], wu.at[slot], w_sem.at[1, slot]).wait()
        return slot

    def d_copy(n):
        cols = pl.ds(pl.multiple_of(n * tn, tn), tn)
        return pltpu.make_async_copy(sd_hbm.at[:, cols], wd.at[lax.rem(n, 2)], d_sem.at[lax.rem(n, 2)])

    def y_copy(n):
        cols = pl.ds(pl.multiple_of(n * tn, tn), tn)
        return pltpu.make_async_copy(yb.at[lax.rem(n, 2)], ys_hbm.at[:, cols], y_sem.at[lax.rem(n, 2)])

    own_copy = pltpu.make_async_copy(x_hbm, xown, own_sem)
    own_copy.start()
    for t in range(slots - 1):
        w_start(t)
    d_copy(0).start()

    barrier = pltpu.get_barrier_semaphore()
    for d in range(1, groups):
        pl.semaphore_signal(barrier, inc=1, device_id={"ep": lax.rem(me + d, groups)}, device_id_type=MESH)
    pl.semaphore_wait(barrier, groups - 1)
    for k in range(3):
        sends[k].start()
    for r in range(4):
        for k in range(2):
            if r == 0:
                @pl.when(k != core)
                def _():
                    table_copy(r, k).start()
            else:
                table_copy(r, k).start()
    tabs[core] = tab_ref[me]
    own_copy.wait()

    def shared_up(t, _):
        w_start(t + slots - 1)
        slot = w_wait(t)
        h_gate = dot(xown[...], wg[slot])
        h_up = dot(xown[...], wu[slot])
        hs[:, pl.ds(pl.multiple_of(t * tn, tn), tn)] = (jax.nn.silu(h_gate) * h_up).astype(BF16)
        return 0

    lax.fori_loop(0, ns, shared_up, 0)

    def shared_down(n, _):
        slot = lax.rem(n, 2)

        @pl.when(n + 1 < nd)
        def _():
            d_copy(n + 1).start()

        d_copy(n).wait()

        @pl.when(n >= 2)
        def _():
            y_copy(n - 2).wait()

        yb[slot] = dot(hs[...], wd[slot])
        y_copy(n).start()
        return 0

    lax.fori_loop(0, nd, shared_down, 0)
    y_copy(nd - 2).wait()
    y_copy(nd - 1).wait()

    row = lax.broadcasted_iota(jnp.int32, (CAP, tokens), 0).astype(F32)

    def x_copy(pos, slot):
        return pltpu.make_async_copy(x_all.at[pos], xbuf.at[slot], x_sem.at[slot])

    def gather(pos, x_ref, base):
        for e in range(per_dev):
            dbuf[e * CAP : (e + 1) * CAP, :] = jnp.where(row == tabs[pos, pl.ds(e, 1), :], 1.0, 0.0).astype(BF16)
        rows = pl.ds(pl.multiple_of(base, CAP), CAP)

        def cols_step(n, _):
            cols = pl.ds(pl.multiple_of(n * xc, xc), xc)
            got = dot(dbuf[...], x_ref[:, cols]).astype(BF16)
            xg[:, rows, cols] = got.reshape(per_dev, CAP, xc)
            return 0

        lax.fori_loop(0, width // xc, cols_step, 0)

    def a_copy(it, n_rows, base):
        cols = pl.ds(pl.multiple_of(lax.rem(it, nt) * tn, tn), tn)
        slot = lax.rem(it, 2)
        return pltpu.make_async_copy(ab.at[slot, pl.ds(0, n_rows)], act_hbm.at[it // nt, pl.ds(base, n_rows), cols], a_sem.at[slot])

    def expert_pass(first, n_rows, base):
        def body(it, _):
            t = first + it
            w_start(t + slots - 1)
            slot = w_wait(t)

            @pl.when(it >= 2)
            def _():
                a_copy(it - 2, n_rows, base).wait()

            e = it // nt
            h_gate = dot(xg[e, :n_rows], wg[slot])
            h_up = dot(xg[e, :n_rows], wu[slot])
            ab[lax.rem(it, 2), :n_rows] = (jax.nn.silu(h_gate) * h_up).astype(BF16)
            a_copy(it, n_rows, base).start()

            if base == 0:
                @pl.when(it == forward_at)
                def _():
                    arrived(2 + core)
                    sends[3].start()
                    arrived(4 + core)
                    sends[4].start()
                    sends[5].start()

            return 0

        lax.fori_loop(0, steps, body, 0)
        a_copy(steps - 2, n_rows, base).wait()
        a_copy(steps - 1, n_rows, base).wait()

    for p in range(groups):
        @pl.when(p != core)
        def _():
            pltpu.make_async_remote_copy(
                src_ref=tab_ref.at[0], dst_ref=tabs.at[p], send_sem=ts_sem.at[p], recv_sem=tr_sem.at[p],
                device_id={"ep": partner}, device_id_type=MESH).wait_recv()

    arrived(1 - core)
    x_copy(1 - core, 0).start()
    gather(core, xown, core * CAP)
    x_copy(1 - core, 0).wait()
    gather(1 - core, xbuf.at[0], (1 - core) * CAP)
    expert_pass(ns, early, 0)

    order = [2 + core, 4 + core, 3 - core, 5 - core, 6 + core, 7 - core]
    x_copy(order[0], 0).start()
    x_copy(order[1], 1).start()
    for n, pos in enumerate(order):
        x_copy(pos, n % 2).wait()
        gather(pos, xbuf.at[n % 2], (pos - 2) * CAP)
        if n + 2 < 6:
            if n + 2 == 2:
                arrived(3 - core)
            if n + 2 == 3:
                arrived(5 - core)
            if n + 2 == 5:
                arrived(7 - core)
            if n + 2 == 4:
                arrived(6 + core)
                sends[6].start()
            x_copy(order[n + 2], n % 2).start()
    expert_pass(ns + steps, late, early)

    for k in range(7):
        sends[k].wait_send()
    for r in range(4):
        for k in range(2):
            if r == 0:
                @pl.when(k != core)
                def _():
                    table_copy(r, k).wait_send()
            else:
                table_copy(r, k).wait_send()
    tabs_ref[...] = tabs[...]


def down_kernel(
    tab_ref, act_hbm, w2_hbm, ys_hbm, y_hbm,
    comb, act, part, wbuf, fsend, frecv, mine, bsend, brecv, acc, ybuf,
    act_sem, w_sem, acc_sem, y_sem, fs_sem, fr_sem, bs_sem, br_sem, credit,
):
    groups, pair, tokens = tab_ref.shape
    per_dev = pair // 2
    rows = per_dev * CAP
    cw = wbuf.shape[2]
    nc = acc.shape[0]
    steps = 4 * nc

    me, core, partner, first_core = relatives()

    def w_copy(it, slot):
        c, e = it // per_dev, lax.rem(it, per_dev)
        cols = pl.ds(pl.multiple_of(c * cw, cw), cw)
        return pltpu.make_async_copy(w2_hbm.at[e, :, cols], wbuf.at[slot], w_sem.at[slot])

    def act_copy(e):
        return pltpu.make_async_copy(act_hbm.at[e], act.at[e], act_sem.at[e])

    def acc_copy(c):
        return pltpu.make_async_copy(ys_hbm.at[:, pl.ds(c * cw, cw)], acc.at[c], acc_sem.at[c])

    w_copy(0, 0).start()
    for e in range(per_dev):
        act_copy(e).start()
    for c in range(nc):
        acc_copy(c).start()

    barrier = pltpu.get_barrier_semaphore()
    pl.semaphore_signal(barrier, inc=1, device_id={"ep": partner}, device_id_type=MESH)
    for j in range(3):
        pl.semaphore_signal(barrier, inc=1, device_id={"ep": first_core(3 - j) + core}, device_id_type=MESH)
    pl.semaphore_wait(barrier, 4)

    lane = lax.broadcasted_iota(jnp.int32, (per_dev, rows), 1)
    first = lax.broadcasted_iota(jnp.int32, (per_dev, rows), 0) * CAP
    inside = (lane >= first) & (lane < first + CAP)
    spread = jnp.where(inside, 1.0, 0.0).astype(BF16)
    want = jnp.sum(jnp.where(inside, lane - first, 0).astype(F32), axis=0, keepdims=True)

    def over_slots(v):
        return lax.dot_general(v, spread, (((0,), (0,)), ((), ())), preferred_element_type=F32)

    def build(s, _):
        hit = over_slots(tab_ref[s, :per_dev, :].astype(BF16)) == want
        gate = tab_ref[s, per_dev:, :]
        hi = gate.astype(BF16)
        rest = gate - hi.astype(F32)
        mid = rest.astype(BF16)
        low = (rest - mid.astype(F32)).astype(BF16)
        for k, piece in enumerate((hi, mid, low)):
            comb[k, s] = jnp.where(hit, over_slots(piece), 0.0).astype(BF16)
        return 0

    lax.fori_loop(0, groups, build, 0)
    for c in range(nc):
        acc_copy(c).wait()

    def f_copy(slot):
        return pltpu.make_async_remote_copy(
            src_ref=fsend.at[slot], dst_ref=frecv.at[slot], send_sem=fs_sem.at[slot], recv_sem=fr_sem.at[slot],
            device_id={"ep": partner}, device_id_type=MESH)

    def b_copy(j, c):
        slot = lax.rem(c, 2)
        return pltpu.make_async_remote_copy(
            src_ref=bsend.at[j, slot], dst_ref=brecv.at[j, c], send_sem=bs_sem.at[j, slot], recv_sem=br_sem.at[j, c],
            device_id={"ep": first_core(3 - j) + core}, device_id_type=MESH)

    def combine(s):
        return dot(comb[0, s], part[s]) + dot(comb[1, s], part[s]) + dot(comb[2, s], part[s])

    def launch(h):
        j = lax.rem(h, 4)

        @pl.when(j < 3)
        def _():
            b_copy(j, h // 4).start()

    def consume(h):
        slot, c, j = lax.rem(h, 2), h // 4, lax.rem(h, 4)
        f_copy(slot).wait_recv()

        @pl.when(j < 3)
        def _():
            @pl.when(c >= 2)
            def _():
                b_copy(j, c - 2).wait_send()

            bsend[j, lax.rem(c, 2)] = (mine[slot] + frecv[slot]).astype(BF16)

        @pl.when(j == 3)
        def _():
            acc[c] = acc[c] + (mine[slot] + frecv[slot])

        @pl.when(h + 2 < steps)
        def _():
            pl.semaphore_signal(credit, inc=1, device_id={"ep": partner}, device_id_type=MESH)

    def chunk(c, _):
        def down(e, _):
            it = c * per_dev + e
            slot = lax.rem(it, 2)

            @pl.when(it + 1 < nc * per_dev)
            def _():
                w_copy(it + 1, 1 - slot).start()

            w_copy(it, slot).wait()

            @pl.when(c == 0)
            def _():
                act_copy(e).wait()

            got = dot(act[e], wbuf[slot]).astype(BF16)
            part[:, pl.ds(pl.multiple_of(e * CAP, CAP), CAP), :] = got.reshape(groups, CAP, cw)
            return 0

        lax.fori_loop(0, per_dev, down, 0)

        def pair_step(j, _):
            g = 4 * c + j
            slot = lax.rem(g, 2)
            p = 2 * (3 - j)

            @pl.when(g >= 2)
            def _():
                f_copy(slot).wait_send()

            fsend[slot] = combine(p + 1 - core)
            mine[slot] = combine(p + core)

            @pl.when(g >= 2)
            def _():
                pl.semaphore_wait(credit, 1)

            f_copy(slot).start()

            @pl.when(g >= 2)
            def _():
                launch(g - 2)

            @pl.when(g >= 1)
            def _():
                consume(g - 1)

            return 0

        lax.fori_loop(0, 4, pair_step, 0)
        return 0

    lax.fori_loop(0, nc, chunk, 0)
    launch(steps - 2)
    consume(steps - 1)
    f_copy(0).wait_send()
    f_copy(1).wait_send()

    def y_copy(c):
        return pltpu.make_async_copy(ybuf.at[c % 2], y_hbm.at[:, pl.ds(c * cw, cw)], y_sem.at[c % 2])

    for c in range(nc):
        for j in range(3):
            b_copy(j, c).wait_recv()
            if c >= nc - 2:
                b_copy(j, c).wait_send()
        if c >= 2:
            y_copy(c - 2).wait()
        total = acc[c]
        for j in range(3):
            total = total + brecv[j, c].astype(F32)
        ybuf[c % 2] = total.astype(BF16)
        y_copy(c).start()
    y_copy(nc - 2).wait()
    y_copy(nc - 1).wait()


def solution(mesh):
    groups = mesh.shape["ep"]
    tok_spec = P(("dp", "ep"), None)
    bank_spec = P("ep", None, None)
    vmem = pl.BlockSpec(memory_space=pltpu.VMEM)
    hbm = pl.BlockSpec(memory_space=pl.ANY)

    def device_fn(hidden, w_router, w_gate, w_up, w_down, shared_gate, shared_up, shared_down, top_idx, keep_mask):
        tokens, width = hidden.shape
        per_dev, _, ff = w_gate.shape
        rows = groups * CAP
        tn, cw = 256, 256
        nc = width // cw
        tab = pl.pallas_call(
            route_kernel,
            out_shape=jax.ShapeDtypeStruct((groups, 2 * per_dev, tokens), F32),
            in_specs=[vmem] * 4,
            out_specs=vmem,
            name="route",
        )(hidden, w_router, top_idx.T, keep_mask.T)
        sff = shared_gate.shape[1]
        slots = 4
        tabs, shared, act, _ = pl.pallas_call(
            up_kernel,
            out_shape=(
                jax.ShapeDtypeStruct(tab.shape, F32),
                jax.ShapeDtypeStruct((tokens, width), F32),
                jax.ShapeDtypeStruct((per_dev, rows, ff), BF16),
                jax.ShapeDtypeStruct((groups, tokens, width), BF16),
            ),
            in_specs=[vmem] + [hbm] * 6,
            out_specs=(vmem, hbm, hbm, hbm),
            scratch_shapes=[
                pltpu.VMEM(tab.shape, F32),
                pltpu.VMEM((tokens, width), BF16),
                pltpu.VMEM((2, tokens, width), BF16),
                pltpu.VMEM((per_dev, rows - 2 * CAP, width), BF16),
                pltpu.VMEM((per_dev * CAP, tokens), BF16),
                pltpu.VMEM((slots, width, tn), BF16),
                pltpu.VMEM((slots, width, tn), BF16),
                pltpu.VMEM((2, sff, tn), BF16),
                pltpu.VMEM((tokens, sff), BF16),
                pltpu.VMEM((2, rows - 2 * CAP, tn), BF16),
                pltpu.VMEM((2, tokens, tn), F32),
                pltpu.SemaphoreType.DMA,
                pltpu.SemaphoreType.DMA((2,)),
                pltpu.SemaphoreType.DMA((2, slots)),
                pltpu.SemaphoreType.DMA((2,)),
                pltpu.SemaphoreType.DMA((2,)),
                pltpu.SemaphoreType.DMA((2,)),
                pltpu.SemaphoreType.DMA((groups,)),
                pltpu.SemaphoreType.DMA((groups,)),
                pltpu.SemaphoreType.DMA((7,)),
                pltpu.SemaphoreType.DMA((groups,)),
            ],
            compiler_params=pltpu.CompilerParams(vmem_limit_bytes=VMEM_BYTES, collective_id=1, has_side_effects=True),
            name="up",
        )(tab, hidden, w_gate, w_up, shared_gate, shared_up, shared_down)
        return pl.pallas_call(
            down_kernel,
            out_shape=jax.ShapeDtypeStruct((tokens, width), BF16),
            in_specs=[vmem, hbm, hbm, hbm],
            out_specs=hbm,
            scratch_shapes=[
                pltpu.VMEM((3, groups, tokens, per_dev * CAP), BF16),
                pltpu.VMEM((per_dev, rows, ff), BF16),
                pltpu.VMEM((groups, per_dev * CAP, cw), BF16),
                pltpu.VMEM((2, ff, cw), BF16),
                pltpu.VMEM((2, tokens, cw), F32),
                pltpu.VMEM((2, tokens, cw), F32),
                pltpu.VMEM((2, tokens, cw), F32),
                pltpu.VMEM((3, 2, tokens, cw), BF16),
                pltpu.VMEM((3, nc, tokens, cw), BF16),
                pltpu.VMEM((nc, tokens, cw), F32),
                pltpu.VMEM((2, tokens, cw), BF16),
                pltpu.SemaphoreType.DMA((per_dev,)),
                pltpu.SemaphoreType.DMA((2,)),
                pltpu.SemaphoreType.DMA((nc,)),
                pltpu.SemaphoreType.DMA((2,)),
                pltpu.SemaphoreType.DMA((2,)),
                pltpu.SemaphoreType.DMA((2,)),
                pltpu.SemaphoreType.DMA((3, 2)),
                pltpu.SemaphoreType.DMA((3, nc)),
                pltpu.SemaphoreType.REGULAR,
            ],
            compiler_params=pltpu.CompilerParams(vmem_limit_bytes=VMEM_BYTES, collective_id=0, has_side_effects=True),
            cost_estimate=pl.CostEstimate(flops=8 * per_dev * rows * width * ff, bytes_accessed=2 * per_dev * width * ff, transcendentals=0),
            name="down",
        )(tabs, act, w_down, shared)

    return jax.shard_map(device_fn, mesh=mesh, in_specs=(tok_spec, P(), bank_spec, bank_spec, bank_spec, P(), P(), P(), tok_spec, tok_spec), out_specs=tok_spec, check_vma=False)
```

```python
import functools

import jax
import jax.numpy as jnp
from jax import lax
from jax.experimental import pallas as pl
from jax.experimental.pallas import tpu as pltpu
from jax.sharding import PartitionSpec as P

ROUTE_SCALE = 16.0
CAP = 96
VMEM_BYTES = 66_900_000
MESH = pl.DeviceIdType.MESH
F32 = jnp.float32
BF16 = jnp.bfloat16


def dot(a, b):
    return jnp.dot(a, b, preferred_element_type=F32)


def route_kernel(x_ref, w_ref, idx_ref, keep_ref, tab_ref):
    experts, tokens = w_ref.shape[0], x_ref.shape[0]
    logits = lax.dot_general(w_ref[...], x_ref[...], (((1,), (1,)), ((), ())), preferred_element_type=F32)
    e = jnp.exp(logits - jnp.max(logits, axis=0, keepdims=True))
    prob = e / jnp.sum(e, axis=0, keepdims=True)
    expert_id = lax.broadcasted_iota(jnp.int32, (experts, tokens), 0)
    member = jnp.zeros((experts, tokens), F32)
    for k in range(idx_ref.shape[0]):
        hit = (expert_id == idx_ref[k : k + 1, :]) & (keep_ref[k : k + 1, :] > 0)
        member = jnp.where(hit, 1.0, member)
    earlier = lax.broadcasted_iota(jnp.int32, (tokens, tokens), 0) < lax.broadcasted_iota(jnp.int32, (tokens, tokens), 1)
    rank = dot(member.astype(BF16), jnp.where(earlier, 1.0, 0.0).astype(BF16))
    slot = jnp.where(member > 0, rank, -1.0)
    gate = ROUTE_SCALE * prob * member
    half = tab_ref.shape[1] // 2
    for d in range(tab_ref.shape[0]):
        tab_ref[d, :half, :] = slot[d * half : (d + 1) * half]
        tab_ref[d, half:, :] = gate[d * half : (d + 1) * half]


def relatives():
    me = lax.axis_index("ep")
    core, chip = lax.rem(me, 2), me // 2
    yb, xb = chip // 2, lax.rem(chip, 2)

    def first_core(r):
        return 2 * (2 * lax.rem(yb + r // 2, 2) + lax.rem(xb + lax.rem(r, 2), 2))

    return me, core, me + 1 - 2 * core, first_core


def up_kernel(
    tab_ref, x_hbm, w1_hbm, w3_hbm, sg_hbm, su_hbm, sd_hbm, tabs_ref, ys_hbm, act_hbm, x_all,
    tabs, xown, xbuf, xg, dbuf, wg, wu, wd, hs, hg, hu, ab, yb,
    own_sem, x_sem, w_sem, d_sem, a_sem, y_sem, ts_sem, tr_sem, xs_sem, xr_sem,
):
    groups = tabs.shape[0]
    tokens, width = x_hbm.shape
    per_dev, _, ff = w1_hbm.shape
    slots, _, tn = wg.shape
    nt, ns, nd = ff // tn, sg_hbm.shape[1] // tn, width // tn
    steps = per_dev * nt
    xc = width // 2
    early = 2 * CAP
    late = groups * CAP - early
    forward_at = steps // 2

    me, core, partner, first_core = relatives()

    def block_copy(k, src, pos, device):
        return pltpu.make_async_remote_copy(
            src_ref=src, dst_ref=x_all.at[pos], send_sem=xs_sem.at[k], recv_sem=xr_sem.at[pos],
            device_id={"ep": device}, device_id_type=MESH)

    def table_copy(r, k):
        dst = first_core(r) + k
        return pltpu.make_async_remote_copy(
            src_ref=tab_ref.at[dst], dst_ref=tabs.at[2 * r + core], send_sem=ts_sem.at[2 * r + k], recv_sem=tr_sem.at[2 * r + core],
            device_id={"ep": dst}, device_id_type=MESH)

    sends = [
        block_copy(0, x_hbm, core, partner),
        block_copy(1, x_hbm, 2 + core, first_core(1) + core),
        block_copy(2, x_hbm, 4 + core, first_core(2) + core),
        block_copy(3, x_all.at[2 + core], 2 + core, partner),
        block_copy(4, x_all.at[4 + core], 4 + core, partner),
        block_copy(5, x_all.at[4 - core], 6 + core, first_core(1 + core) + core),
        block_copy(6, x_all.at[6 + core], 6 + core, partner),
    ]

    def arrived(pos):
        block_copy(0, x_hbm, pos, partner).wait_recv()

    def w_start(t):
        slot = lax.rem(t, slots)

        def go(a, b):
            pltpu.make_async_copy(a, wg.at[slot], w_sem.at[0, slot]).start()
            pltpu.make_async_copy(b, wu.at[slot], w_sem.at[1, slot]).start()

        @pl.when(t < ns)
        def _():
            cols = pl.ds(pl.multiple_of(t * tn, tn), tn)
            go(sg_hbm.at[:, cols], su_hbm.at[:, cols])

        @pl.when((t >= ns) & (t < ns + 2 * steps))
        def _():
            it = lax.rem(t - ns, steps)
            cols = pl.ds(pl.multiple_of(lax.rem(it, nt) * tn, tn), tn)
            go(w1_hbm.at[it // nt, :, cols], w3_hbm.at[it // nt, :, cols])

    def w_wait(t):
        slot = lax.rem(t, slots)
        pltpu.make_async_copy(sg_hbm.at[:, pl.ds(0, tn)], wg.at[slot], w_sem.at[0, slot]).wait()
        pltpu.make_async_copy(sg_hbm.at[:, pl.ds(0, tn)], wu.at[slot], w_sem.at[1, slot]).wait()
        return slot

    def d_copy(n):
        cols = pl.ds(pl.multiple_of(n * tn, tn), tn)
        return pltpu.make_async_copy(sd_hbm.at[:, cols], wd.at[lax.rem(n, 3)], d_sem.at[lax.rem(n, 3)])

    def y_copy(n):
        cols = pl.ds(pl.multiple_of(n * tn, tn), tn)
        return pltpu.make_async_copy(yb.at[lax.rem(n, 2)], ys_hbm.at[:, cols], y_sem.at[lax.rem(n, 2)])

    own_copy = pltpu.make_async_copy(x_hbm, xown, own_sem)
    own_copy.start()
    for t in range(slots - 1):
        w_start(t)
    d_copy(0).start()
    d_copy(1).start()

    barrier = pltpu.get_barrier_semaphore()
    for d in range(1, groups):
        pl.semaphore_signal(barrier, inc=1, device_id={"ep": lax.rem(me + d, groups)}, device_id_type=MESH)
    pl.semaphore_wait(barrier, groups - 1)
    for r in range(4):
        for k in range(2):
            if r == 0:
                @pl.when(k != core)
                def _():
                    table_copy(r, k).start()
            else:
                table_copy(r, k).start()
    for k in range(3):
        sends[k].start()
    tabs[core] = tab_ref[me]
    own_copy.wait()

    def gated_pass(first, n_steps, n_rows, lhs, before, after):
        def activate(h):
            return (jax.nn.silu(hg[h, :n_rows]) * hu[h, :n_rows]).astype(BF16)

        def body(i, _):
            for h in range(2):
                it = 2 * i + h
                w_start(first + it + slots - 1)
                slot = w_wait(first + it)
                last = it - 1
                before(last)
                ab[1 - h, :n_rows] = activate(1 - h)
                x = lhs(it)
                hg[h, :n_rows] = dot(x, wg[slot])
                hu[h, :n_rows] = dot(x, wu[slot])
                after(last)
            return 0

        lax.fori_loop(0, n_steps // 2, body, 0)
        before(n_steps - 1)
        ab[1, :n_rows] = activate(1)
        after(n_steps - 1)

    def s_copy(it):
        cols = pl.ds(pl.multiple_of(it * tn, tn), tn)
        return ab.at[lax.rem(it, 2), pl.ds(0, tokens)], hs.at[:, cols]

    def shared_after(it):
        @pl.when(it >= 0)
        def _():
            src, dst = s_copy(it)
            dst[...] = src[...]

    hg[...] = jnp.zeros_like(hg)
    hu[...] = jnp.zeros_like(hu)
    gated_pass(0, ns, tokens, lambda it: xown[...], lambda it: None, shared_after)

    def shared_down(n, _):
        slot = lax.rem(n, 2)

        @pl.when(n + 2 < nd)
        def _():
            d_copy(n + 2).start()

        d_copy(n).wait()

        @pl.when(n >= 2)
        def _():
            y_copy(n - 2).wait()

        yb[slot] = dot(hs[...], wd[lax.rem(n, 3)])
        y_copy(n).start()
        return 0

    lax.fori_loop(0, nd, shared_down, 0)
    y_copy(nd - 2).wait()
    y_copy(nd - 1).wait()

    row = lax.broadcasted_iota(jnp.int32, (CAP, tokens), 0).astype(F32)

    def x_copy(pos, slot):
        return pltpu.make_async_copy(x_all.at[pos], xbuf.at[slot], x_sem.at[slot])

    def gather(pos, x_ref, base):
        for e in range(per_dev):
            dbuf[e * CAP : (e + 1) * CAP, :] = jnp.where(row == tabs[pos, pl.ds(e, 1), :], 1.0, 0.0).astype(BF16)
        rows = pl.ds(pl.multiple_of(base, CAP), CAP)

        def cols_step(n, _):
            cols = pl.ds(pl.multiple_of(n * xc, xc), xc)
            got = dot(dbuf[...], x_ref[:, cols]).astype(BF16)
            xg[:, rows, cols] = got.reshape(per_dev, CAP, xc)
            return 0

        lax.fori_loop(0, width // xc, cols_step, 0)

    def a_copy(it, n_rows, base):
        cols = pl.ds(pl.multiple_of(lax.rem(it, nt) * tn, tn), tn)
        slot = lax.rem(it, 2)
        return pltpu.make_async_copy(ab.at[slot, pl.ds(0, n_rows)], act_hbm.at[it // nt, pl.ds(base, n_rows), cols], a_sem.at[slot])

    def expert_pass(first, n_rows, base):
        def before(it):
            @pl.when(it >= 2)
            def _():
                a_copy(it - 2, n_rows, base).wait()

        def after(it):
            @pl.when(it >= 0)
            def _():
                a_copy(it, n_rows, base).start()

            if base == 0:
                @pl.when(it == forward_at)
                def _():
                    arrived(2 + core)
                    sends[3].start()
                    arrived(4 + core)
                    sends[4].start()
                    sends[5].start()

        gated_pass(first, steps, n_rows, lambda it: xg[it // nt, :n_rows], before, after)
        a_copy(steps - 2, n_rows, base).wait()
        a_copy(steps - 1, n_rows, base).wait()

    for p in range(groups):
        @pl.when(p != core)
        def _():
            pltpu.make_async_remote_copy(
                src_ref=tab_ref.at[0], dst_ref=tabs.at[p], send_sem=ts_sem.at[p], recv_sem=tr_sem.at[p],
                device_id={"ep": partner}, device_id_type=MESH).wait_recv()

    arrived(1 - core)
    x_copy(1 - core, 0).start()
    gather(core, xown, core * CAP)
    x_copy(1 - core, 0).wait()
    gather(1 - core, xbuf.at[0], (1 - core) * CAP)
    expert_pass(ns, early, 0)

    order = [2 + core, 4 + core, 3 - core, 5 - core, 6 + core, 7 - core]
    x_copy(order[0], 0).start()
    x_copy(order[1], 1).start()
    for n, pos in enumerate(order):
        x_copy(pos, n % 2).wait()
        gather(pos, xbuf.at[n % 2], (pos - 2) * CAP)
        if n + 2 < 6:
            if n + 2 == 2:
                arrived(3 - core)
            if n + 2 == 3:
                arrived(5 - core)
            if n + 2 == 5:
                arrived(7 - core)
            if n + 2 == 4:
                arrived(6 + core)
                sends[6].start()
            x_copy(order[n + 2], n % 2).start()
    expert_pass(ns + steps, late, early)

    for k in range(7):
        sends[k].wait_send()
    for r in range(4):
        for k in range(2):
            if r == 0:
                @pl.when(k != core)
                def _():
                    table_copy(r, k).wait_send()
            else:
                table_copy(r, k).wait_send()
    tabs_ref[...] = tabs[...]


def down_kernel(
    tab_ref, act_hbm, w2_hbm, ys_hbm, y_hbm,
    comb, act, part, wbuf, fsend, frecv, mine, bsend, brecv, acc, ybuf,
    act_sem, w_sem, acc_sem, y_sem, fs_sem, fr_sem, bs_sem, br_sem, credit,
):
    groups, pair, tokens = tab_ref.shape
    per_dev = pair // 2
    rows = per_dev * CAP
    cw = wbuf.shape[2]
    nc = acc.shape[0]
    steps = 4 * nc

    me, core, partner, first_core = relatives()

    def w_copy(it):
        slot = lax.rem(it, 4)
        c, e = it // per_dev, lax.rem(it, per_dev)
        cols = pl.ds(pl.multiple_of(c * cw, cw), cw)
        return pltpu.make_async_copy(w2_hbm.at[e, :, cols], wbuf.at[slot], w_sem.at[slot])

    def act_copy(e):
        return pltpu.make_async_copy(act_hbm.at[e], act.at[e], act_sem.at[e])

    def acc_copy(c):
        return pltpu.make_async_copy(ys_hbm.at[:, pl.ds(c * cw, cw)], acc.at[c], acc_sem.at[c])

    for it in range(2):
        w_copy(it).start()
    for e in range(per_dev):
        act_copy(e).start()
    for c in range(nc):
        acc_copy(c).start()

    barrier = pltpu.get_barrier_semaphore()
    pl.semaphore_signal(barrier, inc=1, device_id={"ep": partner}, device_id_type=MESH)
    for j in range(3):
        pl.semaphore_signal(barrier, inc=1, device_id={"ep": first_core(3 - j) + core}, device_id_type=MESH)
    pl.semaphore_wait(barrier, 4)

    lane = lax.broadcasted_iota(jnp.int32, (per_dev, rows), 1)
    first = lax.broadcasted_iota(jnp.int32, (per_dev, rows), 0) * CAP
    inside = (lane >= first) & (lane < first + CAP)
    spread = jnp.where(inside, 1.0, 0.0).astype(BF16)
    want = jnp.sum(jnp.where(inside, lane - first, 0).astype(F32), axis=0, keepdims=True)

    def over_slots(v):
        return lax.dot_general(v, spread, (((0,), (0,)), ((), ())), preferred_element_type=F32)

    def build(s):
        hit = over_slots(tab_ref[s, :per_dev, :].astype(BF16)) == want
        gate = tab_ref[s, per_dev:, :]
        hi = gate.astype(BF16)
        rest = gate - hi.astype(F32)
        mid = rest.astype(BF16)
        low = (rest - mid.astype(F32)).astype(BF16)
        for k, piece in enumerate((hi, mid, low)):
            comb[s, k * tokens : (k + 1) * tokens] = jnp.where(hit, over_slots(piece), 0.0).astype(BF16)

    for c in range(nc):
        acc_copy(c).wait()

    def f_copy(slot):
        return pltpu.make_async_remote_copy(
            src_ref=fsend.at[slot], dst_ref=frecv.at[slot], send_sem=fs_sem.at[slot], recv_sem=fr_sem.at[slot],
            device_id={"ep": partner}, device_id_type=MESH)

    def b_copy(j, c):
        slot = lax.rem(c, 2)
        return pltpu.make_async_remote_copy(
            src_ref=bsend.at[j, slot], dst_ref=brecv.at[j, c], send_sem=bs_sem.at[j, slot], recv_sem=br_sem.at[j, c],
            device_id={"ep": first_core(3 - j) + core}, device_id_type=MESH)

    def combine(s):
        pieces = dot(comb[s], part[s])
        return pieces[:tokens] + pieces[tokens : 2 * tokens] + pieces[2 * tokens :]

    def launch(h):
        j = lax.rem(h, 4)

        @pl.when(j < 3)
        def _():
            b_copy(j, h // 4).start()

    def consume(h):
        slot, c, j = lax.rem(h, 3), h // 4, lax.rem(h, 4)
        f_copy(slot).wait_recv()

        @pl.when(j < 3)
        def _():
            @pl.when(c >= 2)
            def _():
                b_copy(j, c - 2).wait_send()

            bsend[j, lax.rem(c, 2)] = (mine[slot] + frecv[slot]).astype(BF16)

        @pl.when(j == 3)
        def _():
            acc[c] = acc[c] + (mine[slot] + frecv[slot])

        @pl.when(h + 3 < steps)
        def _():
            pl.semaphore_signal(credit, inc=1, device_id={"ep": partner}, device_id_type=MESH)

    def chunk(c, _):
        def down(i, _):
            for h in range(2):
                it = c * per_dev + 2 * i + h

                @pl.when(it + 2 < nc * per_dev)
                def _():
                    w_copy(it + 2).start()

                @pl.when(c == 0)
                def _():
                    act_copy(2 * i + h).wait()

            for h in range(2):
                w_copy(c * per_dev + 2 * i + h).wait()
            got = []
            for h in range(2):
                it = c * per_dev + 2 * i + h
                got.append(dot(act[2 * i + h], wbuf[lax.rem(it, 4)]).astype(BF16))
            for h in range(2):
                part[:, pl.ds(pl.multiple_of((2 * i + h) * CAP, CAP), CAP), :] = got[h].reshape(groups, CAP, cw)
            return 0

        lax.fori_loop(0, per_dev // 2, down, 0)

        def pair_step(j, _):
            g = 4 * c + j
            slot = lax.rem(g, 3)
            p = 2 * (3 - j)

            @pl.when(c == 0)
            def _():
                build(p)
                build(p + 1)

            @pl.when(g >= 3)
            def _():
                f_copy(slot).wait_send()

            fsend[slot] = combine(p + 1 - core)
            mine[slot] = combine(p + core)

            @pl.when(g >= 3)
            def _():
                pl.semaphore_wait(credit, 1)

            f_copy(slot).start()

            @pl.when(g >= 3)
            def _():
                launch(g - 3)

            @pl.when(g >= 2)
            def _():
                consume(g - 2)

            return 0

        lax.fori_loop(0, 4, pair_step, 0)
        return 0

    lax.fori_loop(0, nc, chunk, 0)
    launch(steps - 3)
    consume(steps - 2)
    launch(steps - 2)
    consume(steps - 1)
    for slot in range(3):
        f_copy(slot).wait_send()

    def y_copy(c):
        return pltpu.make_async_copy(ybuf.at[c % 2], y_hbm.at[:, pl.ds(c * cw, cw)], y_sem.at[c % 2])

    for c in range(nc):
        for j in range(3):
            b_copy(j, c).wait_recv()
            if c >= nc - 2:
                b_copy(j, c).wait_send()
        if c >= 2:
            y_copy(c - 2).wait()
        total = acc[c]
        for j in range(3):
            total = total + brecv[j, c].astype(F32)
        ybuf[c % 2] = total.astype(BF16)
        y_copy(c).start()
    y_copy(nc - 2).wait()
    y_copy(nc - 1).wait()


def solution(mesh):
    groups = mesh.shape["ep"]
    tok_spec = P(("dp", "ep"), None)
    bank_spec = P("ep", None, None)
    vmem = pl.BlockSpec(memory_space=pltpu.VMEM)
    hbm = pl.BlockSpec(memory_space=pl.ANY)

    def device_fn(hidden, w_router, w_gate, w_up, w_down, shared_gate, shared_up, shared_down, top_idx, keep_mask):
        tokens, width = hidden.shape
        per_dev, _, ff = w_gate.shape
        rows = groups * CAP
        tn, cw = 256, 256
        nc = width // cw
        tab = pl.pallas_call(
            route_kernel,
            out_shape=jax.ShapeDtypeStruct((groups, 2 * per_dev, tokens), F32),
            in_specs=[vmem] * 4,
            out_specs=vmem,
            name="route",
        )(hidden, w_router.T, top_idx.T, keep_mask.T)
        sff = shared_gate.shape[1]
        slots = 4
        tabs, shared, act, _ = pl.pallas_call(
            up_kernel,
            out_shape=(
                jax.ShapeDtypeStruct(tab.shape, F32),
                jax.ShapeDtypeStruct((tokens, width), F32),
                jax.ShapeDtypeStruct((per_dev, rows, ff), BF16),
                jax.ShapeDtypeStruct((groups, tokens, width), BF16),
            ),
            in_specs=[vmem] + [hbm] * 6,
            out_specs=(vmem, hbm, hbm, hbm),
            scratch_shapes=[
                pltpu.VMEM(tab.shape, F32),
                pltpu.VMEM((tokens, width), BF16),
                pltpu.VMEM((2, tokens, width), BF16),
                pltpu.VMEM((per_dev, rows - 2 * CAP, width), BF16),
                pltpu.VMEM((per_dev * CAP, tokens), BF16),
                pltpu.VMEM((slots, width, tn), BF16),
                pltpu.VMEM((slots, width, tn), BF16),
                pltpu.VMEM((3, sff, tn), BF16),
                pltpu.VMEM((tokens, sff), BF16),
                pltpu.VMEM((2, rows - 2 * CAP, tn), F32),
                pltpu.VMEM((2, rows - 2 * CAP, tn), F32),
                pltpu.VMEM((2, rows - 2 * CAP, tn), BF16),
                pltpu.VMEM((2, tokens, tn), F32),
                pltpu.SemaphoreType.DMA,
                pltpu.SemaphoreType.DMA((2,)),
                pltpu.SemaphoreType.DMA((2, slots)),
                pltpu.SemaphoreType.DMA((3,)),
                pltpu.SemaphoreType.DMA((2,)),
                pltpu.SemaphoreType.DMA((2,)),
                pltpu.SemaphoreType.DMA((groups,)),
                pltpu.SemaphoreType.DMA((groups,)),
                pltpu.SemaphoreType.DMA((7,)),
                pltpu.SemaphoreType.DMA((groups,)),
            ],
            compiler_params=pltpu.CompilerParams(vmem_limit_bytes=VMEM_BYTES, collective_id=1, has_side_effects=True),
            name="up",
        )(tab, hidden, w_gate, w_up, shared_gate, shared_up, shared_down)
        return pl.pallas_call(
            down_kernel,
            out_shape=jax.ShapeDtypeStruct((tokens, width), BF16),
            in_specs=[vmem, hbm, hbm, hbm],
            out_specs=hbm,
            scratch_shapes=[
                pltpu.VMEM((groups, 3 * tokens, per_dev * CAP), BF16),
                pltpu.VMEM((per_dev, rows, ff), BF16),
                pltpu.VMEM((groups, per_dev * CAP, cw), BF16),
                pltpu.VMEM((4, ff, cw), BF16),
                pltpu.VMEM((3, tokens, cw), F32),
                pltpu.VMEM((3, tokens, cw), F32),
                pltpu.VMEM((3, tokens, cw), F32),
                pltpu.VMEM((3, 2, tokens, cw), BF16),
                pltpu.VMEM((3, nc, tokens, cw), BF16),
                pltpu.VMEM((nc, tokens, cw), F32),
                pltpu.VMEM((2, tokens, cw), BF16),
                pltpu.SemaphoreType.DMA((per_dev,)),
                pltpu.SemaphoreType.DMA((4,)),
                pltpu.SemaphoreType.DMA((nc,)),
                pltpu.SemaphoreType.DMA((2,)),
                pltpu.SemaphoreType.DMA((3,)),
                pltpu.SemaphoreType.DMA((3,)),
                pltpu.SemaphoreType.DMA((3, 2)),
                pltpu.SemaphoreType.DMA((3, nc)),
                pltpu.SemaphoreType.REGULAR,
            ],
            compiler_params=pltpu.CompilerParams(vmem_limit_bytes=VMEM_BYTES, collective_id=0, has_side_effects=True),
            cost_estimate=pl.CostEstimate(flops=8 * per_dev * rows * width * ff, bytes_accessed=2 * per_dev * width * ff, transcendentals=0),
            name="down",
        )(tabs, act, w_down, shared)

    return jax.shard_map(device_fn, mesh=mesh, in_specs=(tok_spec, P(), bank_spec, bank_spec, bank_spec, P(), P(), P(), tok_spec, tok_spec), out_specs=tok_spec, check_vma=False)
```

```python
import functools

import jax
import jax.numpy as jnp
from jax import lax
from jax.experimental import pallas as pl
from jax.experimental.pallas import tpu as pltpu
from jax.sharding import PartitionSpec as P

ROUTE_SCALE = 16.0
CAP = 96
VMEM_BYTES = 66_900_000
MESH = pl.DeviceIdType.MESH
F32 = jnp.float32
BF16 = jnp.bfloat16


def dot(a, b):
    return jnp.dot(a, b, preferred_element_type=F32)


def route(x, w, idx_ref, keep_ref, tab_ref):
    experts, tokens = w.shape[0], x.shape[0]
    logits = lax.dot_general(w, x, (((1,), (1,)), ((), ())), preferred_element_type=F32)
    e = jnp.exp(logits - jnp.max(logits, axis=0, keepdims=True))
    prob = e / jnp.sum(e, axis=0, keepdims=True)
    expert_id = lax.broadcasted_iota(jnp.int32, (experts, tokens), 0)
    member = jnp.zeros((experts, tokens), F32)
    for k in range(idx_ref.shape[0]):
        hit = (expert_id == idx_ref[k : k + 1, :]) & (keep_ref[k : k + 1, :] > 0)
        member = jnp.where(hit, 1.0, member)
    earlier = lax.broadcasted_iota(jnp.int32, (tokens, tokens), 0) < lax.broadcasted_iota(jnp.int32, (tokens, tokens), 1)
    rank = dot(member.astype(BF16), jnp.where(earlier, 1.0, 0.0).astype(BF16))
    slot = jnp.where(member > 0, rank, -1.0)
    gate = ROUTE_SCALE * prob * member
    half = tab_ref.shape[1] // 2
    for d in range(tab_ref.shape[0]):
        tab_ref[d, :half, :] = slot[d * half : (d + 1) * half]
        tab_ref[d, half:, :] = gate[d * half : (d + 1) * half]


def relatives():
    me = lax.axis_index("ep")
    core, chip = lax.rem(me, 2), me // 2
    yb, xb = chip // 2, lax.rem(chip, 2)

    def first_core(r):
        return 2 * (2 * lax.rem(yb + r // 2, 2) + lax.rem(xb + lax.rem(r, 2), 2))

    return me, core, me + 1 - 2 * core, first_core


def up_kernel(
    wr_ref, idx_ref, keep_ref, x_hbm, w1_hbm, w3_hbm, sg_hbm, su_hbm, sd_hbm, comb_hbm, ys_hbm, act_hbm, x_all,
    tab_ref, tabs, cbuf, xown, xbuf, xg, dbuf, wg, wu, wd, hs, hg, hu, ab, yb,
    own_sem, x_sem, w_sem, d_sem, a_sem, y_sem, c_sem, ts_sem, tr_sem, xs_sem, xr_sem,
):
    groups = tabs.shape[0]
    tokens, width = x_hbm.shape
    per_dev, _, ff = w1_hbm.shape
    slots, _, tn = wg.shape
    nt, ns, nd = ff // tn, sg_hbm.shape[1] // tn, width // tn
    steps = per_dev * nt
    xc = width // 2
    early = 2 * CAP
    late = groups * CAP - early
    forward_at = 5 * steps // 8

    me, core, partner, first_core = relatives()

    def block_copy(k, src, pos, device):
        return pltpu.make_async_remote_copy(
            src_ref=src, dst_ref=x_all.at[pos], send_sem=xs_sem.at[k], recv_sem=xr_sem.at[pos],
            device_id={"ep": device}, device_id_type=MESH)

    def table_copy(r, k):
        dst = first_core(r) + k
        return pltpu.make_async_remote_copy(
            src_ref=tab_ref.at[dst], dst_ref=tabs.at[2 * r + core], send_sem=ts_sem.at[2 * r + k], recv_sem=tr_sem.at[2 * r + core],
            device_id={"ep": dst}, device_id_type=MESH)

    sends = [
        block_copy(0, x_hbm, core, partner),
        block_copy(1, x_hbm, 2 + core, first_core(1) + core),
        block_copy(2, x_hbm, 4 + core, first_core(2) + core),
        block_copy(3, x_all.at[2 + core], 2 + core, partner),
        block_copy(4, x_all.at[4 + core], 4 + core, partner),
        block_copy(5, x_all.at[4 - core], 6 + core, first_core(1 + core) + core),
        block_copy(6, x_all.at[6 + core], 6 + core, partner),
    ]

    def arrived(pos):
        block_copy(0, x_hbm, pos, partner).wait_recv()

    def w_start(t):
        slot = lax.rem(t, slots)

        def go(a, b):
            pltpu.make_async_copy(a, wg.at[slot], w_sem.at[0, slot]).start()
            pltpu.make_async_copy(b, wu.at[slot], w_sem.at[1, slot]).start()

        @pl.when(t < ns)
        def _():
            cols = pl.ds(pl.multiple_of(t * tn, tn), tn)
            go(sg_hbm.at[:, cols], su_hbm.at[:, cols])

        @pl.when((t >= ns) & (t < ns + 2 * steps))
        def _():
            it = lax.rem(t - ns, steps)
            cols = pl.ds(pl.multiple_of(lax.rem(it, nt) * tn, tn), tn)
            go(w1_hbm.at[it // nt, :, cols], w3_hbm.at[it // nt, :, cols])

    def w_wait(t):
        slot = lax.rem(t, slots)
        pltpu.make_async_copy(sg_hbm.at[:, pl.ds(0, tn)], wg.at[slot], w_sem.at[0, slot]).wait()
        pltpu.make_async_copy(sg_hbm.at[:, pl.ds(0, tn)], wu.at[slot], w_sem.at[1, slot]).wait()
        return slot

    def d_copy(n):
        cols = pl.ds(pl.multiple_of(n * tn, tn), tn)
        return pltpu.make_async_copy(sd_hbm.at[:, cols], wd.at[lax.rem(n, 3)], d_sem.at[lax.rem(n, 3)])

    def y_copy(n):
        cols = pl.ds(pl.multiple_of(n * tn, tn), tn)
        return pltpu.make_async_copy(yb.at[lax.rem(n, 2)], ys_hbm.at[:, cols], y_sem.at[lax.rem(n, 2)])

    own_copy = pltpu.make_async_copy(x_hbm, xown, own_sem)
    own_copy.start()
    for t in range(slots - 1):
        w_start(t)
    d_copy(0).start()
    d_copy(1).start()

    barrier = pltpu.get_barrier_semaphore()
    for d in range(1, groups):
        pl.semaphore_signal(barrier, inc=1, device_id={"ep": lax.rem(me + d, groups)}, device_id_type=MESH)
    own_copy.wait()
    route(xown[...], wr_ref[...], idx_ref, keep_ref, tab_ref)
    pl.semaphore_wait(barrier, groups - 1)
    for r in range(4):
        for k in range(2):
            if r == 0:
                @pl.when(k != core)
                def _():
                    table_copy(r, k).start()
            else:
                table_copy(r, k).start()
    for k in range(3):
        sends[k].start()
    tabs[core] = tab_ref[me]

    def gated_pass(first, n_steps, n_rows, lhs, before, after):
        def activate(h):
            return (jax.nn.silu(hg[h, :n_rows]) * hu[h, :n_rows]).astype(BF16)

        def body(i, _):
            for h in range(2):
                it = 2 * i + h
                w_start(first + it + slots - 1)
                slot = w_wait(first + it)
                last = it - 1
                before(last)
                ab[1 - h, :n_rows] = activate(1 - h)
                x = lhs(it)
                hg[h, :n_rows] = dot(x, wg[slot])
                hu[h, :n_rows] = dot(x, wu[slot])
                after(last)
            return 0

        lax.fori_loop(0, n_steps // 2, body, 0)
        before(n_steps - 1)
        ab[1, :n_rows] = activate(1)
        after(n_steps - 1)

    def s_copy(it):
        cols = pl.ds(pl.multiple_of(it * tn, tn), tn)
        return ab.at[lax.rem(it, 2), pl.ds(0, tokens)], hs.at[:, cols]

    def shared_after(it):
        @pl.when(it >= 0)
        def _():
            src, dst = s_copy(it)
            dst[...] = src[...]

    hg[...] = jnp.zeros_like(hg)
    hu[...] = jnp.zeros_like(hu)
    gated_pass(0, ns, tokens, lambda it: xown[...], lambda it: None, shared_after)

    def shared_down(n, _):
        slot = lax.rem(n, 2)

        @pl.when(n + 2 < nd)
        def _():
            d_copy(n + 2).start()

        d_copy(n).wait()

        @pl.when(n >= 2)
        def _():
            y_copy(n - 2).wait()

        yb[slot] = dot(hs[...], wd[lax.rem(n, 3)])
        y_copy(n).start()
        return 0

    lax.fori_loop(0, nd, shared_down, 0)
    y_copy(nd - 2).wait()
    y_copy(nd - 1).wait()

    row = lax.broadcasted_iota(jnp.int32, (CAP, tokens), 0).astype(F32)

    def x_copy(pos, slot):
        return pltpu.make_async_copy(x_all.at[pos], xbuf.at[slot], x_sem.at[slot])

    def gather(pos, x_ref, base):
        for e in range(per_dev):
            dbuf[e * CAP : (e + 1) * CAP, :] = jnp.where(row == tabs[pos, pl.ds(e, 1), :], 1.0, 0.0).astype(BF16)
        rows = pl.ds(pl.multiple_of(base, CAP), CAP)

        def cols_step(n, _):
            cols = pl.ds(pl.multiple_of(n * xc, xc), xc)
            got = dot(dbuf[...], x_ref[:, cols]).astype(BF16)
            xg[:, rows, cols] = got.reshape(per_dev, CAP, xc)
            return 0

        lax.fori_loop(0, width // xc, cols_step, 0)

    def a_copy(it, n_rows, base):
        cols = pl.ds(pl.multiple_of(lax.rem(it, nt) * tn, tn), tn)
        slot = lax.rem(it, 2)
        return pltpu.make_async_copy(ab.at[slot, pl.ds(0, n_rows)], act_hbm.at[it // nt, pl.ds(base, n_rows), cols], a_sem.at[slot])

    def expert_pass(first, n_rows, base):
        def before(it):
            @pl.when(it >= 2)
            def _():
                a_copy(it - 2, n_rows, base).wait()

        def after(it):
            @pl.when(it >= 0)
            def _():
                a_copy(it, n_rows, base).start()

            if base == 0:
                @pl.when(it == forward_at)
                def _():
                    arrived(2 + core)
                    sends[3].start()
                    arrived(4 + core)
                    sends[4].start()
                    sends[5].start()
                    x_copy(2 + core, 0).start()
                    x_copy(4 + core, 1).start()

        gated_pass(first, steps, n_rows, lambda it: xg[it // nt, :n_rows], before, after)
        a_copy(steps - 2, n_rows, base).wait()
        a_copy(steps - 1, n_rows, base).wait()

    for p in range(groups):
        @pl.when(p != core)
        def _():
            pltpu.make_async_remote_copy(
                src_ref=tab_ref.at[0], dst_ref=tabs.at[p], send_sem=ts_sem.at[p], recv_sem=tr_sem.at[p],
                device_id={"ep": partner}, device_id_type=MESH).wait_recv()

    arrived(1 - core)
    x_copy(1 - core, 0).start()
    gather(core, xown, core * CAP)
    x_copy(1 - core, 0).wait()
    gather(1 - core, xbuf.at[0], (1 - core) * CAP)
    expert_pass(ns, early, 0)

    n_slots = per_dev * CAP
    lane = lax.broadcasted_iota(jnp.int32, (per_dev, n_slots), 1)
    lead = lax.broadcasted_iota(jnp.int32, (per_dev, n_slots), 0) * CAP
    inside = (lane >= lead) & (lane < lead + CAP)
    spread = jnp.where(inside, 1.0, 0.0).astype(BF16)
    want = jnp.sum(jnp.where(inside, lane - lead, 0).astype(F32), axis=0, keepdims=True)

    def over_slots(v):
        return lax.dot_general(v, spread, (((0,), (0,)), ((), ())), preferred_element_type=F32)

    def c_copy(p):
        return pltpu.make_async_copy(cbuf.at[lax.rem(p, 2)], comb_hbm.at[p], c_sem.at[lax.rem(p, 2)])

    def build(p, _):
        @pl.when(p >= 2)
        def _():
            c_copy(p - 2).wait()

        hit = over_slots(tabs[p, :per_dev, :].astype(BF16)) == want
        gate = tabs[p, per_dev:, :]
        hi = gate.astype(BF16)
        rest = gate - hi.astype(F32)
        mid = rest.astype(BF16)
        low = (rest - mid.astype(F32)).astype(BF16)
        for k, piece in enumerate((hi, mid, low)):
            cbuf[lax.rem(p, 2), k * tokens : (k + 1) * tokens] = jnp.where(hit, over_slots(piece), 0.0).astype(BF16)
        c_copy(p).start()
        return 0

    order = [2 + core, 4 + core, 3 - core, 5 - core, 6 + core, 7 - core]
    for n, pos in enumerate(order):
        x_copy(pos, n % 2).wait()
        gather(pos, xbuf.at[n % 2], (pos - 2) * CAP)
        if n + 2 < 6:
            if n + 2 == 2:
                arrived(3 - core)
            if n + 2 == 3:
                arrived(5 - core)
            if n + 2 < 4:
                x_copy(order[n + 2], n % 2).start()
        if n == 3:
            lax.fori_loop(0, groups, build, 0)
            arrived(6 + core)
            sends[6].start()
            x_copy(order[4], 0).start()
            arrived(7 - core)
            x_copy(order[5], 1).start()
    expert_pass(ns + steps, late, early)

    c_copy(groups - 2).wait()
    c_copy(groups - 1).wait()
    for k in range(7):
        sends[k].wait_send()
    for r in range(4):
        for k in range(2):
            if r == 0:
                @pl.when(k != core)
                def _():
                    table_copy(r, k).wait_send()
            else:
                table_copy(r, k).wait_send()


def down_kernel(
    comb_hbm, act_hbm, w2_hbm, ys_hbm, y_hbm,
    comb, act, part, wbuf, fsend, frecv, mine, bsend, brecv, acc, ybuf,
    act_sem, w_sem, comb_sem, acc_sem, y_sem, fs_sem, fr_sem, bs_sem, br_sem, credit,
):
    groups, per_dev, tokens = comb_hbm.shape[0], w2_hbm.shape[0], y_hbm.shape[0]
    cw = wbuf.shape[2]
    nc = acc.shape[0]
    steps = 4 * nc

    me, core, partner, first_core = relatives()

    def w_copy(it):
        slot = lax.rem(it, 4)
        c, e = it // per_dev, lax.rem(it, per_dev)
        cols = pl.ds(pl.multiple_of(c * cw, cw), cw)
        return pltpu.make_async_copy(w2_hbm.at[e, :, cols], wbuf.at[slot], w_sem.at[slot])

    def act_copy(e):
        return pltpu.make_async_copy(act_hbm.at[e], act.at[e], act_sem.at[e])

    def comb_copy(p):
        return pltpu.make_async_copy(comb_hbm.at[p], comb.at[p], comb_sem.at[p])

    def acc_copy(c):
        return pltpu.make_async_copy(ys_hbm.at[:, pl.ds(pl.multiple_of(c * cw, cw), cw)], acc.at[c], acc_sem.at[c])

    for it in range(2):
        w_copy(it).start()
    for e in range(per_dev):
        act_copy(e).start()
    for p in reversed(range(groups)):
        comb_copy(p).start()
    for c in range(nc):
        acc_copy(c).start()

    barrier = pltpu.get_barrier_semaphore()
    pl.semaphore_signal(barrier, inc=1, device_id={"ep": partner}, device_id_type=MESH)
    for j in range(3):
        pl.semaphore_signal(barrier, inc=1, device_id={"ep": first_core(3 - j) + core}, device_id_type=MESH)
    pl.semaphore_wait(barrier, 4)

    def f_copy(slot):
        return pltpu.make_async_remote_copy(
            src_ref=fsend.at[slot], dst_ref=frecv.at[slot], send_sem=fs_sem.at[slot], recv_sem=fr_sem.at[slot],
            device_id={"ep": partner}, device_id_type=MESH)

    def b_copy(j, c):
        slot = lax.rem(c, 2)
        return pltpu.make_async_remote_copy(
            src_ref=bsend.at[j, slot], dst_ref=brecv.at[j, c], send_sem=bs_sem.at[j, slot], recv_sem=br_sem.at[j, c],
            device_id={"ep": first_core(3 - j) + core}, device_id_type=MESH)

    def combine(s):
        pieces = dot(comb[s], part[s])
        return pieces[:tokens] + pieces[tokens : 2 * tokens] + pieces[2 * tokens :]

    def launch(h):
        j = lax.rem(h, 4)

        @pl.when(j < 3)
        def _():
            b_copy(j, h // 4).start()

    def consume(h):
        slot, c, j = lax.rem(h, 3), h // 4, lax.rem(h, 4)
        f_copy(slot).wait_recv()

        @pl.when(j < 3)
        def _():
            @pl.when(c >= 2)
            def _():
                b_copy(j, c - 2).wait_send()

            bsend[j, lax.rem(c, 2)] = (mine[slot] + frecv[slot]).astype(BF16)

        @pl.when(j == 3)
        def _():
            acc_copy(c).wait()
            acc[c] = acc[c] + (mine[slot] + frecv[slot])

        @pl.when(h + 3 < steps)
        def _():
            pl.semaphore_signal(credit, inc=1, device_id={"ep": partner}, device_id_type=MESH)

    def chunk(c, _):
        def down(i, _):
            for h in range(2):
                it = c * per_dev + 2 * i + h

                @pl.when(it + 2 < nc * per_dev)
                def _():
                    w_copy(it + 2).start()

                @pl.when(c == 0)
                def _():
                    act_copy(2 * i + h).wait()

            for h in range(2):
                w_copy(c * per_dev + 2 * i + h).wait()
            got = []
            for h in range(2):
                it = c * per_dev + 2 * i + h
                got.append(dot(act[2 * i + h], wbuf[lax.rem(it, 4)]).astype(BF16))
            for h in range(2):
                part[:, pl.ds(pl.multiple_of((2 * i + h) * CAP, CAP), CAP), :] = got[h].reshape(groups, CAP, cw)
            return 0

        lax.fori_loop(0, per_dev // 2, down, 0)

        def pair_step(j, _):
            g = 4 * c + j
            slot = lax.rem(g, 3)
            p = 2 * (3 - j)

            @pl.when(c == 0)
            def _():
                comb_copy(p).wait()
                comb_copy(p + 1).wait()

            @pl.when(g >= 3)
            def _():
                f_copy(slot).wait_send()

            fsend[slot] = combine(p + 1 - core)
            mine[slot] = combine(p + core)

            @pl.when(g >= 3)
            def _():
                pl.semaphore_wait(credit, 1)

            f_copy(slot).start()

            @pl.when(g >= 2)
            def _():
                launch(g - 2)

            @pl.when(g >= 1)
            def _():
                consume(g - 1)

            return 0

        lax.fori_loop(0, 4, pair_step, 0)
        return 0

    lax.fori_loop(0, nc, chunk, 0)
    launch(steps - 2)
    consume(steps - 1)
    for slot in range(3):
        f_copy(slot).wait_send()

    def y_copy(c):
        return pltpu.make_async_copy(ybuf.at[c % 2], y_hbm.at[:, pl.ds(c * cw, cw)], y_sem.at[c % 2])

    for c in range(nc):
        for j in range(3):
            b_copy(j, c).wait_recv()
            if c >= nc - 2:
                b_copy(j, c).wait_send()
        if c >= 2:
            y_copy(c - 2).wait()
        total = acc[c]
        for j in range(3):
            total = total + brecv[j, c].astype(F32)
        ybuf[c % 2] = total.astype(BF16)
        y_copy(c).start()
    y_copy(nc - 2).wait()
    y_copy(nc - 1).wait()


def solution(mesh):
    groups = mesh.shape["ep"]
    tok_spec = P(("dp", "ep"), None)
    bank_spec = P("ep", None, None)
    vmem = pl.BlockSpec(memory_space=pltpu.VMEM)
    hbm = pl.BlockSpec(memory_space=pl.ANY)

    def device_fn(hidden, w_router, w_gate, w_up, w_down, shared_gate, shared_up, shared_down, top_idx, keep_mask):
        tokens, width = hidden.shape
        per_dev, _, ff = w_gate.shape
        rows = groups * CAP
        tn, cw = 256, 256
        nc = width // cw
        sff = shared_gate.shape[1]
        slots = 4
        table = (groups, 2 * per_dev, tokens)
        comb, shared, act, _ = pl.pallas_call(
            up_kernel,
            out_shape=(
                jax.ShapeDtypeStruct((groups, 3 * tokens, per_dev * CAP), BF16),
                jax.ShapeDtypeStruct((tokens, width), F32),
                jax.ShapeDtypeStruct((per_dev, rows, ff), BF16),
                jax.ShapeDtypeStruct((groups, tokens, width), BF16),
            ),
            in_specs=[vmem] * 3 + [hbm] * 6,
            out_specs=(hbm,) * 4,
            scratch_shapes=[
                pltpu.VMEM(table, F32),
                pltpu.VMEM(table, F32),
                pltpu.VMEM((2, 3 * tokens, per_dev * CAP), BF16),
                pltpu.VMEM((tokens, width), BF16),
                pltpu.VMEM((2, tokens, width), BF16),
                pltpu.VMEM((per_dev, rows - 2 * CAP, width), BF16),
                pltpu.VMEM((per_dev * CAP, tokens), BF16),
                pltpu.VMEM((slots, width, tn), BF16),
                pltpu.VMEM((slots, width, tn), BF16),
                pltpu.VMEM((3, sff, tn), BF16),
                pltpu.VMEM((tokens, sff), BF16),
                pltpu.VMEM((2, rows - 2 * CAP, tn), F32),
                pltpu.VMEM((2, rows - 2 * CAP, tn), F32),
                pltpu.VMEM((2, rows - 2 * CAP, tn), BF16),
                pltpu.VMEM((2, tokens, tn), F32),
                pltpu.SemaphoreType.DMA,
                pltpu.SemaphoreType.DMA((2,)),
                pltpu.SemaphoreType.DMA((2, slots)),
                pltpu.SemaphoreType.DMA((3,)),
                pltpu.SemaphoreType.DMA((2,)),
                pltpu.SemaphoreType.DMA((2,)),
                pltpu.SemaphoreType.DMA((2,)),
                pltpu.SemaphoreType.DMA((groups,)),
                pltpu.SemaphoreType.DMA((groups,)),
                pltpu.SemaphoreType.DMA((7,)),
                pltpu.SemaphoreType.DMA((groups,)),
            ],
            compiler_params=pltpu.CompilerParams(vmem_limit_bytes=VMEM_BYTES, collective_id=1, has_side_effects=True),
            name="up",
        )(w_router.T, top_idx.T, keep_mask.T, hidden, w_gate, w_up, shared_gate, shared_up, shared_down)
        return pl.pallas_call(
            down_kernel,
            out_shape=jax.ShapeDtypeStruct((tokens, width), BF16),
            in_specs=[hbm] * 4,
            out_specs=hbm,
            scratch_shapes=[
                pltpu.VMEM((groups, 3 * tokens, per_dev * CAP), BF16),
                pltpu.VMEM((per_dev, rows, ff), BF16),
                pltpu.VMEM((groups, per_dev * CAP, cw), BF16),
                pltpu.VMEM((4, ff, cw), BF16),
                pltpu.VMEM((3, tokens, cw), F32),
                pltpu.VMEM((3, tokens, cw), F32),
                pltpu.VMEM((3, tokens, cw), F32),
                pltpu.VMEM((3, 2, tokens, cw), BF16),
                pltpu.VMEM((3, nc, tokens, cw), BF16),
                pltpu.VMEM((nc, tokens, cw), F32),
                pltpu.VMEM((2, tokens, cw), BF16),
                pltpu.SemaphoreType.DMA((per_dev,)),
                pltpu.SemaphoreType.DMA((4,)),
                pltpu.SemaphoreType.DMA((groups,)),
                pltpu.SemaphoreType.DMA((nc,)),
                pltpu.SemaphoreType.DMA((2,)),
                pltpu.SemaphoreType.DMA((3,)),
                pltpu.SemaphoreType.DMA((3,)),
                pltpu.SemaphoreType.DMA((3, 2)),
                pltpu.SemaphoreType.DMA((3, nc)),
                pltpu.SemaphoreType.REGULAR,
            ],
            compiler_params=pltpu.CompilerParams(vmem_limit_bytes=VMEM_BYTES, collective_id=0, has_side_effects=True),
            cost_estimate=pl.CostEstimate(flops=8 * per_dev * rows * width * ff, bytes_accessed=2 * per_dev * width * ff, transcendentals=0),
            name="down",
        )(comb, act, w_down, shared)

    return jax.shard_map(device_fn, mesh=mesh, in_specs=(tok_spec, P(), bank_spec, bank_spec, bank_spec, P(), P(), P(), tok_spec, tok_spec), out_specs=tok_spec, check_vma=False)
```

```python
import functools

import jax
import jax.numpy as jnp
from jax import lax
from jax.experimental import pallas as pl
from jax.experimental.pallas import tpu as pltpu
from jax.sharding import PartitionSpec as P

ROUTE_SCALE = 16.0
CAP = 96
VMEM_BYTES = 66_900_000
MESH = pl.DeviceIdType.MESH
F32 = jnp.float32
BF16 = jnp.bfloat16


def dot(a, b):
    return jnp.dot(a, b, preferred_element_type=F32)


def route(x, w, idx_ref, keep_ref, tab_ref):
    experts, tokens = w.shape[0], x.shape[0]
    logits = lax.dot_general(w, x, (((1,), (1,)), ((), ())), preferred_element_type=F32)
    e = jnp.exp(logits - jnp.max(logits, axis=0, keepdims=True))
    prob = e / jnp.sum(e, axis=0, keepdims=True)
    expert_id = lax.broadcasted_iota(jnp.int32, (experts, tokens), 0)
    member = jnp.zeros((experts, tokens), F32)
    for k in range(idx_ref.shape[0]):
        hit = (expert_id == idx_ref[k : k + 1, :]) & (keep_ref[k : k + 1, :] > 0)
        member = jnp.where(hit, 1.0, member)
    earlier = lax.broadcasted_iota(jnp.int32, (tokens, tokens), 0) < lax.broadcasted_iota(jnp.int32, (tokens, tokens), 1)
    rank = dot(member.astype(BF16), jnp.where(earlier, 1.0, 0.0).astype(BF16))
    slot = jnp.where(member > 0, rank, -1.0)
    gate = ROUTE_SCALE * prob * member
    half = tab_ref.shape[1] // 2
    for d in range(tab_ref.shape[0]):
        tab_ref[d, :half, :] = slot[d * half : (d + 1) * half]
        tab_ref[d, half:, :] = gate[d * half : (d + 1) * half]


def relatives():
    me = lax.axis_index("ep")
    core, chip = lax.rem(me, 2), me // 2
    yb, xb = chip // 2, lax.rem(chip, 2)

    def first_core(r):
        return 2 * (2 * lax.rem(yb + r // 2, 2) + lax.rem(xb + lax.rem(r, 2), 2))

    return me, core, me + 1 - 2 * core, first_core


def up_kernel(
    wr_ref, idx_ref, keep_ref, x_hbm, w1_hbm, w3_hbm, sg_hbm, su_hbm, comb_hbm, hs_hbm, act_hbm, x_all,
    tab_ref, tabs, cbuf, xown, xbuf, xg, dbuf, wg, wu, hs, hg, hu, ab,
    own_sem, x_sem, w_sem, a_sem, hs_sem, c_sem, ts_sem, tr_sem, xs_sem, xr_sem,
):
    groups = tabs.shape[0]
    tokens, width = x_hbm.shape
    per_dev, _, ff = w1_hbm.shape
    slots, _, tn = wg.shape
    nt, ns = ff // tn, sg_hbm.shape[1] // tn
    steps = per_dev * nt
    xc = width // 2
    early = 2 * CAP
    late = groups * CAP - early
    forward_at = 7 * steps // 8
    near = late - 2 * CAP
    ahead = 2 * nt

    me, core, partner, first_core = relatives()

    def block_copy(k, src, pos, device):
        return pltpu.make_async_remote_copy(
            src_ref=src, dst_ref=x_all.at[pos], send_sem=xs_sem.at[k], recv_sem=xr_sem.at[pos],
            device_id={"ep": device}, device_id_type=MESH)

    def table_copy(r, k):
        dst = first_core(r) + k
        return pltpu.make_async_remote_copy(
            src_ref=tab_ref.at[dst], dst_ref=tabs.at[2 * r + core], send_sem=ts_sem.at[2 * r + k], recv_sem=tr_sem.at[2 * r + core],
            device_id={"ep": dst}, device_id_type=MESH)

    sends = [
        block_copy(0, x_hbm, core, partner),
        block_copy(1, x_hbm, 2 + core, first_core(1) + core),
        block_copy(2, x_hbm, 4 + core, first_core(2) + core),
        block_copy(3, x_all.at[2 + core], 2 + core, partner),
        block_copy(4, x_all.at[4 + core], 4 + core, partner),
        block_copy(5, x_all.at[4 - core], 6 + core, first_core(1 + core) + core),
        block_copy(6, x_all.at[6 + core], 6 + core, partner),
    ]

    def arrived(pos):
        block_copy(0, x_hbm, pos, partner).wait_recv()

    def w_start(t):
        slot = lax.rem(t, slots)

        def go(a, b):
            pltpu.make_async_copy(a, wg.at[slot], w_sem.at[0, slot]).start()
            pltpu.make_async_copy(b, wu.at[slot], w_sem.at[1, slot]).start()

        @pl.when(t < ns)
        def _():
            cols = pl.ds(pl.multiple_of(t * tn, tn), tn)
            go(sg_hbm.at[:, cols], su_hbm.at[:, cols])

        for begin, n_tiles in ((ns, steps), (ns + steps, ahead), (ns + steps + ahead, steps)):
            @pl.when((t >= begin) & (t < begin + n_tiles))
            def _():
                it = t - begin
                cols = pl.ds(pl.multiple_of(lax.rem(it, nt) * tn, tn), tn)
                go(w1_hbm.at[it // nt, :, cols], w3_hbm.at[it // nt, :, cols])

    def w_wait(t):
        slot = lax.rem(t, slots)
        pltpu.make_async_copy(sg_hbm.at[:, pl.ds(0, tn)], wg.at[slot], w_sem.at[0, slot]).wait()
        pltpu.make_async_copy(sg_hbm.at[:, pl.ds(0, tn)], wu.at[slot], w_sem.at[1, slot]).wait()
        return slot

    own_copy = pltpu.make_async_copy(x_hbm, xown, own_sem)
    own_copy.start()
    for t in range(slots - 1):
        w_start(t)

    barrier = pltpu.get_barrier_semaphore()
    for d in range(1, groups):
        pl.semaphore_signal(barrier, inc=1, device_id={"ep": lax.rem(me + d, groups)}, device_id_type=MESH)
    own_copy.wait()
    route(xown[...], wr_ref[...], idx_ref, keep_ref, tab_ref)
    pl.semaphore_wait(barrier, groups - 1)
    for r in range(4):
        for k in range(2):
            if r == 0:
                @pl.when(k != core)
                def _():
                    table_copy(r, k).start()
            else:
                table_copy(r, k).start()
    for k in range(3):
        sends[k].start()
    tabs[core] = tab_ref[me]

    def gated_pass(first, n_steps, n_rows, lhs, before, after):
        def activate(h):
            return (jax.nn.silu(hg[h, :n_rows]) * hu[h, :n_rows]).astype(BF16)

        def body(i, _):
            for h in range(2):
                it = 2 * i + h
                w_start(first + it + slots - 1)
                slot = w_wait(first + it)
                last = it - 1
                before(last)
                ab[1 - h, :n_rows] = activate(1 - h)
                x = lhs(it)
                hg[h, :n_rows] = dot(x, wg[slot])
                hu[h, :n_rows] = dot(x, wu[slot])
                after(last)
            return 0

        lax.fori_loop(0, n_steps // 2, body, 0)
        before(n_steps - 1)
        ab[1, :n_rows] = activate(1)
        after(n_steps - 1)

    def s_copy(it):
        cols = pl.ds(pl.multiple_of(it * tn, tn), tn)
        return ab.at[lax.rem(it, 2), pl.ds(0, tokens)], hs.at[:, cols]

    def shared_after(it):
        @pl.when(it >= 0)
        def _():
            src, dst = s_copy(it)
            dst[...] = src[...]

    hg[...] = jnp.zeros_like(hg)
    hu[...] = jnp.zeros_like(hu)
    gated_pass(0, ns, tokens, lambda it: xown[...], lambda it: None, shared_after)

    hs_copy = pltpu.make_async_copy(hs, hs_hbm, hs_sem)
    hs_copy.start()

    row = lax.broadcasted_iota(jnp.int32, (CAP, tokens), 0).astype(F32)

    def x_copy(pos, slot):
        return pltpu.make_async_copy(x_all.at[pos], xbuf.at[slot], x_sem.at[slot])

    def gather(pos, x_ref, base):
        for e in range(per_dev):
            dbuf[e * CAP : (e + 1) * CAP, :] = jnp.where(row == tabs[pos, pl.ds(e, 1), :], 1.0, 0.0).astype(BF16)
        rows = pl.ds(pl.multiple_of(base, CAP), CAP)

        def cols_step(n, _):
            cols = pl.ds(pl.multiple_of(n * xc, xc), xc)
            got = dot(dbuf[...], x_ref[:, cols]).astype(BF16)
            xg[:, rows, cols] = got.reshape(per_dev, CAP, xc)
            return 0

        lax.fori_loop(0, width // xc, cols_step, 0)

    def a_copy(it, n_rows, base):
        cols = pl.ds(pl.multiple_of(lax.rem(it, nt) * tn, tn), tn)
        slot = lax.rem(it, 2)
        return pltpu.make_async_copy(ab.at[slot, pl.ds(0, n_rows)], act_hbm.at[it // nt, pl.ds(base, n_rows), cols], a_sem.at[slot])

    def expert_pass(first, tile0, n_tiles, n_rows, row0, base):
        def before(k):
            @pl.when(k >= 2)
            def _():
                a_copy(tile0 + k - 2, n_rows, base).wait()

        def after(k):
            @pl.when(k >= 0)
            def _():
                a_copy(tile0 + k, n_rows, base).start()

            if base == 0:
                @pl.when(k == forward_at)
                def _():
                    arrived(2 + core)
                    sends[3].start()
                    arrived(4 + core)
                    sends[4].start()
                    sends[5].start()
                    x_copy(2 + core, 0).start()
                    x_copy(4 + core, 1).start()

        def lhs(k):
            return xg[(tile0 + k) // nt, row0 : row0 + n_rows]

        gated_pass(first, n_tiles, n_rows, lhs, before, after)
        a_copy(tile0 + n_tiles - 2, n_rows, base).wait()
        a_copy(tile0 + n_tiles - 1, n_rows, base).wait()

    for p in range(groups):
        @pl.when(p != core)
        def _():
            pltpu.make_async_remote_copy(
                src_ref=tab_ref.at[0], dst_ref=tabs.at[p], send_sem=ts_sem.at[p], recv_sem=tr_sem.at[p],
                device_id={"ep": partner}, device_id_type=MESH).wait_recv()

    arrived(1 - core)
    x_copy(1 - core, 0).start()
    gather(core, xown, core * CAP)
    x_copy(1 - core, 0).wait()
    gather(1 - core, xbuf.at[0], (1 - core) * CAP)
    expert_pass(ns, 0, steps, early, 0, 0)

    n_slots = per_dev * CAP
    lane = lax.broadcasted_iota(jnp.int32, (per_dev, n_slots), 1)
    lead = lax.broadcasted_iota(jnp.int32, (per_dev, n_slots), 0) * CAP
    inside = (lane >= lead) & (lane < lead + CAP)
    spread = jnp.where(inside, 1.0, 0.0).astype(BF16)
    want = jnp.sum(jnp.where(inside, lane - lead, 0).astype(F32), axis=0, keepdims=True)

    def over_slots(v):
        return lax.dot_general(v, spread, (((0,), (0,)), ((), ())), preferred_element_type=F32)

    def c_copy(p):
        return pltpu.make_async_copy(cbuf.at[lax.rem(p, 2)], comb_hbm.at[p], c_sem.at[lax.rem(p, 2)])

    def build(p, _):
        @pl.when(p >= 2)
        def _():
            c_copy(p - 2).wait()

        hit = over_slots(tabs[p, :per_dev, :].astype(BF16)) == want
        gate = tabs[p, per_dev:, :]
        hi = gate.astype(BF16)
        rest = gate - hi.astype(F32)
        mid = rest.astype(BF16)
        low = (rest - mid.astype(F32)).astype(BF16)
        for k, piece in enumerate((hi, mid, low)):
            cbuf[lax.rem(p, 2), k * tokens : (k + 1) * tokens] = jnp.where(hit, over_slots(piece), 0.0).astype(BF16)
        c_copy(p).start()
        return 0

    order = [2 + core, 4 + core, 3 - core, 5 - core, 6 + core, 7 - core]
    for n, pos in enumerate(order):
        x_copy(pos, n % 2).wait()
        gather(pos, xbuf.at[n % 2], (pos - 2) * CAP)
        if n + 2 < 6:
            if n + 2 == 2:
                arrived(3 - core)
            if n + 2 == 3:
                arrived(5 - core)
            if n + 2 < 4:
                x_copy(order[n + 2], n % 2).start()
        if n == 3:
            lax.fori_loop(0, groups, build, 0)
            expert_pass(ns + steps, 0, ahead, near, 0, early)
            arrived(6 + core)
            sends[6].start()
            x_copy(order[4], 0).start()
            arrived(7 - core)
            x_copy(order[5], 1).start()
    expert_pass(ns + steps + ahead, 0, ahead, late - near, near, early + near)
    expert_pass(ns + steps + 2 * ahead, ahead, steps - ahead, late, 0, early)

    hs_copy.wait()
    c_copy(groups - 2).wait()
    c_copy(groups - 1).wait()
    for k in range(7):
        sends[k].wait_send()
    for r in range(4):
        for k in range(2):
            if r == 0:
                @pl.when(k != core)
                def _():
                    table_copy(r, k).wait_send()
            else:
                table_copy(r, k).wait_send()


def down_kernel(
    comb_hbm, act_hbm, w2_hbm, hs_hbm, sd_hbm, y_hbm, through,
    comb, act, part, wbuf, fsend, frecv, mine, bsend, brecv, acc, ybuf,
    act_sem, w_sem, comb_sem, hs_sem, y_sem, fs_sem, fr_sem, bs_sem, br_sem, ts_sem, tr_sem, credit,
):
    groups, per_dev, tokens = comb_hbm.shape[0], w2_hbm.shape[0], y_hbm.shape[0]
    cw = wbuf.shape[2]
    nc = acc.shape[0]
    steps = 4 * nc

    me, core, partner, first_core = relatives()

    def w_copy(it):
        slot = lax.rem(it, 4)
        c, e = it // per_dev, lax.rem(it, per_dev)
        cols = pl.ds(pl.multiple_of(c * cw, cw), cw)
        return pltpu.make_async_copy(w2_hbm.at[e, :, cols], wbuf.at[slot], w_sem.at[slot])

    def act_copy(e):
        return pltpu.make_async_copy(act_hbm.at[e], act.at[e], act_sem.at[e])

    def comb_copy(p):
        return pltpu.make_async_copy(comb_hbm.at[p], comb.at[p], comb_sem.at[p])

    ff = act.shape[2]

    def hs_copy(h):
        return pltpu.make_async_copy(hs_hbm.at[:, pl.ds(h * ff, ff)], act.at[h, pl.ds(0, tokens)], hs_sem.at[h])

    def sd_copy(c, h):
        cols = pl.ds(pl.multiple_of(c * cw, cw), cw)
        slot = 2 * lax.rem(c, 2) + h
        return pltpu.make_async_copy(sd_hbm.at[pl.ds(h * ff, ff), cols], wbuf.at[slot], w_sem.at[slot])

    for it in range(2):
        w_copy(it).start()
    for e in range(per_dev):
        act_copy(e).start()
    for p in reversed(range(groups)):
        comb_copy(p).start()

    barrier = pltpu.get_barrier_semaphore()
    pl.semaphore_signal(barrier, inc=1, device_id={"ep": partner}, device_id_type=MESH)
    for j in range(3):
        pl.semaphore_signal(barrier, inc=1, device_id={"ep": first_core(3 - j) + core}, device_id_type=MESH)
    pl.semaphore_wait(barrier, 4)

    def f_copy(slot):
        return pltpu.make_async_remote_copy(
            src_ref=fsend.at[slot], dst_ref=frecv.at[slot], send_sem=fs_sem.at[slot], recv_sem=fr_sem.at[slot],
            device_id={"ep": partner}, device_id_type=MESH)

    def b_copy(j, c):
        slot = lax.rem(c, 2)
        return pltpu.make_async_remote_copy(
            src_ref=bsend.at[j, slot], dst_ref=brecv.at[j, c], send_sem=bs_sem.at[j, slot], recv_sem=br_sem.at[j, c],
            device_id={"ep": first_core(3 - j) + core}, device_id_type=MESH)

    def t_copy(c):
        slot = lax.rem(c, 2)
        return pltpu.make_async_remote_copy(
            src_ref=bsend.at[0, slot], dst_ref=through.at[c], send_sem=bs_sem.at[0, slot], recv_sem=tr_sem.at[c],
            device_id={"ep": first_core(1 + core) + core}, device_id_type=MESH)

    def pass_on(c):
        slot = lax.rem(c, 2)
        return pltpu.make_async_remote_copy(
            src_ref=through.at[c], dst_ref=brecv.at[0, c], send_sem=ts_sem.at[slot], recv_sem=br_sem.at[0, c],
            device_id={"ep": first_core(2 - core) + core}, device_id_type=MESH)

    def relay(c):
        @pl.when(c >= 2)
        def _():
            pass_on(c - 2).wait_send()

        t_copy(c).wait_recv()
        pass_on(c).start()

    def combine(s):
        pieces = dot(comb[s], part[s])
        return pieces[:tokens] + pieces[tokens : 2 * tokens] + pieces[2 * tokens :]

    def launch(h):
        j = lax.rem(h, 4)

        @pl.when(j == 0)
        def _():
            t_copy(h // 4).start()

        @pl.when((j > 0) & (j < 3))
        def _():
            b_copy(j, h // 4).start()

    def consume(h):
        slot, c, j = lax.rem(h, 3), h // 4, lax.rem(h, 4)
        f_copy(slot).wait_recv()

        @pl.when(j < 3)
        def _():
            @pl.when(c >= 2)
            def _():
                b_copy(j, c - 2).wait_send()

            bsend[j, lax.rem(c, 2)] = (mine[slot] + frecv[slot]).astype(BF16)

        @pl.when(j == 3)
        def _():
            acc[c] = mine[slot] + frecv[slot]

        @pl.when(h + 3 < steps)
        def _():
            pl.semaphore_signal(credit, inc=1, device_id={"ep": partner}, device_id_type=MESH)

    def chunk(c, _):
        def down(i, _):
            for h in range(2):
                it = c * per_dev + 2 * i + h

                @pl.when(it + 2 < nc * per_dev)
                def _():
                    w_copy(it + 2).start()

                @pl.when(c == 0)
                def _():
                    act_copy(2 * i + h).wait()

            for h in range(2):
                w_copy(c * per_dev + 2 * i + h).wait()
            got = []
            for h in range(2):
                it = c * per_dev + 2 * i + h
                got.append(dot(act[2 * i + h], wbuf[lax.rem(it, 4)]).astype(BF16))
            for h in range(2):
                part[:, pl.ds(pl.multiple_of((2 * i + h) * CAP, CAP), CAP), :] = got[h].reshape(groups, CAP, cw)
            return 0

        lax.fori_loop(0, per_dev // 2, down, 0)

        def pair_step(j, _):
            g = 4 * c + j
            slot = lax.rem(g, 3)
            p = 2 * (3 - j)

            @pl.when(c == 0)
            def _():
                comb_copy(p).wait()
                comb_copy(p + 1).wait()

            @pl.when(g >= 3)
            def _():
                f_copy(slot).wait_send()

            fsend[slot] = combine(p + 1 - core)
            mine[slot] = combine(p + core)

            @pl.when(g >= 3)
            def _():
                pl.semaphore_wait(credit, 1)

            f_copy(slot).start()

            @pl.when(g >= 2)
            def _():
                launch(g - 2)

            @pl.when(g >= 1)
            def _():
                consume(g - 1)

            return 0

        @pl.when(c == nc - 1)
        def _():
            for h in range(2):
                hs_copy(h).start()
                sd_copy(0, h).start()
                sd_copy(1, h).start()

        lax.fori_loop(0, 4, pair_step, 0)

        @pl.when(c >= 1)
        def _():
            relay(c - 1)

        return 0

    lax.fori_loop(0, nc, chunk, 0)
    launch(steps - 2)
    consume(steps - 1)
    for slot in range(3):
        f_copy(slot).wait_send()

    def y_copy(c):
        cols = pl.ds(pl.multiple_of(c * cw, cw), cw)
        return pltpu.make_async_copy(ybuf.at[lax.rem(c, 2)], y_hbm.at[:, cols], y_sem.at[lax.rem(c, 2)])

    for h in range(2):
        hs_copy(h).wait()

    def finish(c, _):
        for h in range(2):
            sd_copy(c, h).wait()
        slot = 2 * lax.rem(c, 2)
        shared = dot(act[0, :tokens], wbuf[slot]) + dot(act[1, :tokens], wbuf[slot + 1])

        @pl.when(c + 2 < nc)
        def _():
            for h in range(2):
                sd_copy(c + 2, h).start()

        acc[c] = acc[c] + shared

        @pl.when(c == nc // 2)
        def _():
            relay(nc - 1)

        return 0

    lax.fori_loop(0, nc, finish, 0)

    def write(c, _):
        for j in range(3):
            b_copy(j, c).wait_recv()

        @pl.when(c >= 2)
        def _():
            y_copy(c - 2).wait()

        total = acc[c]
        for j in range(3):
            total = total + brecv[j, c].astype(F32)
        ybuf[lax.rem(c, 2)] = total.astype(BF16)
        y_copy(c).start()
        return 0

    lax.fori_loop(0, nc, write, 0)
    for c in (nc - 2, nc - 1):
        y_copy(c).wait()
        pass_on(c).wait_send()
        for j in range(3):
            b_copy(j, c).wait_send()


def solution(mesh):
    groups = mesh.shape["ep"]
    tok_spec = P(("dp", "ep"), None)
    bank_spec = P("ep", None, None)
    vmem = pl.BlockSpec(memory_space=pltpu.VMEM)
    hbm = pl.BlockSpec(memory_space=pl.ANY)

    def device_fn(hidden, w_router, w_gate, w_up, w_down, shared_gate, shared_up, shared_down, top_idx, keep_mask):
        tokens, width = hidden.shape
        per_dev, _, ff = w_gate.shape
        rows = groups * CAP
        tn, cw = 256, 256
        nc = width // cw
        sff = shared_gate.shape[1]
        slots = 4
        table = (groups, 2 * per_dev, tokens)
        comb, shared_act, act, _ = pl.pallas_call(
            up_kernel,
            out_shape=(
                jax.ShapeDtypeStruct((groups, 3 * tokens, per_dev * CAP), BF16),
                jax.ShapeDtypeStruct((tokens, sff), BF16),
                jax.ShapeDtypeStruct((per_dev, rows, ff), BF16),
                jax.ShapeDtypeStruct((groups, tokens, width), BF16),
            ),
            in_specs=[vmem] * 3 + [hbm] * 5,
            out_specs=(hbm,) * 4,
            scratch_shapes=[
                pltpu.VMEM(table, F32),
                pltpu.VMEM(table, F32),
                pltpu.VMEM((2, 3 * tokens, per_dev * CAP), BF16),
                pltpu.VMEM((tokens, width), BF16),
                pltpu.VMEM((2, tokens, width), BF16),
                pltpu.VMEM((per_dev, rows - 2 * CAP, width), BF16),
                pltpu.VMEM((per_dev * CAP, tokens), BF16),
                pltpu.VMEM((slots, width, tn), BF16),
                pltpu.VMEM((slots, width, tn), BF16),
                pltpu.VMEM((tokens, sff), BF16),
                pltpu.VMEM((2, rows - 2 * CAP, tn), F32),
                pltpu.VMEM((2, rows - 2 * CAP, tn), F32),
                pltpu.VMEM((2, rows - 2 * CAP, tn), BF16),
                pltpu.SemaphoreType.DMA,
                pltpu.SemaphoreType.DMA((2,)),
                pltpu.SemaphoreType.DMA((2, slots)),
                pltpu.SemaphoreType.DMA((2,)),
                pltpu.SemaphoreType.DMA,
                pltpu.SemaphoreType.DMA((2,)),
                pltpu.SemaphoreType.DMA((groups,)),
                pltpu.SemaphoreType.DMA((groups,)),
                pltpu.SemaphoreType.DMA((7,)),
                pltpu.SemaphoreType.DMA((groups,)),
            ],
            compiler_params=pltpu.CompilerParams(vmem_limit_bytes=VMEM_BYTES, collective_id=1, has_side_effects=True),
            name="up",
        )(w_router.T, top_idx.T, keep_mask.T, hidden, w_gate, w_up, shared_gate, shared_up)
        y, _ = pl.pallas_call(
            down_kernel,
            out_shape=(
                jax.ShapeDtypeStruct((tokens, width), BF16),
                jax.ShapeDtypeStruct((nc, tokens, cw), BF16),
            ),
            in_specs=[hbm] * 5,
            out_specs=(hbm, hbm),
            scratch_shapes=[
                pltpu.VMEM((groups, 3 * tokens, per_dev * CAP), BF16),
                pltpu.VMEM((per_dev, rows, ff), BF16),
                pltpu.VMEM((groups, per_dev * CAP, cw), BF16),
                pltpu.VMEM((4, ff, cw), BF16),
                pltpu.VMEM((3, tokens, cw), F32),
                pltpu.VMEM((3, tokens, cw), F32),
                pltpu.VMEM((3, tokens, cw), F32),
                pltpu.VMEM((3, 2, tokens, cw), BF16),
                pltpu.VMEM((3, nc, tokens, cw), BF16),
                pltpu.VMEM((nc, tokens, cw), F32),
                pltpu.VMEM((2, tokens, cw), BF16),
                pltpu.SemaphoreType.DMA((per_dev,)),
                pltpu.SemaphoreType.DMA((4,)),
                pltpu.SemaphoreType.DMA((groups,)),
                pltpu.SemaphoreType.DMA((2,)),
                pltpu.SemaphoreType.DMA((2,)),
                pltpu.SemaphoreType.DMA((3,)),
                pltpu.SemaphoreType.DMA((3,)),
                pltpu.SemaphoreType.DMA((3, 2)),
                pltpu.SemaphoreType.DMA((3, nc)),
                pltpu.SemaphoreType.DMA((2,)),
                pltpu.SemaphoreType.DMA((nc,)),
                pltpu.SemaphoreType.REGULAR,
            ],
            compiler_params=pltpu.CompilerParams(vmem_limit_bytes=VMEM_BYTES, collective_id=0, has_side_effects=True),
            cost_estimate=pl.CostEstimate(flops=8 * per_dev * rows * width * ff, bytes_accessed=2 * per_dev * width * ff, transcendentals=0),
            name="down",
        )(comb, act, w_down, shared_act, shared_down)
        return y

    return jax.shard_map(device_fn, mesh=mesh, in_specs=(tok_spec, P(), bank_spec, bank_spec, bank_spec, P(), P(), P(), tok_spec, tok_spec), out_specs=tok_spec, check_vma=False)
```

```python
import functools

import jax
import jax.numpy as jnp
from jax import lax
from jax.experimental import pallas as pl
from jax.experimental.pallas import tpu as pltpu
from jax.sharding import PartitionSpec as P

ROUTE_SCALE = 16.0
CAP = 96
VMEM_BYTES = 66_900_000
MESH = pl.DeviceIdType.MESH
F32 = jnp.float32
BF16 = jnp.bfloat16


def dot(a, b):
    return jnp.dot(a, b, preferred_element_type=F32)


def route(x, w, idx_ref, keep_ref, tab_ref):
    experts, tokens = w.shape[0], x.shape[0]
    logits = lax.dot_general(w, x, (((1,), (1,)), ((), ())), preferred_element_type=F32)
    e = jnp.exp(logits - jnp.max(logits, axis=0, keepdims=True))
    prob = e / jnp.sum(e, axis=0, keepdims=True)
    expert_id = lax.broadcasted_iota(jnp.int32, (experts, tokens), 0)
    member = jnp.zeros((experts, tokens), F32)
    for k in range(idx_ref.shape[0]):
        hit = (expert_id == idx_ref[k : k + 1, :]) & (keep_ref[k : k + 1, :] > 0)
        member = jnp.where(hit, 1.0, member)
    earlier = lax.broadcasted_iota(jnp.int32, (tokens, tokens), 0) < lax.broadcasted_iota(jnp.int32, (tokens, tokens), 1)
    rank = dot(member.astype(BF16), jnp.where(earlier, 1.0, 0.0).astype(BF16))
    slot = jnp.where(member > 0, rank, -1.0)
    gate = ROUTE_SCALE * prob * member
    half = tab_ref.shape[1] // 2
    for d in range(tab_ref.shape[0]):
        tab_ref[d, :half, :] = slot[d * half : (d + 1) * half]
        tab_ref[d, half:, :] = gate[d * half : (d + 1) * half]


def relatives():
    me = lax.axis_index("ep")
    core, chip = lax.rem(me, 2), me // 2
    yb, xb = chip // 2, lax.rem(chip, 2)

    def first_core(r):
        return 2 * (2 * lax.rem(yb + r // 2, 2) + lax.rem(xb + lax.rem(r, 2), 2))

    return me, core, me + 1 - 2 * core, first_core


def up_kernel(
    wr_ref, idx_ref, keep_ref, x_hbm, w1_hbm, w3_hbm, sg_hbm, su_hbm, comb_hbm, hs_hbm, act_hbm, x_all,
    tab_ref, tabs, cbuf, xown, xbuf, xg, dbuf, wg, wu, hs, hg, hu, ab,
    own_sem, x_sem, w_sem, a_sem, hs_sem, c_sem, ts_sem, tr_sem, xs_sem, xr_sem,
):
    groups = tabs.shape[0]
    tokens, width = x_hbm.shape
    per_dev, _, ff = w1_hbm.shape
    slots, _, tn = wg.shape
    nt, ns = ff // tn, sg_hbm.shape[1] // tn
    steps = per_dev * nt
    xc = width // 2
    early = 2 * CAP
    late = groups * CAP - early
    forward_at = 7 * steps // 8
    near = late - 2 * CAP
    ahead = 2 * nt

    me, core, partner, first_core = relatives()

    def block_copy(k, src, pos, device):
        return pltpu.make_async_remote_copy(
            src_ref=src, dst_ref=x_all.at[pos], send_sem=xs_sem.at[k], recv_sem=xr_sem.at[pos],
            device_id={"ep": device}, device_id_type=MESH)

    def table_copy(r, k):
        dst = first_core(r) + k
        return pltpu.make_async_remote_copy(
            src_ref=tab_ref.at[dst], dst_ref=tabs.at[2 * r + core], send_sem=ts_sem.at[2 * r + k], recv_sem=tr_sem.at[2 * r + core],
            device_id={"ep": dst}, device_id_type=MESH)

    sends = [
        block_copy(0, x_hbm, core, partner),
        block_copy(1, x_hbm, 2 + core, first_core(1) + core),
        block_copy(2, x_hbm, 4 + core, first_core(2) + core),
        block_copy(3, x_all.at[2 + core], 2 + core, partner),
        block_copy(4, x_all.at[4 + core], 4 + core, partner),
        block_copy(5, x_all.at[4 - core], 6 + core, first_core(1 + core) + core),
        block_copy(6, x_all.at[6 + core], 6 + core, partner),
    ]

    def arrived(pos):
        block_copy(0, x_hbm, pos, partner).wait_recv()

    def w_start(t):
        slot = lax.rem(t, slots)

        def go(a, b):
            pltpu.make_async_copy(a, wg.at[slot], w_sem.at[0, slot]).start()
            pltpu.make_async_copy(b, wu.at[slot], w_sem.at[1, slot]).start()

        @pl.when(t < ns)
        def _():
            cols = pl.ds(pl.multiple_of(t * tn, tn), tn)
            go(sg_hbm.at[:, cols], su_hbm.at[:, cols])

        for begin, n_tiles in ((ns, steps), (ns + steps, ahead), (ns + steps + ahead, steps)):
            @pl.when((t >= begin) & (t < begin + n_tiles))
            def _():
                it = t - begin
                cols = pl.ds(pl.multiple_of(lax.rem(it, nt) * tn, tn), tn)
                go(w1_hbm.at[it // nt, :, cols], w3_hbm.at[it // nt, :, cols])

    def w_wait(t):
        slot = lax.rem(t, slots)
        pltpu.make_async_copy(sg_hbm.at[:, pl.ds(0, tn)], wg.at[slot], w_sem.at[0, slot]).wait()
        pltpu.make_async_copy(sg_hbm.at[:, pl.ds(0, tn)], wu.at[slot], w_sem.at[1, slot]).wait()
        return slot

    own_copy = pltpu.make_async_copy(x_hbm, xown, own_sem)
    own_copy.start()
    for t in range(slots - 1):
        w_start(t)

    barrier = pltpu.get_barrier_semaphore()
    for d in range(1, groups):
        pl.semaphore_signal(barrier, inc=1, device_id={"ep": lax.rem(me + d, groups)}, device_id_type=MESH)
    own_copy.wait()
    route(xown[...], wr_ref[...], idx_ref, keep_ref, tab_ref)
    pl.semaphore_wait(barrier, groups - 1)
    for r in range(4):
        for k in range(2):
            if r == 0:
                @pl.when(k != core)
                def _():
                    table_copy(r, k).start()
            else:
                table_copy(r, k).start()
    for k in range(3):
        sends[k].start()
    tabs[core] = tab_ref[me]

    def gated_pass(first, n_steps, n_rows, lhs, before, after):
        def activate(h):
            return (jax.nn.silu(hg[h, :n_rows]) * hu[h, :n_rows]).astype(BF16)

        def body(i, _):
            for h in range(2):
                it = 2 * i + h
                w_start(first + it + slots - 1)
                slot = w_wait(first + it)
                last = it - 1
                before(last)
                ab[1 - h, :n_rows] = activate(1 - h)
                x = lhs(it)
                hg[h, :n_rows] = dot(x, wg[slot])
                hu[h, :n_rows] = dot(x, wu[slot])
                after(last)
            return 0

        lax.fori_loop(0, n_steps // 2, body, 0)
        before(n_steps - 1)
        ab[1, :n_rows] = activate(1)
        after(n_steps - 1)

    def s_copy(it):
        cols = pl.ds(pl.multiple_of(it * tn, tn), tn)
        return ab.at[lax.rem(it, 2), pl.ds(0, tokens)], hs.at[:, cols]

    def shared_after(it):
        @pl.when(it >= 0)
        def _():
            src, dst = s_copy(it)
            dst[...] = src[...]

    hg[...] = jnp.zeros_like(hg)
    hu[...] = jnp.zeros_like(hu)
    gated_pass(0, ns, tokens, lambda it: xown[...], lambda it: None, shared_after)

    hs_copy = pltpu.make_async_copy(hs, hs_hbm, hs_sem)
    hs_copy.start()

    row = lax.broadcasted_iota(jnp.int32, (CAP, tokens), 0).astype(F32)

    def x_copy(pos, slot):
        return pltpu.make_async_copy(x_all.at[pos], xbuf.at[slot], x_sem.at[slot])

    def gather(pos, x_ref, base):
        for e in range(per_dev):
            dbuf[e * CAP : (e + 1) * CAP, :] = jnp.where(row == tabs[pos, pl.ds(e, 1), :], 1.0, 0.0).astype(BF16)
        rows = pl.ds(pl.multiple_of(base, CAP), CAP)

        def cols_step(n, _):
            cols = pl.ds(pl.multiple_of(n * xc, xc), xc)
            got = dot(dbuf[...], x_ref[:, cols]).astype(BF16)
            xg[:, rows, cols] = got.reshape(per_dev, CAP, xc)
            return 0

        lax.fori_loop(0, width // xc, cols_step, 0)

    def a_copy(it, n_rows, base):
        cols = pl.ds(pl.multiple_of(lax.rem(it, nt) * tn, tn), tn)
        slot = lax.rem(it, 2)
        return pltpu.make_async_copy(ab.at[slot, pl.ds(0, n_rows)], act_hbm.at[it // nt, pl.ds(base, n_rows), cols], a_sem.at[slot])

    def expert_pass(first, tile0, n_tiles, n_rows, row0, base):
        def before(k):
            @pl.when(k >= 2)
            def _():
                a_copy(tile0 + k - 2, n_rows, base).wait()

        def after(k):
            @pl.when(k >= 0)
            def _():
                a_copy(tile0 + k, n_rows, base).start()

            if base == 0:
                @pl.when(k == forward_at)
                def _():
                    arrived(2 + core)
                    sends[3].start()
                    arrived(4 + core)
                    sends[4].start()
                    sends[5].start()
                    x_copy(2 + core, 0).start()
                    x_copy(4 + core, 1).start()

        def lhs(k):
            return xg[(tile0 + k) // nt, row0 : row0 + n_rows]

        gated_pass(first, n_tiles, n_rows, lhs, before, after)
        a_copy(tile0 + n_tiles - 2, n_rows, base).wait()
        a_copy(tile0 + n_tiles - 1, n_rows, base).wait()

    for p in range(groups):
        @pl.when(p != core)
        def _():
            pltpu.make_async_remote_copy(
                src_ref=tab_ref.at[0], dst_ref=tabs.at[p], send_sem=ts_sem.at[p], recv_sem=tr_sem.at[p],
                device_id={"ep": partner}, device_id_type=MESH).wait_recv()

    arrived(1 - core)
    x_copy(1 - core, 0).start()
    gather(core, xown, core * CAP)
    x_copy(1 - core, 0).wait()
    gather(1 - core, xbuf.at[0], (1 - core) * CAP)
    expert_pass(ns, 0, steps, early, 0, 0)

    n_slots = per_dev * CAP
    lane = lax.broadcasted_iota(jnp.int32, (per_dev, n_slots), 1)
    lead = lax.broadcasted_iota(jnp.int32, (per_dev, n_slots), 0) * CAP
    inside = (lane >= lead) & (lane < lead + CAP)
    spread = jnp.where(inside, 1.0, 0.0).astype(BF16)
    want = jnp.sum(jnp.where(inside, lane - lead, 0).astype(F32), axis=0, keepdims=True)

    def over_slots(v):
        return lax.dot_general(v, spread, (((0,), (0,)), ((), ())), preferred_element_type=F32)

    def c_copy(p):
        return pltpu.make_async_copy(cbuf.at[lax.rem(p, 2)], comb_hbm.at[p], c_sem.at[lax.rem(p, 2)])

    def build(p, _):
        @pl.when(p >= 2)
        def _():
            c_copy(p - 2).wait()

        hit = over_slots(tabs[p, :per_dev, :].astype(BF16)) == want
        gate = tabs[p, per_dev:, :]
        hi = gate.astype(BF16)
        rest = gate - hi.astype(F32)
        mid = rest.astype(BF16)
        low = (rest - mid.astype(F32)).astype(BF16)
        for k, piece in enumerate((hi, mid, low)):
            cbuf[lax.rem(p, 2), k * tokens : (k + 1) * tokens] = jnp.where(hit, over_slots(piece), 0.0).astype(BF16)
        c_copy(p).start()
        return 0

    order = [2 + core, 4 + core, 3 - core, 5 - core, 6 + core, 7 - core]
    for n, pos in enumerate(order):
        x_copy(pos, n % 2).wait()
        gather(pos, xbuf.at[n % 2], (pos - 2) * CAP)
        if n + 2 < 6:
            if n + 2 == 2:
                arrived(3 - core)
            if n + 2 == 3:
                arrived(5 - core)
            if n + 2 < 4:
                x_copy(order[n + 2], n % 2).start()
        if n == 3:
            lax.fori_loop(0, groups, build, 0)
            expert_pass(ns + steps, 0, ahead, near, 0, early)
            arrived(6 + core)
            sends[6].start()
            x_copy(order[4], 0).start()
            arrived(7 - core)
            x_copy(order[5], 1).start()
    expert_pass(ns + steps + ahead, 0, ahead, late - near, near, early + near)
    expert_pass(ns + steps + 2 * ahead, ahead, steps - ahead, late, 0, early)

    hs_copy.wait()
    c_copy(groups - 2).wait()
    c_copy(groups - 1).wait()
    for k in range(7):
        sends[k].wait_send()
    for r in range(4):
        for k in range(2):
            if r == 0:
                @pl.when(k != core)
                def _():
                    table_copy(r, k).wait_send()
            else:
                table_copy(r, k).wait_send()


def down_kernel(
    comb_hbm, act_hbm, w2_hbm, hs_hbm, sd_hbm, y_hbm, through,
    comb, act, part, wbuf, fsend, frecv, mine, bsend, brecv, acc, ybuf,
    act_sem, w_sem, comb_sem, hs_sem, y_sem, fs_sem, fr_sem, bs_sem, br_sem, ts_sem, tr_sem, credit,
):
    groups, per_dev, tokens = comb_hbm.shape[0], w2_hbm.shape[0], y_hbm.shape[0]
    cw = wbuf.shape[2]
    nc = acc.shape[0]
    steps = 4 * nc

    me, core, partner, first_core = relatives()

    def w_copy(it):
        slot = lax.rem(it, 4)
        c, e = it // per_dev, lax.rem(it, per_dev)
        cols = pl.ds(pl.multiple_of(c * cw, cw), cw)
        return pltpu.make_async_copy(w2_hbm.at[e, :, cols], wbuf.at[slot], w_sem.at[slot])

    def act_copy(e):
        return pltpu.make_async_copy(act_hbm.at[e], act.at[e], act_sem.at[e])

    def comb_copy(p):
        return pltpu.make_async_copy(comb_hbm.at[p], comb.at[p], comb_sem.at[p])

    ff = act.shape[2]

    def hs_copy(h):
        return pltpu.make_async_copy(hs_hbm.at[:, pl.ds(h * ff, ff)], act.at[h, pl.ds(0, tokens)], hs_sem.at[h])

    def sd_copy(c, h):
        cols = pl.ds(pl.multiple_of(c * cw, cw), cw)
        slot = 2 * lax.rem(c, 2) + h
        return pltpu.make_async_copy(sd_hbm.at[pl.ds(h * ff, ff), cols], wbuf.at[slot], w_sem.at[slot])

    for it in range(2):
        w_copy(it).start()
    for e in range(per_dev):
        act_copy(e).start()
    for p in reversed(range(groups)):
        comb_copy(p).start()

    barrier = pltpu.get_barrier_semaphore()
    pl.semaphore_signal(barrier, inc=1, device_id={"ep": partner}, device_id_type=MESH)
    for j in range(3):
        pl.semaphore_signal(barrier, inc=1, device_id={"ep": first_core(3 - j) + core}, device_id_type=MESH)
    pl.semaphore_wait(barrier, 4)

    def f_copy(g):
        out, land = lax.rem(g, 3), lax.rem(g, 4)
        return pltpu.make_async_remote_copy(
            src_ref=fsend.at[out], dst_ref=frecv.at[land], send_sem=fs_sem.at[out], recv_sem=fr_sem.at[land],
            device_id={"ep": partner}, device_id_type=MESH)

    def b_copy(j, c):
        slot = lax.rem(c, 2)
        return pltpu.make_async_remote_copy(
            src_ref=bsend.at[j, slot], dst_ref=brecv.at[j, c], send_sem=bs_sem.at[j, slot], recv_sem=br_sem.at[j, c],
            device_id={"ep": first_core(3 - j) + core}, device_id_type=MESH)

    def t_copy(c):
        slot = lax.rem(c, 2)
        return pltpu.make_async_remote_copy(
            src_ref=bsend.at[0, slot], dst_ref=through.at[c], send_sem=bs_sem.at[0, slot], recv_sem=tr_sem.at[c],
            device_id={"ep": first_core(1 + core) + core}, device_id_type=MESH)

    def pass_on(c):
        slot = lax.rem(c, 2)
        return pltpu.make_async_remote_copy(
            src_ref=through.at[c], dst_ref=brecv.at[0, c], send_sem=ts_sem.at[slot], recv_sem=br_sem.at[0, c],
            device_id={"ep": first_core(2 - core) + core}, device_id_type=MESH)

    def relay(c):
        @pl.when(c >= 2)
        def _():
            pass_on(c - 2).wait_send()

        t_copy(c).wait_recv()
        pass_on(c).start()

    def combine(s):
        pieces = dot(comb[s], part[s])
        return pieces[:tokens] + pieces[tokens : 2 * tokens] + pieces[2 * tokens :]

    def launch(j, c):
        if j == 0:
            t_copy(c).start()
        elif j < 3:
            b_copy(j, c).start()

    def settle_wait(j, c):
        f_copy(4 * c + j).wait_recv()
        if j < 3:
            @pl.when(c >= 2)
            def _():
                b_copy(j, c - 2).wait_send()

    def settle(j, c):
        total = mine[lax.rem(4 * c + j, 3)] + frecv[j]
        if j < 3:
            bsend[j, lax.rem(c, 2)] = total.astype(BF16)
        else:
            acc[c] = total

    def credit_back(h):
        @pl.when((h >= 0) & (h + 4 < steps))
        def _():
            pl.semaphore_signal(credit, inc=1, device_id={"ep": partner}, device_id_type=MESH)

    def chunk(c, _, first=False):
        def down(i, _):
            for h in range(2):
                it = c * per_dev + 2 * i + h

                @pl.when(it + 2 < nc * per_dev)
                def _():
                    w_copy(it + 2).start()

                @pl.when(c == 0)
                def _():
                    act_copy(2 * i + h).wait()

            for h in range(2):
                w_copy(c * per_dev + 2 * i + h).wait()
            got = []
            for h in range(2):
                it = c * per_dev + 2 * i + h
                got.append(dot(act[2 * i + h], wbuf[lax.rem(it, 4)]).astype(BF16))
            for h in range(2):
                part[:, pl.ds(pl.multiple_of((2 * i + h) * CAP, CAP), CAP), :] = got[h].reshape(groups, CAP, cw)
            return 0

        lax.fori_loop(0, per_dev // 2, down, 0)

        @pl.when(c == nc - 1)
        def _():
            for h in range(2):
                hs_copy(h).start()
                sd_copy(0, h).start()
                sd_copy(1, h).start()

        for j in range(4):
            g = 4 * c + j
            p = 2 * (3 - j)
            jj, cc = (j + 1) % 4, c if j == 3 else c - 1

            @pl.when(c == 0)
            def _():
                comb_copy(p).wait()
                comb_copy(p + 1).wait()

            @pl.when(g >= 3)
            def _():
                f_copy(g - 3).wait_send()
                settle_wait(jj, cc)

            if not first or j == 3:
                settle(jj, cc)
            fsend[lax.rem(g, 3)] = combine(p + 1 - core)
            mine[lax.rem(g, 3)] = combine(p + core)
            credit_back(g - 3)

            @pl.when(g >= 4)
            def _():
                pl.semaphore_wait(credit, 1)

            f_copy(g).start()

            @pl.when(g >= 3)
            def _():
                launch(jj, cc)

        @pl.when(c >= 1)
        def _():
            relay(c - 1)

        return 0

    chunk(0, 0, first=True)
    lax.fori_loop(1, nc, chunk, 0)
    for j in range(1, 4):
        settle_wait(j, nc - 1)
        settle(j, nc - 1)
        launch(j, nc - 1)
    for g in range(steps - 3, steps):
        f_copy(g).wait_send()

    def y_copy(c):
        cols = pl.ds(pl.multiple_of(c * cw, cw), cw)
        return pltpu.make_async_copy(ybuf.at[lax.rem(c, 2)], y_hbm.at[:, cols], y_sem.at[lax.rem(c, 2)])

    for h in range(2):
        hs_copy(h).wait()

    def finish(c, _):
        for h in range(2):
            sd_copy(c, h).wait()
        for j in range(3):
            b_copy(j, c).wait_recv()

        @pl.when(c >= 2)
        def _():
            y_copy(c - 2).wait()

        slot = 2 * lax.rem(c, 2)
        total = acc[c] + dot(act[0, :tokens], wbuf[slot]) + dot(act[1, :tokens], wbuf[slot + 1])
        for j in range(3):
            total = total + brecv[j, c].astype(F32)
        ybuf[lax.rem(c, 2)] = total.astype(BF16)
        y_copy(c).start()

        @pl.when(c + 2 < nc)
        def _():
            for h in range(2):
                sd_copy(c + 2, h).start()

        @pl.when(c == nc // 2)
        def _():
            relay(nc - 1)

        return 0

    lax.fori_loop(0, nc, finish, 0)
    for c in (nc - 2, nc - 1):
        y_copy(c).wait()
        pass_on(c).wait_send()
        for j in range(3):
            b_copy(j, c).wait_send()


def solution(mesh):
    groups = mesh.shape["ep"]
    tok_spec = P(("dp", "ep"), None)
    bank_spec = P("ep", None, None)
    vmem = pl.BlockSpec(memory_space=pltpu.VMEM)
    hbm = pl.BlockSpec(memory_space=pl.ANY)

    def device_fn(hidden, w_router, w_gate, w_up, w_down, shared_gate, shared_up, shared_down, top_idx, keep_mask):
        tokens, width = hidden.shape
        per_dev, _, ff = w_gate.shape
        rows = groups * CAP
        tn, cw = 256, 256
        nc = width // cw
        sff = shared_gate.shape[1]
        slots = 4
        table = (groups, 2 * per_dev, tokens)
        comb, shared_act, act, _ = pl.pallas_call(
            up_kernel,
            out_shape=(
                jax.ShapeDtypeStruct((groups, 3 * tokens, per_dev * CAP), BF16),
                jax.ShapeDtypeStruct((tokens, sff), BF16),
                jax.ShapeDtypeStruct((per_dev, rows, ff), BF16),
                jax.ShapeDtypeStruct((groups, tokens, width), BF16),
            ),
            in_specs=[vmem] * 3 + [hbm] * 5,
            out_specs=(hbm,) * 4,
            scratch_shapes=[
                pltpu.VMEM(table, F32),
                pltpu.VMEM(table, F32),
                pltpu.VMEM((2, 3 * tokens, per_dev * CAP), BF16),
                pltpu.VMEM((tokens, width), BF16),
                pltpu.VMEM((2, tokens, width), BF16),
                pltpu.VMEM((per_dev, rows - 2 * CAP, width), BF16),
                pltpu.VMEM((per_dev * CAP, tokens), BF16),
                pltpu.VMEM((slots, width, tn), BF16),
                pltpu.VMEM((slots, width, tn), BF16),
                pltpu.VMEM((tokens, sff), BF16),
                pltpu.VMEM((2, rows - 2 * CAP, tn), F32),
                pltpu.VMEM((2, rows - 2 * CAP, tn), F32),
                pltpu.VMEM((2, rows - 2 * CAP, tn), BF16),
                pltpu.SemaphoreType.DMA,
                pltpu.SemaphoreType.DMA((2,)),
                pltpu.SemaphoreType.DMA((2, slots)),
                pltpu.SemaphoreType.DMA((2,)),
                pltpu.SemaphoreType.DMA,
                pltpu.SemaphoreType.DMA((2,)),
                pltpu.SemaphoreType.DMA((groups,)),
                pltpu.SemaphoreType.DMA((groups,)),
                pltpu.SemaphoreType.DMA((7,)),
                pltpu.SemaphoreType.DMA((groups,)),
            ],
            compiler_params=pltpu.CompilerParams(vmem_limit_bytes=VMEM_BYTES, collective_id=1, has_side_effects=True),
            name="up",
        )(w_router.T, top_idx.T, keep_mask.T, hidden, w_gate, w_up, shared_gate, shared_up)
        y, _ = pl.pallas_call(
            down_kernel,
            out_shape=(
                jax.ShapeDtypeStruct((tokens, width), BF16),
                jax.ShapeDtypeStruct((nc, tokens, cw), BF16),
            ),
            in_specs=[hbm] * 5,
            out_specs=(hbm, hbm),
            scratch_shapes=[
                pltpu.VMEM((groups, 3 * tokens, per_dev * CAP), BF16),
                pltpu.VMEM((per_dev, rows, ff), BF16),
                pltpu.VMEM((groups, per_dev * CAP, cw), BF16),
                pltpu.VMEM((4, ff, cw), BF16),
                pltpu.VMEM((3, tokens, cw), F32),
                pltpu.VMEM((4, tokens, cw), F32),
                pltpu.VMEM((3, tokens, cw), F32),
                pltpu.VMEM((3, 2, tokens, cw), BF16),
                pltpu.VMEM((3, nc, tokens, cw), BF16),
                pltpu.VMEM((nc, tokens, cw), F32),
                pltpu.VMEM((2, tokens, cw), BF16),
                pltpu.SemaphoreType.DMA((per_dev,)),
                pltpu.SemaphoreType.DMA((4,)),
                pltpu.SemaphoreType.DMA((groups,)),
                pltpu.SemaphoreType.DMA((2,)),
                pltpu.SemaphoreType.DMA((2,)),
                pltpu.SemaphoreType.DMA((3,)),
                pltpu.SemaphoreType.DMA((4,)),
                pltpu.SemaphoreType.DMA((3, 2)),
                pltpu.SemaphoreType.DMA((3, nc)),
                pltpu.SemaphoreType.DMA((2,)),
                pltpu.SemaphoreType.DMA((nc,)),
                pltpu.SemaphoreType.REGULAR,
            ],
            compiler_params=pltpu.CompilerParams(vmem_limit_bytes=VMEM_BYTES, collective_id=0, has_side_effects=True),
            cost_estimate=pl.CostEstimate(flops=8 * per_dev * rows * width * ff, bytes_accessed=2 * per_dev * width * ff, transcendentals=0),
            name="down",
        )(comb, act, w_down, shared_act, shared_down)
        return y

    return jax.shard_map(device_fn, mesh=mesh, in_specs=(tok_spec, P(), bank_spec, bank_spec, bank_spec, P(), P(), P(), tok_spec, tok_spec), out_specs=tok_spec, check_vma=False)
```

```python
import functools

import jax
import jax.numpy as jnp
from jax import lax
from jax.experimental import pallas as pl
from jax.experimental.pallas import tpu as pltpu
from jax.sharding import PartitionSpec as P

ROUTE_SCALE = 16.0
scope = jax.named_scope
CAP = 96
VMEM_BYTES = 66_900_000
MESH = pl.DeviceIdType.MESH
F32 = jnp.float32
BF16 = jnp.bfloat16


def dot(a, b):
    return jnp.dot(a, b, preferred_element_type=F32)


def route(x, w, idx_ref, keep_ref, tab_ref):
    experts, tokens = w.shape[0], x.shape[0]
    logits = lax.dot_general(w, x, (((1,), (1,)), ((), ())), preferred_element_type=F32)
    e = jnp.exp(logits - jnp.max(logits, axis=0, keepdims=True))
    prob = e / jnp.sum(e, axis=0, keepdims=True)
    expert_id = lax.broadcasted_iota(jnp.int32, (experts, tokens), 0)
    member = jnp.zeros((experts, tokens), F32)
    for k in range(idx_ref.shape[0]):
        hit = (expert_id == idx_ref[k : k + 1, :]) & (keep_ref[k : k + 1, :] > 0)
        member = jnp.where(hit, 1.0, member)
    earlier = lax.broadcasted_iota(jnp.int32, (tokens, tokens), 0) < lax.broadcasted_iota(jnp.int32, (tokens, tokens), 1)
    rank = dot(member.astype(BF16), jnp.where(earlier, 1.0, 0.0).astype(BF16))
    slot = jnp.where(member > 0, rank, -1.0)
    gate = ROUTE_SCALE * prob * member
    half = tab_ref.shape[1] // 2
    for d in range(tab_ref.shape[0]):
        tab_ref[d, :half, :] = slot[d * half : (d + 1) * half]
        tab_ref[d, half:, :] = gate[d * half : (d + 1) * half]


def relatives():
    me = lax.axis_index("ep")
    core, chip = lax.rem(me, 2), me // 2
    yb, xb = chip // 2, lax.rem(chip, 2)

    def first_core(r):
        return 2 * (2 * lax.rem(yb + r // 2, 2) + lax.rem(xb + lax.rem(r, 2), 2))

    return me, core, me + 1 - 2 * core, first_core


def up_kernel(
    wr_ref, idx_ref, keep_ref, x_hbm, w1_hbm, w3_hbm, sg_hbm, su_hbm, comb_hbm, hs_hbm, act_hbm, x_all,
    tab_ref, tabs, cbuf, xown, xbuf, xg, dbuf, wg, wu, hs, hg, hu, ab,
    own_sem, x_sem, w_sem, a_sem, hs_sem, c_sem, ts_sem, tr_sem, xs_sem, xr_sem,
):
    groups = tabs.shape[0]
    tokens, width = x_hbm.shape
    per_dev, _, ff = w1_hbm.shape
    slots, _, tn = wg.shape
    nt, ns = ff // tn, sg_hbm.shape[1] // tn
    steps = per_dev * nt
    xc = width // 2
    early = 2 * CAP
    late = groups * CAP - early
    forward_at = 7 * steps // 8
    near = late - 2 * CAP
    ahead = 2 * nt

    me, core, partner, first_core = relatives()

    def block_copy(k, src, pos, device):
        return pltpu.make_async_remote_copy(
            src_ref=src, dst_ref=x_all.at[pos], send_sem=xs_sem.at[k], recv_sem=xr_sem.at[pos],
            device_id={"ep": device}, device_id_type=MESH)

    def table_copy(r, k):
        dst = first_core(r) + k
        return pltpu.make_async_remote_copy(
            src_ref=tab_ref.at[dst], dst_ref=tabs.at[2 * r + core], send_sem=ts_sem.at[2 * r + k], recv_sem=tr_sem.at[2 * r + core],
            device_id={"ep": dst}, device_id_type=MESH)

    sends = [
        block_copy(0, x_hbm, core, partner),
        block_copy(1, x_hbm, 2 + core, first_core(1) + core),
        block_copy(2, x_hbm, 4 + core, first_core(2) + core),
        block_copy(3, x_all.at[2 + core], 2 + core, partner),
        block_copy(4, x_all.at[4 + core], 4 + core, partner),
        block_copy(5, x_all.at[4 - core], 6 + core, first_core(1 + core) + core),
        block_copy(6, x_all.at[6 + core], 6 + core, partner),
    ]

    def arrived(pos):
        block_copy(0, x_hbm, pos, partner).wait_recv()

    def w_start(t):
        slot = lax.rem(t, slots)

        def go(a, b):
            pltpu.make_async_copy(a, wg.at[slot], w_sem.at[0, slot]).start()
            pltpu.make_async_copy(b, wu.at[slot], w_sem.at[1, slot]).start()

        @pl.when(t < ns)
        def _():
            cols = pl.ds(pl.multiple_of(t * tn, tn), tn)
            go(sg_hbm.at[:, cols], su_hbm.at[:, cols])

        for begin, n_tiles in ((ns, steps), (ns + steps, ahead), (ns + steps + ahead, steps)):
            @pl.when((t >= begin) & (t < begin + n_tiles))
            def _():
                it = t - begin
                cols = pl.ds(pl.multiple_of(lax.rem(it, nt) * tn, tn), tn)
                go(w1_hbm.at[it // nt, :, cols], w3_hbm.at[it // nt, :, cols])

    def w_wait(t):
        slot = lax.rem(t, slots)
        pltpu.make_async_copy(sg_hbm.at[:, pl.ds(0, tn)], wg.at[slot], w_sem.at[0, slot]).wait()
        pltpu.make_async_copy(sg_hbm.at[:, pl.ds(0, tn)], wu.at[slot], w_sem.at[1, slot]).wait()
        return slot

    own_copy = pltpu.make_async_copy(x_hbm, xown, own_sem)
    own_copy.start()
    for t in range(slots - 1):
        w_start(t)

    barrier = pltpu.get_barrier_semaphore()
    for d in range(1, groups):
        pl.semaphore_signal(barrier, inc=1, device_id={"ep": lax.rem(me + d, groups)}, device_id_type=MESH)
    own_copy.wait()
    route(xown[...], wr_ref[...], idx_ref, keep_ref, tab_ref)
    with scope('barrier1'):
        pl.semaphore_wait(barrier, groups - 1)
    for r in range(4):
        for k in range(2):
            if r == 0:
                @pl.when(k != core)
                def _():
                    table_copy(r, k).start()
            else:
                table_copy(r, k).start()
    for k in range(3):
        sends[k].start()
    tabs[core] = tab_ref[me]

    def gated_pass(first, n_steps, n_rows, lhs, before, after):
        def activate(h):
            return (jax.nn.silu(hg[h, :n_rows]) * hu[h, :n_rows]).astype(BF16)

        def body(i, _):
            for h in range(2):
                it = 2 * i + h
                w_start(first + it + slots - 1)
                slot = w_wait(first + it)
                last = it - 1
                before(last)
                ab[1 - h, :n_rows] = activate(1 - h)
                x = lhs(it)
                hg[h, :n_rows] = dot(x, wg[slot])
                hu[h, :n_rows] = dot(x, wu[slot])
                after(last)
            return 0

        lax.fori_loop(0, n_steps // 2, body, 0)
        before(n_steps - 1)
        ab[1, :n_rows] = activate(1)
        after(n_steps - 1)

    def s_copy(it):
        cols = pl.ds(pl.multiple_of(it * tn, tn), tn)
        return ab.at[lax.rem(it, 2), pl.ds(0, tokens)], hs.at[:, cols]

    def shared_after(it):
        @pl.when(it >= 0)
        def _():
            src, dst = s_copy(it)
            dst[...] = src[...]

    hg[...] = jnp.zeros_like(hg)
    hu[...] = jnp.zeros_like(hu)
    with scope('shared_up'):
      gated_pass(0, ns, tokens, lambda it: xown[...], lambda it: None, shared_after)

    hs_copy = pltpu.make_async_copy(hs, hs_hbm, hs_sem)
    hs_copy.start()

    row = lax.broadcasted_iota(jnp.int32, (CAP, tokens), 0).astype(F32)

    def x_copy(pos, slot):
        return pltpu.make_async_copy(x_all.at[pos], xbuf.at[slot], x_sem.at[slot])

    def gather(pos, x_ref, base):
        for e in range(per_dev):
            dbuf[e * CAP : (e + 1) * CAP, :] = jnp.where(row == tabs[pos, pl.ds(e, 1), :], 1.0, 0.0).astype(BF16)
        rows = pl.ds(pl.multiple_of(base, CAP), CAP)

        def cols_step(n, _):
            cols = pl.ds(pl.multiple_of(n * xc, xc), xc)
            got = dot(dbuf[...], x_ref[:, cols]).astype(BF16)
            xg[:, rows, cols] = got.reshape(per_dev, CAP, xc)
            return 0

        lax.fori_loop(0, width // xc, cols_step, 0)

    def a_copy(it, n_rows, base):
        cols = pl.ds(pl.multiple_of(lax.rem(it, nt) * tn, tn), tn)
        slot = lax.rem(it, 2)
        return pltpu.make_async_copy(ab.at[slot, pl.ds(0, n_rows)], act_hbm.at[it // nt, pl.ds(base, n_rows), cols], a_sem.at[slot])

    def expert_pass(first, tile0, n_tiles, n_rows, row0, base):
        def before(k):
            @pl.when(k >= 2)
            def _():
                a_copy(tile0 + k - 2, n_rows, base).wait()

        def after(k):
            @pl.when(k >= 0)
            def _():
                a_copy(tile0 + k, n_rows, base).start()

            if base == 0:
                @pl.when(k == forward_at)
                def _():
                    with scope('wait_x'):
                        arrived(2 + core)
                    sends[3].start()
                    with scope('wait_y'):
                        arrived(4 + core)
                    sends[4].start()
                    sends[5].start()
                    x_copy(2 + core, 0).start()
                    x_copy(4 + core, 1).start()

        def lhs(k):
            return xg[(tile0 + k) // nt, row0 : row0 + n_rows]

        gated_pass(first, n_tiles, n_rows, lhs, before, after)
        a_copy(tile0 + n_tiles - 2, n_rows, base).wait()
        a_copy(tile0 + n_tiles - 1, n_rows, base).wait()

    for p in range(groups):
        @pl.when(p != core)
        def _():
            pltpu.make_async_remote_copy(
                src_ref=tab_ref.at[0], dst_ref=tabs.at[p], send_sem=ts_sem.at[p], recv_sem=tr_sem.at[p],
                device_id={"ep": partner}, device_id_type=MESH).wait_recv()

    arrived(1 - core)
    x_copy(1 - core, 0).start()
    gather(core, xown, core * CAP)
    x_copy(1 - core, 0).wait()
    gather(1 - core, xbuf.at[0], (1 - core) * CAP)
    with scope('pass_a'):
        expert_pass(ns, 0, steps, early, 0, 0)

    n_slots = per_dev * CAP
    lane = lax.broadcasted_iota(jnp.int32, (per_dev, n_slots), 1)
    lead = lax.broadcasted_iota(jnp.int32, (per_dev, n_slots), 0) * CAP
    inside = (lane >= lead) & (lane < lead + CAP)
    spread = jnp.where(inside, 1.0, 0.0).astype(BF16)
    want = jnp.sum(jnp.where(inside, lane - lead, 0).astype(F32), axis=0, keepdims=True)

    def over_slots(v):
        return lax.dot_general(v, spread, (((0,), (0,)), ((), ())), preferred_element_type=F32)

    def c_copy(p):
        return pltpu.make_async_copy(cbuf.at[lax.rem(p, 2)], comb_hbm.at[p], c_sem.at[lax.rem(p, 2)])

    def build(p, _):
        @pl.when(p >= 2)
        def _():
            c_copy(p - 2).wait()

        hit = over_slots(tabs[p, :per_dev, :].astype(BF16)) == want
        gate = tabs[p, per_dev:, :]
        hi = gate.astype(BF16)
        rest = gate - hi.astype(F32)
        mid = rest.astype(BF16)
        low = (rest - mid.astype(F32)).astype(BF16)
        for k, piece in enumerate((hi, mid, low)):
            cbuf[lax.rem(p, 2), k * tokens : (k + 1) * tokens] = jnp.where(hit, over_slots(piece), 0.0).astype(BF16)
        c_copy(p).start()
        return 0

    order = [2 + core, 4 + core, 3 - core, 5 - core, 6 + core, 7 - core]
    for n, pos in enumerate(order):
        x_copy(pos, n % 2).wait()
        gather(pos, xbuf.at[n % 2], (pos - 2) * CAP)
        if n + 2 < 6:
            if n + 2 == 2:
                arrived(3 - core)
            if n + 2 == 3:
                arrived(5 - core)
            if n + 2 < 4:
                x_copy(order[n + 2], n % 2).start()
        if n == 3:
            with scope('build'):
                lax.fori_loop(0, groups, build, 0)
            with scope('pass_a2'):
                expert_pass(ns + steps, 0, ahead, near, 0, early)
            with scope('wait_diag'):
                arrived(6 + core)
            sends[6].start()
            x_copy(order[4], 0).start()
            arrived(7 - core)
            x_copy(order[5], 1).start()
    with scope('pass_b1'):
        expert_pass(ns + steps + ahead, 0, ahead, late - near, near, early + near)
    with scope('pass_b2'):
        expert_pass(ns + steps + 2 * ahead, ahead, steps - ahead, late, 0, early)

    hs_copy.wait()
    c_copy(groups - 2).wait()
    c_copy(groups - 1).wait()
    for k in range(7):
        sends[k].wait_send()
    for r in range(4):
        for k in range(2):
            if r == 0:
                @pl.when(k != core)
                def _():
                    table_copy(r, k).wait_send()
            else:
                table_copy(r, k).wait_send()


def down_kernel(
    comb_hbm, act_hbm, w2_hbm, hs_hbm, sd_hbm, y_hbm, through,
    comb, act, part, wbuf, fsend, frecv, mine, bsend, brecv, acc, ybuf,
    act_sem, w_sem, comb_sem, hs_sem, y_sem, fs_sem, fr_sem, bs_sem, br_sem, ts_sem, tr_sem, credit,
):
    groups, per_dev, tokens = comb_hbm.shape[0], w2_hbm.shape[0], y_hbm.shape[0]
    cw = wbuf.shape[2]
    nc = acc.shape[0]
    steps = 4 * nc

    me, core, partner, first_core = relatives()

    def w_copy(it):
        slot = lax.rem(it, 4)
        c, e = it // per_dev, lax.rem(it, per_dev)
        cols = pl.ds(pl.multiple_of(c * cw, cw), cw)
        return pltpu.make_async_copy(w2_hbm.at[e, :, cols], wbuf.at[slot], w_sem.at[slot])

    def act_copy(e):
        return pltpu.make_async_copy(act_hbm.at[e], act.at[e], act_sem.at[e])

    def comb_copy(p):
        return pltpu.make_async_copy(comb_hbm.at[p], comb.at[p], comb_sem.at[p])

    ff = act.shape[2]

    def hs_copy(h):
        return pltpu.make_async_copy(hs_hbm.at[:, pl.ds(h * ff, ff)], act.at[h, pl.ds(0, tokens)], hs_sem.at[h])

    def sd_copy(c, h):
        cols = pl.ds(pl.multiple_of(c * cw, cw), cw)
        slot = 2 * lax.rem(c, 2) + h
        return pltpu.make_async_copy(sd_hbm.at[pl.ds(h * ff, ff), cols], wbuf.at[slot], w_sem.at[slot])

    for it in range(2):
        w_copy(it).start()
    for e in range(per_dev):
        act_copy(e).start()
    for p in reversed(range(groups)):
        comb_copy(p).start()

    barrier = pltpu.get_barrier_semaphore()
    pl.semaphore_signal(barrier, inc=1, device_id={"ep": partner}, device_id_type=MESH)
    for j in range(3):
        pl.semaphore_signal(barrier, inc=1, device_id={"ep": first_core(3 - j) + core}, device_id_type=MESH)
    pl.semaphore_wait(barrier, 4)

    def f_copy(g):
        out, land = lax.rem(g, 3), lax.rem(g, 4)
        return pltpu.make_async_remote_copy(
            src_ref=fsend.at[out], dst_ref=frecv.at[land], send_sem=fs_sem.at[out], recv_sem=fr_sem.at[land],
            device_id={"ep": partner}, device_id_type=MESH)

    def b_copy(j, c):
        slot = lax.rem(c, 2)
        return pltpu.make_async_remote_copy(
            src_ref=bsend.at[j, slot], dst_ref=brecv.at[j, c], send_sem=bs_sem.at[j, slot], recv_sem=br_sem.at[j, c],
            device_id={"ep": first_core(3 - j) + core}, device_id_type=MESH)

    def t_copy(c):
        slot = lax.rem(c, 2)
        return pltpu.make_async_remote_copy(
            src_ref=bsend.at[0, slot], dst_ref=through.at[c], send_sem=bs_sem.at[0, slot], recv_sem=tr_sem.at[c],
            device_id={"ep": first_core(1 + core) + core}, device_id_type=MESH)

    def pass_on(c):
        slot = lax.rem(c, 2)
        return pltpu.make_async_remote_copy(
            src_ref=through.at[c], dst_ref=brecv.at[0, c], send_sem=ts_sem.at[slot], recv_sem=br_sem.at[0, c],
            device_id={"ep": first_core(2 - core) + core}, device_id_type=MESH)

    def relay(c):
        @pl.when(c >= 2)
        def _():
            with scope('pass_on_wait'):
                pass_on(c - 2).wait_send()

        with scope('through_wait'):
            t_copy(c).wait_recv()
        pass_on(c).start()

    def combine(s):
        pieces = dot(comb[s], part[s])
        return pieces[:tokens] + pieces[tokens : 2 * tokens] + pieces[2 * tokens :]

    def launch(j, c):
        if j == 0:
            t_copy(c).start()
        elif j < 3:
            b_copy(j, c).start()

    def settle_wait(j, c):
        with scope('f_wait'):
            f_copy(4 * c + j).wait_recv()
        if j < 3:
            @pl.when(c >= 2)
            def _():
                with scope('b_send_wait%d' % j):
                    b_copy(j, c - 2).wait_send()

    def settle(j, c):
        total = mine[lax.rem(4 * c + j, 3)] + frecv[j]
        if j < 3:
            bsend[j, lax.rem(c, 2)] = total.astype(BF16)
        else:
            acc[c] = total

    def credit_back(h):
        @pl.when((h >= 0) & (h + 4 < steps))
        def _():
            pl.semaphore_signal(credit, inc=1, device_id={"ep": partner}, device_id_type=MESH)

    def chunk(c, _, early=None):
        def down(i, _):
            for h in range(2):
                it = c * per_dev + 2 * i + h

                @pl.when(it + 2 < nc * per_dev)
                def _():
                    w_copy(it + 2).start()

                @pl.when(c == 0)
                def _():
                    act_copy(2 * i + h).wait()

            for h in range(2):
                w_copy(c * per_dev + 2 * i + h).wait()
            got = []
            for h in range(2):
                it = c * per_dev + 2 * i + h
                got.append(dot(act[2 * i + h], wbuf[lax.rem(it, 4)]).astype(BF16))
            for h in range(2):
                part[:, pl.ds(pl.multiple_of((2 * i + h) * CAP, CAP), CAP), :] = got[h].reshape(groups, CAP, cw)
            return 0

        with scope('down_dots'):
            lax.fori_loop(0, per_dev // 2, down, 0)

        @pl.when(c == nc - 1)
        def _():
            for h in range(2):
                hs_copy(h).start()
                sd_copy(0, h).start()
                sd_copy(1, h).start()

        for j in range(4):
            g = 4 * c + j
            p = 2 * (3 - j)
            jj, cc = (j + 1) % 4, c if j == 3 else c - 1

            @pl.when(c == 0)
            def _():
                comb_copy(p).wait()
                comb_copy(p + 1).wait()

            late = early is None or (early == 1 and j >= 2)

            @pl.when(g >= 3)
            def _():
                f_copy(g - 3).wait_send()
                if late:
                    settle_wait(jj, cc)

            if late:
                settle(jj, cc)
            fsend[lax.rem(g, 3)] = combine(p + 1 - core)
            mine[lax.rem(g, 3)] = combine(p + core)
            if late:
                credit_back(g - 3)

            @pl.when(g >= 4)
            def _():
                with scope('credit_wait'):
                    pl.semaphore_wait(credit, 1)

            f_copy(g).start()

            if late:
                launch(jj, cc)
            elif early == 0 and j >= 1:
                settle_wait(j - 1, 0)
                settle(j - 1, 0)
                credit_back(j - 1)
                launch(j - 1, 0)

        @pl.when(c >= 1)
        def _():
            relay(c - 1)

        return 0

    for c in range(2):
        chunk(c, 0, early=c)
    lax.fori_loop(2, nc, chunk, 0)
    for j in range(1, 4):
        settle_wait(j, nc - 1)
        settle(j, nc - 1)
        launch(j, nc - 1)
    for g in range(steps - 3, steps):
        f_copy(g).wait_send()

    def y_copy(c):
        cols = pl.ds(pl.multiple_of(c * cw, cw), cw)
        return pltpu.make_async_copy(ybuf.at[lax.rem(c, 2)], y_hbm.at[:, cols], y_sem.at[lax.rem(c, 2)])

    for h in range(2):
        hs_copy(h).wait()

    def finish(c, _):
        for h in range(2):
            sd_copy(c, h).wait()
        for j in range(3):
            with scope('tail_wait%d' % j):
                b_copy(j, c).wait_recv()

        @pl.when(c >= 2)
        def _():
            y_copy(c - 2).wait()

        slot = 2 * lax.rem(c, 2)
        total = acc[c] + dot(act[0, :tokens], wbuf[slot]) + dot(act[1, :tokens], wbuf[slot + 1])
        for j in range(3):
            total = total + brecv[j, c].astype(F32)
        ybuf[lax.rem(c, 2)] = total.astype(BF16)
        y_copy(c).start()

        @pl.when(c + 2 < nc)
        def _():
            for h in range(2):
                sd_copy(c + 2, h).start()

        @pl.when(c == nc // 2)
        def _():
            relay(nc - 1)

        return 0

    with scope('finish'):
        lax.fori_loop(0, nc, finish, 0)
    for c in (nc - 2, nc - 1):
        y_copy(c).wait()
        pass_on(c).wait_send()
        for j in range(3):
            b_copy(j, c).wait_send()


def solution(mesh):
    groups = mesh.shape["ep"]
    tok_spec = P(("dp", "ep"), None)
    bank_spec = P("ep", None, None)
    vmem = pl.BlockSpec(memory_space=pltpu.VMEM)
    hbm = pl.BlockSpec(memory_space=pl.ANY)

    def device_fn(hidden, w_router, w_gate, w_up, w_down, shared_gate, shared_up, shared_down, top_idx, keep_mask):
        tokens, width = hidden.shape
        per_dev, _, ff = w_gate.shape
        rows = groups * CAP
        tn, cw = 256, 256
        nc = width // cw
        sff = shared_gate.shape[1]
        slots = 4
        table = (groups, 2 * per_dev, tokens)
        comb, shared_act, act, _ = pl.pallas_call(
            up_kernel,
            out_shape=(
                jax.ShapeDtypeStruct((groups, 3 * tokens, per_dev * CAP), BF16),
                jax.ShapeDtypeStruct((tokens, sff), BF16),
                jax.ShapeDtypeStruct((per_dev, rows, ff), BF16),
                jax.ShapeDtypeStruct((groups, tokens, width), BF16),
            ),
            in_specs=[vmem] * 3 + [hbm] * 5,
            out_specs=(hbm,) * 4,
            scratch_shapes=[
                pltpu.VMEM(table, F32),
                pltpu.VMEM(table, F32),
                pltpu.VMEM((2, 3 * tokens, per_dev * CAP), BF16),
                pltpu.VMEM((tokens, width), BF16),
                pltpu.VMEM((2, tokens, width), BF16),
                pltpu.VMEM((per_dev, rows - 2 * CAP, width), BF16),
                pltpu.VMEM((per_dev * CAP, tokens), BF16),
                pltpu.VMEM((slots, width, tn), BF16),
                pltpu.VMEM((slots, width, tn), BF16),
                pltpu.VMEM((tokens, sff), BF16),
                pltpu.VMEM((2, rows - 2 * CAP, tn), F32),
                pltpu.VMEM((2, rows - 2 * CAP, tn), F32),
                pltpu.VMEM((2, rows - 2 * CAP, tn), BF16),
                pltpu.SemaphoreType.DMA,
                pltpu.SemaphoreType.DMA((2,)),
                pltpu.SemaphoreType.DMA((2, slots)),
                pltpu.SemaphoreType.DMA((2,)),
                pltpu.SemaphoreType.DMA,
                pltpu.SemaphoreType.DMA((2,)),
                pltpu.SemaphoreType.DMA((groups,)),
                pltpu.SemaphoreType.DMA((groups,)),
                pltpu.SemaphoreType.DMA((7,)),
                pltpu.SemaphoreType.DMA((groups,)),
            ],
            compiler_params=pltpu.CompilerParams(vmem_limit_bytes=VMEM_BYTES, collective_id=1, has_side_effects=True),
            name="up",
        )(w_router.T, top_idx.T, keep_mask.T, hidden, w_gate, w_up, shared_gate, shared_up)
        y, _ = pl.pallas_call(
            down_kernel,
            out_shape=(
                jax.ShapeDtypeStruct((tokens, width), BF16),
                jax.ShapeDtypeStruct((nc, tokens, cw), BF16),
            ),
            in_specs=[hbm] * 5,
            out_specs=(hbm, hbm),
            scratch_shapes=[
                pltpu.VMEM((groups, 3 * tokens, per_dev * CAP), BF16),
                pltpu.VMEM((per_dev, rows, ff), BF16),
                pltpu.VMEM((groups, per_dev * CAP, cw), BF16),
                pltpu.VMEM((4, ff, cw), BF16),
                pltpu.VMEM((3, tokens, cw), F32),
                pltpu.VMEM((4, tokens, cw), F32),
                pltpu.VMEM((3, tokens, cw), F32),
                pltpu.VMEM((3, 2, tokens, cw), BF16),
                pltpu.VMEM((3, nc, tokens, cw), BF16),
                pltpu.VMEM((nc, tokens, cw), F32),
                pltpu.VMEM((2, tokens, cw), BF16),
                pltpu.SemaphoreType.DMA((per_dev,)),
                pltpu.SemaphoreType.DMA((4,)),
                pltpu.SemaphoreType.DMA((groups,)),
                pltpu.SemaphoreType.DMA((2,)),
                pltpu.SemaphoreType.DMA((2,)),
                pltpu.SemaphoreType.DMA((3,)),
                pltpu.SemaphoreType.DMA((4,)),
                pltpu.SemaphoreType.DMA((3, 2)),
                pltpu.SemaphoreType.DMA((3, nc)),
                pltpu.SemaphoreType.DMA((2,)),
                pltpu.SemaphoreType.DMA((nc,)),
                pltpu.SemaphoreType.REGULAR,
            ],
            compiler_params=pltpu.CompilerParams(vmem_limit_bytes=VMEM_BYTES, collective_id=0, has_side_effects=True),
            cost_estimate=pl.CostEstimate(flops=8 * per_dev * rows * width * ff, bytes_accessed=2 * per_dev * width * ff, transcendentals=0),
            name="down",
        )(comb, act, w_down, shared_act, shared_down)
        return y

    return jax.shard_map(device_fn, mesh=mesh, in_specs=(tok_spec, P(), bank_spec, bank_spec, bank_spec, P(), P(), P(), tok_spec, tok_spec), out_specs=tok_spec, check_vma=False)
```

```python
import functools

import jax
import jax.numpy as jnp
from jax import lax
from jax.experimental import pallas as pl
from jax.experimental.pallas import tpu as pltpu
from jax.sharding import PartitionSpec as P

ROUTE_SCALE = 16.0
CAP = 96
VMEM_BYTES = 66_900_000
MESH = pl.DeviceIdType.MESH
F32 = jnp.float32
BF16 = jnp.bfloat16


def dot(a, b):
    return jnp.dot(a, b, preferred_element_type=F32)


def route(x, w, idx_ref, keep_ref, tab_ref):
    experts, tokens = w.shape[0], x.shape[0]
    logits = lax.dot_general(w, x, (((1,), (1,)), ((), ())), preferred_element_type=F32)
    e = jnp.exp(logits - jnp.max(logits, axis=0, keepdims=True))
    prob = e / jnp.sum(e, axis=0, keepdims=True)
    expert_id = lax.broadcasted_iota(jnp.int32, (experts, tokens), 0)
    member = jnp.zeros((experts, tokens), F32)
    for k in range(idx_ref.shape[0]):
        hit = (expert_id == idx_ref[k : k + 1, :]) & (keep_ref[k : k + 1, :] > 0)
        member = jnp.where(hit, 1.0, member)
    earlier = lax.broadcasted_iota(jnp.int32, (tokens, tokens), 0) < lax.broadcasted_iota(jnp.int32, (tokens, tokens), 1)
    rank = dot(member.astype(BF16), jnp.where(earlier, 1.0, 0.0).astype(BF16))
    slot = jnp.where(member > 0, rank, -1.0)
    gate = ROUTE_SCALE * prob * member
    half = tab_ref.shape[1] // 2
    for d in range(tab_ref.shape[0]):
        tab_ref[d, :half, :] = slot[d * half : (d + 1) * half]
        tab_ref[d, half:, :] = gate[d * half : (d + 1) * half]


def relatives():
    me = lax.axis_index("ep")
    core, chip = lax.rem(me, 2), me // 2
    yb, xb = chip // 2, lax.rem(chip, 2)

    def first_core(r):
        return 2 * (2 * lax.rem(yb + r // 2, 2) + lax.rem(xb + lax.rem(r, 2), 2))

    return me, core, me + 1 - 2 * core, first_core


def up_kernel(
    wr_ref, idx_ref, keep_ref, x_hbm, w1_hbm, w3_hbm, sg_hbm, su_hbm, comb_hbm, hs_hbm, act_hbm, x_all,
    tab_ref, tabs, cbuf, xown, xbuf, xg, dbuf, wg, wu, hs, hg, hu, ab,
    own_sem, x_sem, w_sem, a_sem, hs_sem, c_sem, ts_sem, tr_sem, xs_sem, xr_sem,
):
    groups = tabs.shape[0]
    tokens, width = x_hbm.shape
    per_dev, _, ff = w1_hbm.shape
    slots, _, tn = wg.shape
    nt, ns = ff // tn, sg_hbm.shape[1] // tn
    steps = per_dev * nt
    xc = width // 2
    early = 2 * CAP
    late = groups * CAP - early
    forward_at = 7 * steps // 8
    near = late - 2 * CAP
    ahead = 2 * nt
    hand_at = 7 * ahead // 12

    me, core, partner, first_core = relatives()

    def block_copy(k, src, pos, device):
        return pltpu.make_async_remote_copy(
            src_ref=src, dst_ref=x_all.at[pos], send_sem=xs_sem.at[k], recv_sem=xr_sem.at[pos],
            device_id={"ep": device}, device_id_type=MESH)

    def table_copy(r, k):
        dst = first_core(r) + k
        return pltpu.make_async_remote_copy(
            src_ref=tab_ref.at[dst], dst_ref=tabs.at[2 * r + core], send_sem=ts_sem.at[2 * r + k], recv_sem=tr_sem.at[2 * r + core],
            device_id={"ep": dst}, device_id_type=MESH)

    sends = [
        block_copy(0, x_hbm, core, partner),
        block_copy(1, x_hbm, 2 + core, first_core(1) + core),
        block_copy(2, x_hbm, 4 + core, first_core(2) + core),
        block_copy(3, x_all.at[2 + core], 2 + core, partner),
        block_copy(4, x_all.at[4 + core], 4 + core, partner),
        block_copy(5, x_all.at[4 - core], 6 + core, first_core(1 + core) + core),
        block_copy(6, x_all.at[6 + core], 6 + core, partner),
    ]

    def arrived(pos):
        block_copy(0, x_hbm, pos, partner).wait_recv()

    def w_start(t):
        slot = lax.rem(t, slots)

        def go(a, b):
            pltpu.make_async_copy(a, wg.at[slot], w_sem.at[0, slot]).start()
            pltpu.make_async_copy(b, wu.at[slot], w_sem.at[1, slot]).start()

        @pl.when(t < ns)
        def _():
            cols = pl.ds(pl.multiple_of(t * tn, tn), tn)
            go(sg_hbm.at[:, cols], su_hbm.at[:, cols])

        for begin, n_tiles in ((ns, steps), (ns + steps, ahead), (ns + steps + ahead, steps)):
            @pl.when((t >= begin) & (t < begin + n_tiles))
            def _():
                it = t - begin
                cols = pl.ds(pl.multiple_of(lax.rem(it, nt) * tn, tn), tn)
                go(w1_hbm.at[it // nt, :, cols], w3_hbm.at[it // nt, :, cols])

    def w_wait(t):
        slot = lax.rem(t, slots)
        pltpu.make_async_copy(sg_hbm.at[:, pl.ds(0, tn)], wg.at[slot], w_sem.at[0, slot]).wait()
        pltpu.make_async_copy(sg_hbm.at[:, pl.ds(0, tn)], wu.at[slot], w_sem.at[1, slot]).wait()
        return slot

    own_copy = pltpu.make_async_copy(x_hbm, xown, own_sem)
    own_copy.start()
    for t in range(slots - 1):
        w_start(t)

    barrier = pltpu.get_barrier_semaphore()
    for d in range(1, groups):
        pl.semaphore_signal(barrier, inc=1, device_id={"ep": lax.rem(me + d, groups)}, device_id_type=MESH)
    own_copy.wait()
    route(xown[...], wr_ref[...], idx_ref, keep_ref, tab_ref)
    pl.semaphore_wait(barrier, groups - 1)
    for r in range(4):
        for k in range(2):
            if r == 0:
                @pl.when(k != core)
                def _():
                    table_copy(r, k).start()
            else:
                table_copy(r, k).start()
    for k in range(3):
        sends[k].start()
    tabs[core] = tab_ref[me]

    def gated_pass(first, n_steps, n_rows, lhs, before, after):
        def activate(h):
            return (jax.nn.silu(hg[h, :n_rows]) * hu[h, :n_rows]).astype(BF16)

        def body(i, _):
            for h in range(2):
                it = 2 * i + h
                w_start(first + it + slots - 1)
                slot = w_wait(first + it)
                last = it - 1
                before(last)
                ab[1 - h, :n_rows] = activate(1 - h)
                x = lhs(it)
                hg[h, :n_rows] = dot(x, wg[slot])
                hu[h, :n_rows] = dot(x, wu[slot])
                after(last)
            return 0

        lax.fori_loop(0, n_steps // 2, body, 0)
        before(n_steps - 1)
        ab[1, :n_rows] = activate(1)
        after(n_steps - 1)

    def s_copy(it):
        cols = pl.ds(pl.multiple_of(it * tn, tn), tn)
        return ab.at[lax.rem(it, 2), pl.ds(0, tokens)], hs.at[:, cols]

    def shared_after(it):
        @pl.when(it >= 0)
        def _():
            src, dst = s_copy(it)
            dst[...] = src[...]

    hg[...] = jnp.zeros_like(hg)
    hu[...] = jnp.zeros_like(hu)
    gated_pass(0, ns, tokens, lambda it: xown[...], lambda it: None, shared_after)

    hs_copy = pltpu.make_async_copy(hs, hs_hbm, hs_sem)
    hs_copy.start()

    row = lax.broadcasted_iota(jnp.int32, (CAP, tokens), 0).astype(F32)

    def x_copy(pos, slot):
        return pltpu.make_async_copy(x_all.at[pos], xbuf.at[slot], x_sem.at[slot])

    def gather(pos, x_ref, base):
        for e in range(per_dev):
            dbuf[e * CAP : (e + 1) * CAP, :] = jnp.where(row == tabs[pos, pl.ds(e, 1), :], 1.0, 0.0).astype(BF16)
        rows = pl.ds(pl.multiple_of(base, CAP), CAP)

        def cols_step(n, _):
            cols = pl.ds(pl.multiple_of(n * xc, xc), xc)
            got = dot(dbuf[...], x_ref[:, cols]).astype(BF16)
            xg[:, rows, cols] = got.reshape(per_dev, CAP, xc)
            return 0

        lax.fori_loop(0, width // xc, cols_step, 0)

    def a_copy(it, n_rows, base):
        cols = pl.ds(pl.multiple_of(lax.rem(it, nt) * tn, tn), tn)
        slot = lax.rem(it, 2)
        return pltpu.make_async_copy(ab.at[slot, pl.ds(0, n_rows)], act_hbm.at[it // nt, pl.ds(base, n_rows), cols], a_sem.at[slot])

    def expert_pass(first, tile0, n_tiles, n_rows, row0, base):
        def before(k):
            @pl.when(k >= 2)
            def _():
                a_copy(tile0 + k - 2, n_rows, base).wait()

        def after(k):
            @pl.when(k >= 0)
            def _():
                a_copy(tile0 + k, n_rows, base).start()

            if n_rows == near:
                @pl.when(k == hand_at)
                def _():
                    arrived(6 + core)
                    sends[6].start()
                    x_copy(6 + core, 0).start()

            if base == 0:
                @pl.when(k == forward_at)
                def _():
                    arrived(2 + core)
                    sends[3].start()
                    arrived(4 + core)
                    sends[4].start()
                    sends[5].start()
                    x_copy(2 + core, 0).start()
                    x_copy(4 + core, 1).start()

        def lhs(k):
            return xg[(tile0 + k) // nt, row0 : row0 + n_rows]

        gated_pass(first, n_tiles, n_rows, lhs, before, after)
        a_copy(tile0 + n_tiles - 2, n_rows, base).wait()
        a_copy(tile0 + n_tiles - 1, n_rows, base).wait()

    for p in range(groups):
        @pl.when(p != core)
        def _():
            pltpu.make_async_remote_copy(
                src_ref=tab_ref.at[0], dst_ref=tabs.at[p], send_sem=ts_sem.at[p], recv_sem=tr_sem.at[p],
                device_id={"ep": partner}, device_id_type=MESH).wait_recv()

    arrived(1 - core)
    x_copy(1 - core, 0).start()
    gather(core, xown, core * CAP)
    x_copy(1 - core, 0).wait()
    gather(1 - core, xbuf.at[0], (1 - core) * CAP)
    expert_pass(ns, 0, steps, early, 0, 0)

    n_slots = per_dev * CAP
    lane = lax.broadcasted_iota(jnp.int32, (per_dev, n_slots), 1)
    lead = lax.broadcasted_iota(jnp.int32, (per_dev, n_slots), 0) * CAP
    inside = (lane >= lead) & (lane < lead + CAP)
    spread = jnp.where(inside, 1.0, 0.0).astype(BF16)
    want = jnp.sum(jnp.where(inside, lane - lead, 0).astype(F32), axis=0, keepdims=True)

    def over_slots(v):
        return lax.dot_general(v, spread, (((0,), (0,)), ((), ())), preferred_element_type=F32)

    def c_copy(p):
        return pltpu.make_async_copy(cbuf.at[lax.rem(p, 2)], comb_hbm.at[p], c_sem.at[lax.rem(p, 2)])

    def build(p, _):
        @pl.when(p >= 2)
        def _():
            c_copy(p - 2).wait()

        hit = over_slots(tabs[p, :per_dev, :].astype(BF16)) == want
        gate = tabs[p, per_dev:, :]
        hi = gate.astype(BF16)
        rest = gate - hi.astype(F32)
        mid = rest.astype(BF16)
        low = (rest - mid.astype(F32)).astype(BF16)
        for k, piece in enumerate((hi, mid, low)):
            cbuf[lax.rem(p, 2), k * tokens : (k + 1) * tokens] = jnp.where(hit, over_slots(piece), 0.0).astype(BF16)
        c_copy(p).start()
        return 0

    order = [2 + core, 4 + core, 3 - core, 5 - core, 6 + core, 7 - core]
    for n, pos in enumerate(order):
        x_copy(pos, n % 2).wait()
        gather(pos, xbuf.at[n % 2], (pos - 2) * CAP)
        if n + 2 < 6:
            if n + 2 == 2:
                arrived(3 - core)
            if n + 2 == 3:
                arrived(5 - core)
            if n + 2 < 4:
                x_copy(order[n + 2], n % 2).start()
        if n == 3:
            lax.fori_loop(0, groups, build, 0)
            expert_pass(ns + steps, 0, ahead, near, 0, early)
            arrived(7 - core)
            x_copy(order[5], 1).start()
    expert_pass(ns + steps + ahead, 0, ahead, late - near, near, early + near)
    expert_pass(ns + steps + 2 * ahead, ahead, steps - ahead, late, 0, early)

    hs_copy.wait()
    c_copy(groups - 2).wait()
    c_copy(groups - 1).wait()
    for k in range(7):
        sends[k].wait_send()
    for r in range(4):
        for k in range(2):
            if r == 0:
                @pl.when(k != core)
                def _():
                    table_copy(r, k).wait_send()
            else:
                table_copy(r, k).wait_send()


def down_kernel(
    comb_hbm, act_hbm, w2_hbm, hs_hbm, sd_hbm, y_hbm, through,
    comb, act, part, wbuf, fsend, frecv, mine, bsend, brecv, acc, ybuf,
    act_sem, w_sem, comb_sem, hs_sem, y_sem, fs_sem, fr_sem, bs_sem, br_sem, ts_sem, tr_sem, credit,
):
    groups, per_dev, tokens = comb_hbm.shape[0], w2_hbm.shape[0], y_hbm.shape[0]
    cw = wbuf.shape[2]
    nc = acc.shape[0]
    steps = 4 * nc

    me, core, partner, first_core = relatives()

    def w_copy(it):
        slot = lax.rem(it, 4)
        c, e = it // per_dev, lax.rem(it, per_dev)
        cols = pl.ds(pl.multiple_of(c * cw, cw), cw)
        return pltpu.make_async_copy(w2_hbm.at[e, :, cols], wbuf.at[slot], w_sem.at[slot])

    def act_copy(e):
        return pltpu.make_async_copy(act_hbm.at[e], act.at[e], act_sem.at[e])

    def comb_copy(p):
        return pltpu.make_async_copy(comb_hbm.at[p], comb.at[p], comb_sem.at[p])

    ff = act.shape[2]

    def hs_copy(h):
        return pltpu.make_async_copy(hs_hbm.at[:, pl.ds(h * ff, ff)], act.at[h, pl.ds(0, tokens)], hs_sem.at[h])

    def sd_copy(c, h):
        cols = pl.ds(pl.multiple_of(c * cw, cw), cw)
        slot = 2 * lax.rem(c, 2) + h
        return pltpu.make_async_copy(sd_hbm.at[pl.ds(h * ff, ff), cols], wbuf.at[slot], w_sem.at[slot])

    for it in range(2):
        w_copy(it).start()
    for e in range(4):
        act_copy(e).start()

    barrier = pltpu.get_barrier_semaphore()
    pl.semaphore_signal(barrier, inc=1, device_id={"ep": partner}, device_id_type=MESH)
    for j in range(3):
        pl.semaphore_signal(barrier, inc=1, device_id={"ep": first_core(3 - j) + core}, device_id_type=MESH)
    pl.semaphore_wait(barrier, 4)

    def f_copy(g):
        out, land = lax.rem(g, 3), lax.rem(g, 4)
        return pltpu.make_async_remote_copy(
            src_ref=fsend.at[out], dst_ref=frecv.at[land], send_sem=fs_sem.at[out], recv_sem=fr_sem.at[land],
            device_id={"ep": partner}, device_id_type=MESH)

    def b_copy(j, c):
        slot = lax.rem(c, 2)
        return pltpu.make_async_remote_copy(
            src_ref=bsend.at[j, slot], dst_ref=brecv.at[j, c], send_sem=bs_sem.at[j, slot], recv_sem=br_sem.at[j, c],
            device_id={"ep": first_core(3 - j) + core}, device_id_type=MESH)

    def t_copy(c):
        slot = lax.rem(c, 2)
        return pltpu.make_async_remote_copy(
            src_ref=bsend.at[0, slot], dst_ref=through.at[c], send_sem=bs_sem.at[0, slot], recv_sem=tr_sem.at[c],
            device_id={"ep": first_core(1 + core) + core}, device_id_type=MESH)

    def pass_on(c):
        slot = lax.rem(c, 2)
        return pltpu.make_async_remote_copy(
            src_ref=through.at[c], dst_ref=brecv.at[0, c], send_sem=ts_sem.at[slot], recv_sem=br_sem.at[0, c],
            device_id={"ep": first_core(2 - core) + core}, device_id_type=MESH)

    def relay(c):
        @pl.when(c >= 2)
        def _():
            pass_on(c - 2).wait_send()

        t_copy(c).wait_recv()
        pass_on(c).start()

    def combine(s):
        pieces = dot(comb[s], part[s])
        return pieces[:tokens] + pieces[tokens : 2 * tokens] + pieces[2 * tokens :]

    def launch(j, c):
        if j == 0:
            @pl.when(c < nc - 1)
            def _():
                t_copy(c).start()

            @pl.when(c == nc - 1)
            def _():
                b_copy(0, c).start()
        elif j < 3:
            b_copy(j, c).start()

    def settle_wait(j, c):
        f_copy(4 * c + j).wait_recv()
        if j < 3:
            @pl.when(c >= 2)
            def _():
                b_copy(j, c - 2).wait_send()

    def settle(j, c):
        total = mine[lax.rem(4 * c + j, 3)] + frecv[j]
        if j < 3:
            bsend[j, lax.rem(c, 2)] = total.astype(BF16)
        else:
            acc[c] = total

    def credit_back(h):
        @pl.when((h >= 0) & (h + 4 < steps))
        def _():
            pl.semaphore_signal(credit, inc=1, device_id={"ep": partner}, device_id_type=MESH)

    def chunk(c, _, early=None):
        def down(i, _):
            for h in range(2):
                it = c * per_dev + 2 * i + h

                @pl.when(it + 2 < nc * per_dev)
                def _():
                    w_copy(it + 2).start()

                if early == 0:
                    act_copy(2 * i + h).wait()

                    @pl.when(2 * i + h + 4 < per_dev)
                    def _():
                        act_copy(2 * i + h + 4).start()

                    @pl.when(i == per_dev // 2 - 2)
                    def _():
                        comb_copy(6 + h).start()

                    @pl.when(i == per_dev // 2 - 1)
                    def _():
                        comb_copy(4 + h).start()

            for h in range(2):
                w_copy(c * per_dev + 2 * i + h).wait()
            got = []
            for h in range(2):
                it = c * per_dev + 2 * i + h
                got.append(dot(act[2 * i + h], wbuf[lax.rem(it, 4)]).astype(BF16))
            for h in range(2):
                part[:, pl.ds(pl.multiple_of((2 * i + h) * CAP, CAP), CAP), :] = got[h].reshape(groups, CAP, cw)
            return 0

        lax.fori_loop(0, per_dev // 2, down, 0)

        @pl.when(c == nc - 1)
        def _():
            for h in range(2):
                hs_copy(h).start()
                sd_copy(0, h).start()
                sd_copy(1, h).start()

        for j in range(4):
            g = 4 * c + j
            p = 2 * (3 - j)
            jj, cc = (j + 1) % 4, c if j == 3 else c - 1

            if early == 0:
                for k in range(2):
                    comb_copy(p + k).wait()
                    if j < 2:
                        comb_copy(p - 4 + k).start()

            late = early is None or (early == 1 and j >= 2)

            @pl.when(g >= 3)
            def _():
                f_copy(g - 3).wait_send()
                if late:
                    settle_wait(jj, cc)

            if late:
                settle(jj, cc)
            fsend[lax.rem(g, 3)] = combine(p + 1 - core)
            mine[lax.rem(g, 3)] = combine(p + core)
            if late:
                credit_back(g - 3)

            @pl.when(g >= 4)
            def _():
                pl.semaphore_wait(credit, 1)

            f_copy(g).start()

            if late:
                launch(jj, cc)
            elif early == 0 and j >= 1:
                settle_wait(j - 1, 0)
                settle(j - 1, 0)
                credit_back(j - 1)
                launch(j - 1, 0)

        @pl.when(c >= 1)
        def _():
            relay(c - 1)

        return 0

    for c in range(2):
        chunk(c, 0, early=c)
    lax.fori_loop(2, nc, chunk, 0)
    for j in range(1, 4):
        settle_wait(j, nc - 1)
        settle(j, nc - 1)
        launch(j, nc - 1)
    for g in range(steps - 3, steps):
        f_copy(g).wait_send()

    def y_copy(c):
        cols = pl.ds(pl.multiple_of(c * cw, cw), cw)
        return pltpu.make_async_copy(ybuf.at[lax.rem(c, 2)], y_hbm.at[:, cols], y_sem.at[lax.rem(c, 2)])

    for h in range(2):
        hs_copy(h).wait()

    def finish(c, _):
        for h in range(2):
            sd_copy(c, h).wait()
        for j in range(3):
            b_copy(j, c).wait_recv()

        @pl.when(c >= 2)
        def _():
            y_copy(c - 2).wait()

        slot = 2 * lax.rem(c, 2)
        total = acc[c] + dot(act[0, :tokens], wbuf[slot]) + dot(act[1, :tokens], wbuf[slot + 1])
        for j in range(3):
            total = total + brecv[j, c].astype(F32)
        ybuf[lax.rem(c, 2)] = total.astype(BF16)
        y_copy(c).start()

        @pl.when(c + 2 < nc)
        def _():
            for h in range(2):
                sd_copy(c + 2, h).start()

        return 0

    lax.fori_loop(0, nc, finish, 0)
    for c in (nc - 2, nc - 1):
        y_copy(c).wait()
        pass_on(c - 1).wait_send()
        for j in range(3):
            b_copy(j, c).wait_send()


def solution(mesh):
    groups = mesh.shape["ep"]
    tok_spec = P(("dp", "ep"), None)
    bank_spec = P("ep", None, None)
    vmem = pl.BlockSpec(memory_space=pltpu.VMEM)
    hbm = pl.BlockSpec(memory_space=pl.ANY)

    def device_fn(hidden, w_router, w_gate, w_up, w_down, shared_gate, shared_up, shared_down, top_idx, keep_mask):
        tokens, width = hidden.shape
        per_dev, _, ff = w_gate.shape
        rows = groups * CAP
        tn, cw = 256, 256
        nc = width // cw
        sff = shared_gate.shape[1]
        slots = 4
        table = (groups, 2 * per_dev, tokens)
        comb, shared_act, act, _ = pl.pallas_call(
            up_kernel,
            out_shape=(
                jax.ShapeDtypeStruct((groups, 3 * tokens, per_dev * CAP), BF16),
                jax.ShapeDtypeStruct((tokens, sff), BF16),
                jax.ShapeDtypeStruct((per_dev, rows, ff), BF16),
                jax.ShapeDtypeStruct((groups, tokens, width), BF16),
            ),
            in_specs=[vmem] * 3 + [hbm] * 5,
            out_specs=(hbm,) * 4,
            scratch_shapes=[
                pltpu.VMEM(table, F32),
                pltpu.VMEM(table, F32),
                pltpu.VMEM((2, 3 * tokens, per_dev * CAP), BF16),
                pltpu.VMEM((tokens, width), BF16),
                pltpu.VMEM((2, tokens, width), BF16),
                pltpu.VMEM((per_dev, rows - 2 * CAP, width), BF16),
                pltpu.VMEM((per_dev * CAP, tokens), BF16),
                pltpu.VMEM((slots, width, tn), BF16),
                pltpu.VMEM((slots, width, tn), BF16),
                pltpu.VMEM((tokens, sff), BF16),
                pltpu.VMEM((2, rows - 2 * CAP, tn), F32),
                pltpu.VMEM((2, rows - 2 * CAP, tn), F32),
                pltpu.VMEM((2, rows - 2 * CAP, tn), BF16),
                pltpu.SemaphoreType.DMA,
                pltpu.SemaphoreType.DMA((2,)),
                pltpu.SemaphoreType.DMA((2, slots)),
                pltpu.SemaphoreType.DMA((2,)),
                pltpu.SemaphoreType.DMA,
                pltpu.SemaphoreType.DMA((2,)),
                pltpu.SemaphoreType.DMA((groups,)),
                pltpu.SemaphoreType.DMA((groups,)),
                pltpu.SemaphoreType.DMA((7,)),
                pltpu.SemaphoreType.DMA((groups,)),
            ],
            compiler_params=pltpu.CompilerParams(vmem_limit_bytes=VMEM_BYTES, collective_id=1, has_side_effects=True),
            name="up",
        )(w_router.T, top_idx.T, keep_mask.T, hidden, w_gate, w_up, shared_gate, shared_up)
        y, _ = pl.pallas_call(
            down_kernel,
            out_shape=(
                jax.ShapeDtypeStruct((tokens, width), BF16),
                jax.ShapeDtypeStruct((nc, tokens, cw), BF16),
            ),
            in_specs=[hbm] * 5,
            out_specs=(hbm, hbm),
            scratch_shapes=[
                pltpu.VMEM((groups, 3 * tokens, per_dev * CAP), BF16),
                pltpu.VMEM((per_dev, rows, ff), BF16),
                pltpu.VMEM((groups, per_dev * CAP, cw), BF16),
                pltpu.VMEM((4, ff, cw), BF16),
                pltpu.VMEM((3, tokens, cw), F32),
                pltpu.VMEM((4, tokens, cw), F32),
                pltpu.VMEM((3, tokens, cw), F32),
                pltpu.VMEM((3, 2, tokens, cw), BF16),
                pltpu.VMEM((3, nc, tokens, cw), BF16),
                pltpu.VMEM((nc, tokens, cw), F32),
                pltpu.VMEM((2, tokens, cw), BF16),
                pltpu.SemaphoreType.DMA((per_dev,)),
                pltpu.SemaphoreType.DMA((4,)),
                pltpu.SemaphoreType.DMA((groups,)),
                pltpu.SemaphoreType.DMA((2,)),
                pltpu.SemaphoreType.DMA((2,)),
                pltpu.SemaphoreType.DMA((3,)),
                pltpu.SemaphoreType.DMA((4,)),
                pltpu.SemaphoreType.DMA((3, 2)),
                pltpu.SemaphoreType.DMA((3, nc)),
                pltpu.SemaphoreType.DMA((2,)),
                pltpu.SemaphoreType.DMA((nc,)),
                pltpu.SemaphoreType.REGULAR,
            ],
            compiler_params=pltpu.CompilerParams(vmem_limit_bytes=VMEM_BYTES, collective_id=0, has_side_effects=True),
            cost_estimate=pl.CostEstimate(flops=8 * per_dev * rows * width * ff, bytes_accessed=2 * per_dev * width * ff, transcendentals=0),
            name="down",
        )(comb, act, w_down, shared_act, shared_down)
        return y

    return jax.shard_map(device_fn, mesh=mesh, in_specs=(tok_spec, P(), bank_spec, bank_spec, bank_spec, P(), P(), P(), tok_spec, tok_spec), out_specs=tok_spec, check_vma=False)
```
